8 devices in a mesh: dp: 1 (over z), ing: 2 (over y), grp: 4 (over x, core).
Axes of the slice: x: 2, y: 2, z: 1, core: 2. Of those that a mesh axis runs over, the one named last changes fastest.
Arguments:
- x_tokens: bfloat16 [4096, 1536], P(('dp', 'grp', 'ing'))
- expert_ids: int32 [4096, 6], P(('dp', 'grp', 'ing'))
- gate_vals: float32 [4096, 6], P(('dp', 'grp', 'ing'))
- y_grad: bfloat16 [4096, 1536], P(('dp', 'grp', 'ing'))
- w_gate: bfloat16 [64, 1536, 512], P(('grp', 'ing'))
- w_up: bfloat16 [64, 1536, 512], P(('grp', 'ing'))
- w_down: bfloat16 [64, 512, 1536], P(('grp', 'ing'))
Outputs:
- output 1: bfloat16 [4096, 1536], P(('dp', 'grp', 'ing'))
- output 2: bfloat16 [4096, 1536], P(('dp', 'grp', 'ing'))
- output 3: float32 [64, 1536, 512], P(('dp', 'grp', 'ing'))
- output 4: float32 [64, 1536, 512], P(('dp', 'grp', 'ing'))
- output 5: float32 [64, 512, 1536], P(('dp', 'grp', 'ing'))
All inputs are finite; a program needn't handle non-finite values.
Results may differ from the reference program's by a relative error of at most 0.00959982.
Values are sent between devices in bfloat16 or wider.
A program may use at most 1 GiB of HBM per device.

```python
import jax
import jax.numpy as jnp
from jax import lax

HIDDEN = 1536
EXPERT_FF = 512
NUM_EXPERTS = 64
TOP_K = 6
TOKENS = 512
GROUPS = 4
INNER = 2
GROUP_LIMIT = 2

DEVICES = GROUPS * INNER
PER_GROUP = NUM_EXPERTS // GROUPS
PICKS = TOP_K // GROUP_LIMIT
GROUP_SLOTS = TOKENS * GROUP_LIMIT // GROUPS
CAPACITY = 3 * TOKENS * TOP_K // (2 * NUM_EXPERTS)


def draw_routing(dev_key):
    key_rank, key_group, key_expert, key_cols = jax.random.split(dev_key, 4)
    token_rank = jax.random.permutation(key_rank, TOKENS)
    group_perm = jax.random.permutation(key_group, GROUPS)
    expert_perm = jax.vmap(lambda sub_key: jax.random.permutation(sub_key, PER_GROUP))(jax.random.split(key_expert, GROUPS))
    col_perm = jax.vmap(lambda sub_key: jax.random.permutation(sub_key, TOP_K))(jax.random.split(key_cols, TOKENS))
    cycle_pos = token_rank[:, None] * GROUP_LIMIT + jnp.arange(GROUP_LIMIT)[None, :]
    chosen = group_perm[cycle_pos % GROUPS]
    order_in = (cycle_pos // GROUPS)[:, :, None]
    pick_ids = jnp.arange(PICKS)[None, None, :]
    half_slots = GROUP_SLOTS // 2
    wide_pos = (order_in * PICKS + pick_ids) % PER_GROUP
    narrow_pos = ((order_in - half_slots) * PICKS + pick_ids) % (PER_GROUP // 2)
    local_pos = jnp.where(order_in < half_slots, wide_pos, narrow_pos)
    local_ids = expert_perm[chosen[:, :, None], local_pos]
    global_ids = (chosen[:, :, None] * PER_GROUP + local_ids).reshape(TOKENS, TOP_K)
    return jnp.take_along_axis(global_ids, col_perm, axis=1).astype(jnp.int32)


def setup_inputs(seed: int = 0, part: int = 0) -> dict:
    part_key = jax.random.fold_in(jax.random.key(seed), part)
    key_route, key_gate, key_x, key_dy = jax.random.split(part_key, 4)
    route_keys = jax.random.split(key_route, DEVICES)
    expert_ids = jax.vmap(draw_routing)(route_keys).reshape(DEVICES * TOKENS, TOP_K)
    raw_gate = jnp.exp(0.5 * jax.random.normal(key_gate, (DEVICES * TOKENS, TOP_K), jnp.float32))
    gate_vals = raw_gate / jnp.sum(raw_gate, axis=1, keepdims=True)
    x_tokens = jax.random.normal(key_x, (DEVICES * TOKENS, HIDDEN), jnp.float32).astype(jnp.bfloat16)
    y_grad = jax.random.normal(key_dy, (DEVICES * TOKENS, HIDDEN), jnp.float32).astype(jnp.bfloat16)
    key_wg, key_wu, key_wd = jax.random.split(jax.random.key(seed + 1), 3)
    w_gate = (jax.random.normal(key_wg, (NUM_EXPERTS, HIDDEN, EXPERT_FF), jnp.float32) * HIDDEN ** -0.5).astype(jnp.bfloat16)
    w_up = (jax.random.normal(key_wu, (NUM_EXPERTS, HIDDEN, EXPERT_FF), jnp.float32) * HIDDEN ** -0.5).astype(jnp.bfloat16)
    w_down = (jax.random.normal(key_wd, (NUM_EXPERTS, EXPERT_FF, HIDDEN), jnp.float32) * EXPERT_FF ** -0.5).astype(jnp.bfloat16)
    return {'x_tokens': x_tokens, 'expert_ids': expert_ids, 'gate_vals': gate_vals, 'y_grad': y_grad, 'w_gate': w_gate, 'w_up': w_up, 'w_down': w_down}


def reference(x_tokens, expert_ids, gate_vals, y_grad, w_gate, w_up, w_down):
    total_tok = x_tokens.shape[0]
    slot_count = DEVICES * CAPACITY
    flat_ids = expert_ids.reshape(-1)
    flat_gates = gate_vals.reshape(-1)
    pair_order = jnp.argsort(flat_ids, stable=True).astype(jnp.int32)
    counts = jnp.bincount(flat_ids, length=NUM_EXPERTS)
    starts = jnp.cumsum(counts) - counts
    padded_order = jnp.concatenate([pair_order, jnp.zeros((slot_count,), jnp.int32)])
    zero_acc = jnp.zeros((total_tok, HIDDEN), jnp.float32)

    def expert_step(acc_pair, expert):
        part_y, part_dx = acc_pair
        pair_ids = lax.dynamic_slice(padded_order, (starts[expert],), (slot_count,))
        is_valid = jnp.arange(slot_count) < counts[expert]
        tok_rows = pair_ids // TOP_K
        slot_gate = jnp.where(is_valid, flat_gates[pair_ids], 0.0)
        xs_rows = x_tokens[tok_rows]
        dy_rows = y_grad[tok_rows]
        h_gate = jnp.dot(xs_rows, w_gate[expert], preferred_element_type=jnp.float32)
        h_up = jnp.dot(xs_rows, w_up[expert], preferred_element_type=jnp.float32)
        sig_gate = jax.nn.sigmoid(h_gate)
        silu_gate = h_gate * sig_gate
        act_bf = (silu_gate * h_up).astype(jnp.bfloat16)
        out_bf = jnp.dot(act_bf, w_down[expert], preferred_element_type=jnp.float32).astype(jnp.bfloat16)
        d_out = (slot_gate[:, None] * dy_rows.astype(jnp.float32)).astype(jnp.bfloat16)
        d_act = jnp.dot(d_out, w_down[expert].T, preferred_element_type=jnp.float32)
        d_hgate = (d_act * h_up * sig_gate * (1.0 + h_gate * (1.0 - sig_gate))).astype(jnp.bfloat16)
        d_hup = (d_act * silu_gate).astype(jnp.bfloat16)
        dx_rows = (jnp.dot(d_hgate, w_gate[expert].T, preferred_element_type=jnp.float32) + jnp.dot(d_hup, w_up[expert].T, preferred_element_type=jnp.float32)).astype(jnp.bfloat16)
        part_y = part_y.at[tok_rows].add(slot_gate[:, None] * out_bf.astype(jnp.float32))
        part_dx = part_dx.at[tok_rows].add(dx_rows.astype(jnp.float32))
        grad_gate = jnp.dot(xs_rows.T, d_hgate, preferred_element_type=jnp.float32)
        grad_up = jnp.dot(xs_rows.T, d_hup, preferred_element_type=jnp.float32)
        grad_down = jnp.dot(act_bf.T, d_out, preferred_element_type=jnp.float32)
        return (part_y, part_dx), (grad_gate, grad_up, grad_down)

    def group_step(acc_pair, group_id):
        y_acc, dx_acc = acc_pair
        expert_list = group_id * PER_GROUP + jnp.arange(PER_GROUP)
        (part_y, part_dx), grad_stack = lax.scan(expert_step, (zero_acc, zero_acc), expert_list)
        y_acc = y_acc + part_y.astype(jnp.bfloat16).astype(jnp.float32)
        dx_acc = dx_acc + part_dx.astype(jnp.bfloat16).astype(jnp.float32)
        return (y_acc, dx_acc), grad_stack

    (y_acc, dx_acc), grad_stack = lax.scan(group_step, (zero_acc, zero_acc), jnp.arange(GROUPS))
    grad_gate, grad_up, grad_down = grad_stack
    return (y_acc.astype(jnp.bfloat16), dx_acc.astype(jnp.bfloat16), grad_gate.reshape(NUM_EXPERTS, HIDDEN, EXPERT_FF), grad_up.reshape(NUM_EXPERTS, HIDDEN, EXPERT_FF), grad_down.reshape(NUM_EXPERTS, EXPERT_FF, HIDDEN))
```

```python
import functools

import jax
import jax.numpy as jnp
from jax import lax
from jax.experimental import pallas as pl
from jax.experimental.pallas import tpu as pltpu
from jax.sharding import PartitionSpec as P


BF = jnp.bfloat16
F32 = jnp.float32
PAIR = 2


def dot(a, b):
    return lax.dot_general(a, b, (((1,), (0,)), ((), ())), preferred_element_type=F32)


def dot_bt(a, b):
    return lax.dot_general(a, b, (((1,), (1,)), ((), ())), preferred_element_type=F32)


def dot_at(a, b):
    return lax.dot_general(a, b, (((0,), (0,)), ((), ())), preferred_element_type=F32)


def pick_rows(tok_col, rows_ref, source):
    tokens = rows_ref.shape[1]
    lanes = lax.broadcasted_iota(jnp.int32, (tok_col.shape[0], tokens), 1)
    one_hot = jnp.where(tok_col == lanes, 1.0, 0.0).astype(BF)
    return dot(one_hot, rows_ref[source])


def store_by_expert(dst_ref, rows, cap):
    for e in range(dst_ref.shape[0]):
        dst_ref[e] = jnp.concatenate([r[e * cap:(e + 1) * cap] for r in rows], axis=0).astype(BF)


def keep_rows(dst_ref, rows, e, cap, pad):
    zeros = jnp.zeros((pad - cap, rows.shape[1]), F32)
    for s in range(PAIR):
        padded = jnp.concatenate([rows[s * cap:(s + 1) * cap], zeros], axis=0).astype(BF)
        dst_ref[s, pl.ds(pl.multiple_of(e * pad, pad), pad), :] = padded


def fwd_kernel(cap, pad, x_ref, tok_ref, q_ref, g_ref, w1_ref, w3_ref, w2_ref, xg_ref, a_ref, u_ref, v_ref, p0_ref, p1_ref, xg_scr, o_scr):
    e = pl.program_id(0)

    @pl.when(e == 0)
    def _():
        store_by_expert(xg_scr, [pick_rows(tok_ref[s], x_ref, s) for s in range(PAIR)], cap)

    xg = xg_scr[e]
    xg_ref[0] = xg
    h1 = dot(xg, w1_ref[0])
    h3 = dot(xg, w3_ref[0])
    sig = jax.nn.sigmoid(h1)
    silu = h1 * sig
    act = (silu * h3).astype(BF)
    a_ref[0] = act
    u_ref[0] = h3 * (sig * (1.0 + h1 * (1.0 - sig)))
    v_ref[0] = silu
    keep_rows(o_scr, dot(act, w2_ref[0]), e, cap, pad)

    @pl.when(e == pl.num_programs(0) - 1)
    def _():
        for s, p_ref in enumerate((p0_ref, p1_ref)):
            slots = lax.broadcasted_iota(jnp.int32, (p_ref.shape[0], q_ref.shape[2]), 0)
            hit = q_ref[s] == slots
            rest = g_ref[s]
            total = None
            for _ in range(3):
                part = rest.astype(BF)
                term = dot(jnp.where(hit, part.astype(F32), 0.0).astype(BF), o_scr[s])
                total = term if total is None else total + term
                rest = rest - part.astype(F32)
            p_ref[...] = total


def bwd_kernel(cap, pad, dy_ref, tok_ref, gcol_ref, q_ref, w1_ref, w3_ref, w2_ref, u_ref, v_ref, d_ref, dh1_ref, dh3_ref, p0_ref, p1_ref, d_scr, r_scr):
    e = pl.program_id(0)

    @pl.when(e == 0)
    def _():
        store_by_expert(d_scr, [gcol_ref[s] * pick_rows(tok_ref[s], dy_ref, s) for s in range(PAIR)], cap)

    d = d_scr[e]
    d_ref[0] = d
    da = dot_bt(d, w2_ref[0])
    dh1 = (da * u_ref[0]).astype(BF)
    dh3 = (da * v_ref[0]).astype(BF)
    dh1_ref[0] = dh1
    dh3_ref[0] = dh3
    keep_rows(r_scr, dot_bt(dh1, w1_ref[0]) + dot_bt(dh3, w3_ref[0]), e, cap, pad)

    @pl.when(e == pl.num_programs(0) - 1)
    def _():
        for s, p_ref in enumerate((p0_ref, p1_ref)):
            slots = lax.broadcasted_iota(jnp.int32, (p_ref.shape[0], q_ref.shape[2]), 0)
            p_ref[...] = dot(jnp.where(q_ref[s] == slots, 1.0, 0.0).astype(BF), r_scr[s])


def whole(shape):
    return pl.BlockSpec(shape, lambda e: (0,) * len(shape))


def per_expert(shape):
    return pl.BlockSpec((1,) + shape[1:], lambda e: (e,) + (0,) * (len(shape) - 1))


def params():
    return pltpu.CompilerParams(dimension_semantics=("arbitrary",), vmem_limit_bytes=60 * 1024 * 1024)


def forward_pair(x2, tok_col, q_row, g_row, w1, w3, w2, cap, pad, grp_cap):
    experts, hidden, ff = w1.shape
    rows = PAIR * cap
    outs = [((experts, rows, hidden), BF), ((experts, rows, ff), BF), ((experts, rows, ff), F32), ((experts, rows, ff), F32), ((grp_cap, hidden), F32), ((grp_cap, hidden), F32)]
    return pl.pallas_call(
        functools.partial(fwd_kernel, cap, pad),
        grid=(experts,),
        in_specs=[whole(x2.shape), whole(tok_col.shape), whole(q_row.shape), whole(g_row.shape), per_expert(w1.shape), per_expert(w3.shape), per_expert(w2.shape)],
        out_specs=[per_expert(s) if len(s) == 3 else whole(s) for s, _ in outs],
        out_shape=[jax.ShapeDtypeStruct(s, t) for s, t in outs],
        scratch_shapes=[pltpu.VMEM((experts, rows, hidden), BF), pltpu.VMEM((PAIR, experts * pad, hidden), BF)],
        compiler_params=params(),
        cost_estimate=pl.CostEstimate(flops=14 * 10**9, bytes_accessed=50 * 10**6, transcendentals=0),
        name="fwd_pair",
    )(x2, tok_col, q_row, g_row, w1, w3, w2)


def backward_pair(dy2, tok_col, g_col, q_row, w1, w3, w2, u, v, cap, pad, grp_cap):
    experts, hidden, ff = w1.shape
    rows = PAIR * cap
    outs = [((experts, rows, hidden), BF), ((experts, rows, ff), BF), ((experts, rows, ff), BF), ((grp_cap, hidden), F32), ((grp_cap, hidden), F32)]
    return pl.pallas_call(
        functools.partial(bwd_kernel, cap, pad),
        grid=(experts,),
        in_specs=[whole(dy2.shape), whole(tok_col.shape), whole(g_col.shape), whole(q_row.shape), per_expert(w1.shape), per_expert(w3.shape), per_expert(w2.shape), per_expert(u.shape), per_expert(v.shape)],
        out_specs=[per_expert(s) if len(s) == 3 else whole(s) for s, _ in outs],
        out_shape=[jax.ShapeDtypeStruct(s, t) for s, t in outs],
        scratch_shapes=[pltpu.VMEM((experts, rows, hidden), BF), pltpu.VMEM((PAIR, experts * pad, hidden), BF)],
        compiler_params=params(),
        cost_estimate=pl.CostEstimate(flops=14 * 10**9, bytes_accessed=50 * 10**6, transcendentals=0),
        name="bwd_pair",
    )(dy2, tok_col, g_col, q_row, w1, w3, w2, u, v)


def dw_kernel(chunks, *refs):
    ins, (g1_ref, g3_ref, g2_ref) = refs[:5 * chunks], refs[5 * chunks:]

    def joined(k):
        return jnp.concatenate([ins[k * chunks + c][0] for c in range(chunks)], axis=0)

    x, a, d, dh1, dh3 = (joined(k) for k in range(5))
    g1_ref[0] = dot_at(x, dh1)
    g3_ref[0] = dot_at(x, dh3)
    g2_ref[0] = dot_at(a, d)


def weight_grads(xs, acts, ds, dh1s, dh3s):
    chunks = len(xs)
    experts, _, hidden = xs[0].shape
    ff = acts[0].shape[2]
    args = [*xs, *acts, *ds, *dh1s, *dh3s]
    outs = [(experts, hidden, ff), (experts, hidden, ff), (experts, ff, hidden)]
    return pl.pallas_call(
        functools.partial(dw_kernel, chunks),
        grid=(experts,),
        in_specs=[per_expert(a.shape) for a in args],
        out_specs=[per_expert(s) for s in outs],
        out_shape=[jax.ShapeDtypeStruct(s, F32) for s in outs],
        compiler_params=params(),
        cost_estimate=pl.CostEstimate(flops=25 * 10**9, bytes_accessed=120 * 10**6, transcendentals=0),
        name="weight_grads",
    )(*args)


def final_kernel(groups, *refs):
    q_ref, out_ref = refs[groups], refs[groups + 1]
    total = None
    for h in range(groups):
        lanes = lax.broadcasted_iota(jnp.int32, (out_ref.shape[0], refs[h].shape[0]), 1)
        one_hot = jnp.where(q_ref[:, h:h + 1] == lanes, 1.0, 0.0).astype(BF)
        term = dot(one_hot, refs[h][...])
        total = term if total is None else total + term
    out_ref[...] = total.astype(BF)


def collect(parts, q_cols):
    groups = len(parts)
    tokens = q_cols.shape[0]
    hidden = parts[0].shape[1]
    block = tokens // 4
    return pl.pallas_call(
        functools.partial(final_kernel, groups),
        grid=(4,),
        in_specs=[whole(p.shape) for p in parts] + [pl.BlockSpec((block, groups), lambda e: (e, 0))],
        out_specs=pl.BlockSpec((block, hidden), lambda e: (e, 0)),
        out_shape=jax.ShapeDtypeStruct((tokens, hidden), BF),
        compiler_params=params(),
        cost_estimate=pl.CostEstimate(flops=2 * 10**9, bytes_accessed=5 * 10**6, transcendentals=0),
        name="collect",
    )(*parts, q_cols)


def source_tables(ids_loc, gates_loc, num_exp, groups, cap):
    tokens, top_k = ids_loc.shape
    per_group = num_exp // groups
    ids_t, gates_t = ids_loc.T, gates_loc.T
    eq = ids_t[:, None, :] == jnp.arange(num_exp)[None, :, None]
    hit = jnp.any(eq, axis=0)
    gate = jnp.sum(jnp.where(eq, gates_t[:, None, :], 0.0), axis=0)
    member = jnp.any(hit.reshape(groups, per_group, tokens), axis=1)
    marks = jnp.concatenate([hit, member], axis=0).astype(BF)
    earlier = (jnp.arange(tokens)[:, None] < jnp.arange(tokens)[None, :]).astype(BF)
    pos = jnp.dot(marks, earlier, preferred_element_type=F32)
    exp_pos, grp_pos = pos[:num_exp], pos[num_exp:]
    taken = hit[:, None, :] & (exp_pos[:, None, :] == jnp.arange(cap, dtype=F32)[None, :, None])
    numbers = jnp.arange(1, tokens + 1, dtype=F32)[None, None, :]
    places = jnp.repeat(grp_pos + 1.0, per_group, axis=0)[:, None, :]
    tok = jnp.sum(jnp.where(taken, numbers, 0.0), axis=2) - 1.0
    place = jnp.sum(jnp.where(taken, places, 0.0), axis=2) - 1.0
    weight = jnp.sum(jnp.where(taken, gate[:, None, :], 0.0), axis=2)
    table = jnp.stack([tok, place, weight], axis=1)
    return table, jnp.where(member, grp_pos, -1.0).astype(jnp.int32)


def solution(mesh):
    groups = mesh.shape['grp']
    inner = mesh.shape['ing']
    devices = groups * inner
    tok_spec = P(('dp', 'grp', 'ing'), None)
    weight_spec = P(('grp', 'ing'), None, None)
    grad_spec = P(('dp', 'grp', 'ing'), None, None)

    def hop_y(a):
        return lax.ppermute(a, 'ing', [(0, 1), (1, 0)])

    def hop_g(a, bits):
        return lax.ppermute(a, 'grp', [(g, g ^ bits) for g in range(groups)])

    def device_fn(x_loc, ids_loc, gates_loc, dy_loc, w1, w3, w2):
        tokens, hidden = x_loc.shape
        top_k = ids_loc.shape[1]
        experts = w1.shape[0]
        num_exp = experts * devices
        grp_cap = tokens * 2 // groups
        cap = 3 * tokens * top_k // (2 * num_exp)
        pad = -(-cap // 16) * 16
        grp, ing = lax.axis_index('grp'), lax.axis_index('ing')

        def spread(rows):
            far = hop_y(rows)
            far_x = hop_g(far, 2)
            near_c = hop_g(rows, 1)
            far_c = hop_g(far, 1)
            near_x = hop_g(rows, 2)
            near_xc = hop_g(near_x, 1)
            far_xc = hop_g(far_x, 1)
            return [(far, far_c), (far_x, far_xc), (rows, near_c), (near_x, near_xc)]

        x_pairs = spread(x_loc)
        dy_pairs = spread(dy_loc)

        table, q_tok = source_tables(ids_loc, gates_loc, num_exp, groups, cap)
        table = lax.all_to_all(table.reshape(devices, experts, 3, cap), ('grp', 'ing'), 0, 0, tiled=True)
        order = [((grp ^ (2 * dx + dc)) * inner + (ing ^ dy)) for dx, dy in ((0, 1), (1, 1), (0, 0), (1, 0)) for dc in (0, 1)]
        table = jnp.take(table, jnp.stack(order), axis=0).transpose(2, 0, 1, 3)
        tok_rel, place_rel, weight_rel = table[0], table[1], table[2]
        slots = experts * cap
        tok_cols = tok_rel.astype(jnp.int32).reshape(devices, slots, 1)
        g_cols = weight_rel.reshape(devices, slots, 1)
        spare = ((0, 0), (0, 0), (0, pad - cap))
        q_rows = jnp.pad(place_rel, spare, constant_values=-1.0).astype(jnp.int32).reshape(devices, 1, experts * pad)
        g_rows = jnp.pad(weight_rel, spare).reshape(devices, 1, experts * pad)

        fwd, bwd = [], []
        for c in range(4):
            part = slice(PAIR * c, PAIR * c + PAIR)
            fwd.append(forward_pair(jnp.stack(x_pairs[c]), tok_cols[part], q_rows[part], g_rows[part], w1, w3, w2, cap, pad, grp_cap))
            bwd.append(backward_pair(jnp.stack(dy_pairs[c]), tok_cols[part], g_cols[part], q_rows[part], w1, w3, w2, fwd[c][2], fwd[c][3], cap, pad, grp_cap))

        grads = weight_grads([f[0] for f in fwd], [f[1] for f in fwd], [b[0] for b in bwd], [b[1] for b in bwd], [b[2] for b in bwd])

        def combine(results):
            sums = []
            for far, near in ((0, 2), (1, 3)):
                for s in (0, 1):
                    sums.append((results[near][s] + hop_y(results[far][s])).astype(BF))
            return [sums[0]] + [hop_g(sums[k], k) for k in (1, 2, 3)]

        q_cols = jnp.take(q_tok, jnp.stack([grp ^ k for k in range(groups)]), axis=0).T
        y_out = collect(combine([f[4:6] for f in fwd]), q_cols)
        dx_out = collect(combine([b[3:5] for b in bwd]), q_cols)
        return y_out, dx_out, grads[0], grads[1], grads[2]

    return jax.shard_map(device_fn, mesh=mesh, in_specs=(tok_spec, tok_spec, tok_spec, tok_spec, weight_spec, weight_spec, weight_spec), out_specs=(tok_spec, tok_spec, grad_spec, grad_spec, grad_spec), check_vma=False)
```

```python
import functools

import jax
import jax.numpy as jnp
from jax import lax
from jax.experimental import pallas as pl
from jax.experimental.pallas import tpu as pltpu
from jax.sharding import PartitionSpec as P


BF = jnp.bfloat16
F32 = jnp.float32
PAIR = 2

KERNEL_ORDER = (('f', 2), ('f', 0), ('b', 2), ('f', 1), ('b', 1), ('b', 0), ('f', 3), ('b', 3))


def dot(a, b):
    return lax.dot_general(a, b, (((1,), (0,)), ((), ())), preferred_element_type=F32)


def dot_bt(a, b):
    return lax.dot_general(a, b, (((1,), (1,)), ((), ())), preferred_element_type=F32)


def dot_at(a, b):
    return lax.dot_general(a, b, (((0,), (0,)), ((), ())), preferred_element_type=F32)


def pick_rows(tok_col, rows_ref):
    tokens = rows_ref.shape[0]
    lanes = lax.broadcasted_iota(jnp.int32, (tok_col.shape[0], tokens), 1)
    one_hot = jnp.where(tok_col == lanes, 1.0, 0.0).astype(BF)
    return dot(one_hot, rows_ref[...])


def store_by_expert(dst_ref, rows, cap):
    for e in range(dst_ref.shape[0]):
        dst_ref[e] = jnp.concatenate([r[e * cap:(e + 1) * cap] for r in rows], axis=0).astype(BF)


def keep_rows(dst_ref, rows, e, cap, pad):
    zeros = jnp.zeros((pad - cap, rows.shape[1]), F32)
    for s in range(PAIR):
        padded = jnp.concatenate([rows[s * cap:(s + 1) * cap], zeros], axis=0).astype(BF)
        dst_ref[s, pl.ds(pl.multiple_of(e * pad, pad), pad), :] = padded


def fwd_kernel(cap, pad, xa_ref, xb_ref, tok_ref, q_ref, g_ref, w1_ref, w3_ref, w2_ref, xg_ref, a_ref, u_ref, v_ref, p0_ref, p1_ref, xg_scr, o_scr):
    e = pl.program_id(0)

    @pl.when(e == 0)
    def _():
        store_by_expert(xg_scr, [pick_rows(tok_ref[s], r) for s, r in enumerate((xa_ref, xb_ref))], cap)

    xg = xg_scr[e]
    xg_ref[0] = xg
    h1 = dot(xg, w1_ref[0])
    h3 = dot(xg, w3_ref[0])
    sig = jax.nn.sigmoid(h1)
    silu = h1 * sig
    act = (silu * h3).astype(BF)
    a_ref[0] = act
    u_ref[0] = h3 * (sig * (1.0 + h1 * (1.0 - sig)))
    v_ref[0] = silu
    keep_rows(o_scr, dot(act, w2_ref[0]), e, cap, pad)

    @pl.when(e == pl.num_programs(0) - 1)
    def _():
        for s, p_ref in enumerate((p0_ref, p1_ref)):
            slots = lax.broadcasted_iota(jnp.int32, (p_ref.shape[0], q_ref.shape[2]), 0)
            hit = q_ref[s] == slots
            rest = g_ref[s]
            total = None
            for _ in range(3):
                part = rest.astype(BF)
                term = dot(jnp.where(hit, part.astype(F32), 0.0).astype(BF), o_scr[s])
                total = term if total is None else total + term
                rest = rest - part.astype(F32)
            p_ref[...] = total


def bwd_kernel(cap, pad, dya_ref, dyb_ref, tok_ref, gcol_ref, q_ref, w1_ref, w3_ref, w2_ref, u_ref, v_ref, d_ref, dh1_ref, dh3_ref, p0_ref, p1_ref, d_scr, r_scr):
    e = pl.program_id(0)

    @pl.when(e == 0)
    def _():
        store_by_expert(d_scr, [gcol_ref[s] * pick_rows(tok_ref[s], r) for s, r in enumerate((dya_ref, dyb_ref))], cap)

    d = d_scr[e]
    d_ref[0] = d
    da = dot_bt(d, w2_ref[0])
    dh1 = (da * u_ref[0]).astype(BF)
    dh3 = (da * v_ref[0]).astype(BF)
    dh1_ref[0] = dh1
    dh3_ref[0] = dh3
    keep_rows(r_scr, dot_bt(dh1, w1_ref[0]) + dot_bt(dh3, w3_ref[0]), e, cap, pad)

    @pl.when(e == pl.num_programs(0) - 1)
    def _():
        for s, p_ref in enumerate((p0_ref, p1_ref)):
            slots = lax.broadcasted_iota(jnp.int32, (p_ref.shape[0], q_ref.shape[2]), 0)
            p_ref[...] = dot(jnp.where(q_ref[s] == slots, 1.0, 0.0).astype(BF), r_scr[s])


def whole(shape):
    return pl.BlockSpec(shape, lambda e: (0,) * len(shape))


def per_expert(shape):
    return pl.BlockSpec((1,) + shape[1:], lambda e: (e,) + (0,) * (len(shape) - 1))


def of_pair(pair, shape):
    return pl.BlockSpec((PAIR,) + shape[1:], lambda e: (pair,) + (0,) * (len(shape) - 1))


def params():
    return pltpu.CompilerParams(dimension_semantics=("arbitrary",), vmem_limit_bytes=60 * 1024 * 1024)


def forward_pair(pair, xa, xb, tok_col, q_row, g_row, w1, w3, w2, cap, pad, grp_cap):
    experts, hidden, ff = w1.shape
    rows = PAIR * cap
    outs = [((experts, rows, hidden), BF), ((experts, rows, ff), BF), ((experts, rows, ff), F32), ((experts, rows, ff), F32), ((grp_cap, hidden), F32), ((grp_cap, hidden), F32)]
    return pl.pallas_call(
        functools.partial(fwd_kernel, cap, pad),
        grid=(experts,),
        in_specs=[whole(xa.shape), whole(xb.shape), of_pair(pair, tok_col.shape), of_pair(pair, q_row.shape), of_pair(pair, g_row.shape), per_expert(w1.shape), per_expert(w3.shape), per_expert(w2.shape)],
        out_specs=[per_expert(s) if len(s) == 3 else whole(s) for s, _ in outs],
        out_shape=[jax.ShapeDtypeStruct(s, t) for s, t in outs],
        scratch_shapes=[pltpu.VMEM((experts, rows, hidden), BF), pltpu.VMEM((PAIR, experts * pad, hidden), BF)],
        compiler_params=params(),
        cost_estimate=pl.CostEstimate(flops=14 * 10**9, bytes_accessed=50 * 10**6, transcendentals=0),
        name="fwd_pair",
    )(xa, xb, tok_col, q_row, g_row, w1, w3, w2)


def backward_pair(pair, dya, dyb, tok_col, g_col, q_row, w1, w3, w2, u, v, cap, pad, grp_cap):
    experts, hidden, ff = w1.shape
    rows = PAIR * cap
    outs = [((experts, rows, hidden), BF), ((experts, rows, ff), BF), ((experts, rows, ff), BF), ((grp_cap, hidden), F32), ((grp_cap, hidden), F32)]
    return pl.pallas_call(
        functools.partial(bwd_kernel, cap, pad),
        grid=(experts,),
        in_specs=[whole(dya.shape), whole(dyb.shape), of_pair(pair, tok_col.shape), of_pair(pair, g_col.shape), of_pair(pair, q_row.shape), per_expert(w1.shape), per_expert(w3.shape), per_expert(w2.shape), per_expert(u.shape), per_expert(v.shape)],
        out_specs=[per_expert(s) if len(s) == 3 else whole(s) for s, _ in outs],
        out_shape=[jax.ShapeDtypeStruct(s, t) for s, t in outs],
        scratch_shapes=[pltpu.VMEM((experts, rows, hidden), BF), pltpu.VMEM((PAIR, experts * pad, hidden), BF)],
        compiler_params=params(),
        cost_estimate=pl.CostEstimate(flops=14 * 10**9, bytes_accessed=50 * 10**6, transcendentals=0),
        name="bwd_pair",
    )(dya, dyb, tok_col, g_col, q_row, w1, w3, w2, u, v)


def dw_kernel(chunks, *refs):
    ins, (g1_ref, g3_ref, g2_ref) = refs[:5 * chunks], refs[5 * chunks:]

    def joined(k):
        return jnp.concatenate([ins[k * chunks + c][0] for c in range(chunks)], axis=0)

    x, a, d, dh1, dh3 = (joined(k) for k in range(5))
    g1_ref[0] = dot_at(x, dh1)
    g3_ref[0] = dot_at(x, dh3)
    g2_ref[0] = dot_at(a, d)


def weight_grads(xs, acts, ds, dh1s, dh3s):
    chunks = len(xs)
    experts, _, hidden = xs[0].shape
    ff = acts[0].shape[2]
    args = [*xs, *acts, *ds, *dh1s, *dh3s]
    outs = [(experts, hidden, ff), (experts, hidden, ff), (experts, ff, hidden)]
    return pl.pallas_call(
        functools.partial(dw_kernel, chunks),
        grid=(experts,),
        in_specs=[per_expert(a.shape) for a in args],
        out_specs=[per_expert(s) for s in outs],
        out_shape=[jax.ShapeDtypeStruct(s, F32) for s in outs],
        compiler_params=params(),
        cost_estimate=pl.CostEstimate(flops=25 * 10**9, bytes_accessed=120 * 10**6, transcendentals=0),
        name="weight_grads",
    )(*args)


def final_kernel(groups, *refs):
    q_ref, out_ref = refs[groups], refs[groups + 1]
    total = None
    for h in range(groups):
        lanes = lax.broadcasted_iota(jnp.int32, (out_ref.shape[0], refs[h].shape[0]), 1)
        one_hot = jnp.where(q_ref[:, h:h + 1] == lanes, 1.0, 0.0).astype(BF)
        term = dot(one_hot, refs[h][...])
        total = term if total is None else total + term
    out_ref[...] = total.astype(BF)


def collect(parts, q_cols):
    groups = len(parts)
    tokens = q_cols.shape[0]
    hidden = parts[0].shape[1]
    block = tokens // 4
    return pl.pallas_call(
        functools.partial(final_kernel, groups),
        grid=(4,),
        in_specs=[whole(p.shape) for p in parts] + [pl.BlockSpec((block, groups), lambda e: (e, 0))],
        out_specs=pl.BlockSpec((block, hidden), lambda e: (e, 0)),
        out_shape=jax.ShapeDtypeStruct((tokens, hidden), BF),
        compiler_params=params(),
        cost_estimate=pl.CostEstimate(flops=2 * 10**9, bytes_accessed=5 * 10**6, transcendentals=0),
        name="collect",
    )(*parts, q_cols)


def after(earlier, value):
    return lax.optimization_barrier((earlier, value))[1]


def slot_tables(ids, gates, first_exp, experts, group, per_group, cap):
    sources, _, tokens = ids.shape
    eq = ids[:, None] == (first_exp + jnp.arange(experts))[None, :, None, None]
    hit = jnp.any(eq, axis=2)
    gate = jnp.sum(jnp.where(eq, gates[:, None], 0.0), axis=2)
    member = jnp.any(ids // per_group == group, axis=1, keepdims=True)
    pos = count_earlier(jnp.concatenate([hit, member], axis=1).reshape(sources * (experts + 1), tokens))
    pos = pos.reshape(sources, experts + 1, tokens)
    exp_pos, grp_pos = pos[:, :experts], pos[:, experts:]
    taken = hit[:, :, None, :] & (exp_pos[:, :, None, :] == jnp.arange(cap, dtype=F32)[None, None, :, None])
    numbers = jnp.arange(1, tokens + 1, dtype=F32)[None, None, None, :]
    tok = jnp.sum(jnp.where(taken, numbers, 0.0), axis=3) - 1.0
    place = jnp.sum(jnp.where(taken, grp_pos[:, :, None, :] + 1.0, 0.0), axis=3) - 1.0
    weight = jnp.sum(jnp.where(taken, gate[:, :, None, :], 0.0), axis=3)
    return tok, place, weight


def count_earlier(marks):
    tokens = marks.shape[1]
    earlier = (jnp.arange(tokens)[:, None] < jnp.arange(tokens)[None, :]).astype(BF)
    return jnp.dot(marks.astype(BF), earlier, preferred_element_type=F32)


def solution(mesh):
    groups = mesh.shape['grp']
    inner = mesh.shape['ing']
    devices = groups * inner
    tok_spec = P(('dp', 'grp', 'ing'), None)
    weight_spec = P(('grp', 'ing'), None, None)
    grad_spec = P(('dp', 'grp', 'ing'), None, None)

    def hop_y(a):
        return lax.ppermute(a, 'ing', [(0, 1), (1, 0)])

    def hop_g(a, bits):
        return lax.ppermute(a, 'grp', [(g, g ^ bits) for g in range(groups)])

    def device_fn(x_loc, ids_loc, gates_loc, dy_loc, w1, w3, w2):
        tokens, _ = x_loc.shape
        top_k = ids_loc.shape[1]
        experts = w1.shape[0]
        num_exp = experts * devices
        grp_cap = tokens * 2 // groups
        cap = 3 * tokens * top_k // (2 * num_exp)
        pad = -(-cap // 16) * 16
        grp, ing = lax.axis_index('grp'), lax.axis_index('ing')

        per_group = experts * inner
        packed = jnp.concatenate([ids_loc.T.astype(F32), gates_loc.T], axis=0)
        routing = lax.all_gather(packed, ('grp', 'ing'))
        order = [((grp ^ (2 * dx + dc)) * inner + (ing ^ dy)) for dx, dy in ((0, 1), (1, 1), (0, 0), (1, 0)) for dc in (0, 1)]

        x_loc, dy_loc, routing = lax.optimization_barrier((x_loc, dy_loc, routing))
        x_far = hop_y(x_loc)
        x_near_c = hop_g(x_loc, 1)
        x_near_x = hop_g(x_loc, 2)
        dy_far = hop_y(dy_loc)
        dy_near_c = hop_g(dy_loc, 1)
        x_far_c, x_far_x = hop_g(x_far, 1), hop_g(x_far, 2)
        x_near_xc, x_far_xc = hop_g(x_near_x, 1), hop_g(x_far_x, 1)
        dy_far_c, dy_far_x = hop_g(dy_far, 1), hop_g(dy_far, 2)
        dy_far_xc = hop_g(dy_far_x, 1)
        dy_near_x = hop_g(after(x_far_x, dy_loc), 2)
        dy_near_xc = hop_g(dy_near_x, 1)
        x_pairs = [(x_far, x_far_c), (x_far_x, x_far_xc), (x_loc, x_near_c), (x_near_x, x_near_xc)]
        dy_pairs = [(dy_far, dy_far_c), (dy_far_x, dy_far_xc), (dy_loc, dy_near_c), (dy_near_x, dy_near_xc)]

        routing = jnp.take(routing, jnp.stack(order), axis=0)
        ids_rel, gates_rel = routing[:, :top_k].astype(jnp.int32), routing[:, top_k:]
        tok_rel, place_rel, weight_rel = slot_tables(ids_rel, gates_rel, (grp * inner + ing) * experts, experts, grp, per_group, cap)
        own_groups = ids_loc.T[None] // per_group == (grp ^ jnp.arange(groups))[:, None, None]
        own_member = jnp.any(own_groups, axis=1)
        q_cols = jnp.where(own_member, count_earlier(own_member), -1.0).astype(jnp.int32).T
        slots = experts * cap
        tok_cols = tok_rel.astype(jnp.int32).reshape(devices, slots, 1)
        g_cols = weight_rel.reshape(devices, slots, 1)
        spare = ((0, 0), (0, 0), (0, pad - cap))
        q_rows = jnp.pad(place_rel, spare, constant_values=-1.0).astype(jnp.int32).reshape(devices, 1, experts * pad)
        g_rows = jnp.pad(weight_rel, spare).reshape(devices, 1, experts * pad)

        fwd, bwd = [None] * 4, [None] * 4
        last = None
        for step, c in KERNEL_ORDER:
            rows = x_pairs[c] if step == 'f' else dy_pairs[c]
            places = q_rows if last is None else after(last, q_rows)
            if step == 'f':
                fwd[c] = forward_pair(c, *rows, tok_cols, places, g_rows, w1, w3, w2, cap, pad, grp_cap)
                last = fwd[c][4]
            else:
                bwd[c] = backward_pair(c, *rows, tok_cols, g_cols, places, w1, w3, w2, fwd[c][2], fwd[c][3], cap, pad, grp_cap)
                last = bwd[c][3]

        grads = weight_grads([f[0] for f in fwd], [f[1] for f in fwd], [b[0] for b in bwd], [b[1] for b in bwd], [b[2] for b in bwd])

        def combine(results):
            sums = []
            for far, near in ((0, 2), (1, 3)):
                for s in (0, 1):
                    sums.append((results[near][s] + hop_y(results[far][s])).astype(BF))
            return [sums[0]] + [hop_g(sums[k], k) for k in (1, 2, 3)]

        y_out = collect(combine([f[4:6] for f in fwd]), q_cols)
        dx_out = collect(combine([b[3:5] for b in bwd]), q_cols)
        return y_out, dx_out, grads[0], grads[1], grads[2]

    return jax.shard_map(device_fn, mesh=mesh, in_specs=(tok_spec, tok_spec, tok_spec, tok_spec, weight_spec, weight_spec, weight_spec), out_specs=(tok_spec, tok_spec, grad_spec, grad_spec, grad_spec), check_vma=False)
```

```python
import functools

import jax
import jax.numpy as jnp
from jax import lax
from jax.experimental import pallas as pl
from jax.experimental.pallas import tpu as pltpu
from jax.sharding import PartitionSpec as P


BF = jnp.bfloat16
F32 = jnp.float32
PAIR = 2

KERNEL_ORDER = (('f', 2), ('f', 0), ('b', 2), ('f', 1), ('b', 1), ('b', 0), ('f', 3), ('b', 3))


def dot(a, b):
    return lax.dot_general(a, b, (((1,), (0,)), ((), ())), preferred_element_type=F32)


def dot_bt(a, b):
    return lax.dot_general(a, b, (((1,), (1,)), ((), ())), preferred_element_type=F32)


def dot_at(a, b):
    return lax.dot_general(a, b, (((0,), (0,)), ((), ())), preferred_element_type=F32)


def pick_rows(tok_col, rows_ref):
    tokens = rows_ref.shape[0]
    lanes = lax.broadcasted_iota(jnp.int32, (tok_col.shape[0], tokens), 1)
    one_hot = jnp.where(tok_col == lanes, 1.0, 0.0).astype(BF)
    return dot(one_hot, rows_ref[...])


def store_by_expert(dst_ref, rows, cap):
    for e in range(dst_ref.shape[0]):
        dst_ref[e] = jnp.concatenate([r[e * cap:(e + 1) * cap] for r in rows], axis=0).astype(BF)


def keep_rows(dst_ref, rows, e, cap, pad):
    zeros = jnp.zeros((pad - cap, rows.shape[1]), F32)
    for s in range(PAIR):
        padded = jnp.concatenate([rows[s * cap:(s + 1) * cap], zeros], axis=0).astype(BF)
        dst_ref[s, pl.ds(pl.multiple_of(e * pad, pad), pad), :] = padded


def fwd_kernel(cap, pad, xa_ref, xb_ref, tok_ref, q_ref, g_ref, w1_ref, w3_ref, w2_ref, xg_ref, a_ref, u_ref, v_ref, p0_ref, p1_ref, xg_scr, o_scr):
    e = pl.program_id(0)

    @pl.when(e == 0)
    def _():
        store_by_expert(xg_scr, [pick_rows(tok_ref[s], r) for s, r in enumerate((xa_ref, xb_ref))], cap)

    xg = xg_scr[e]
    xg_ref[0] = xg
    h1 = dot(xg, w1_ref[0])
    h3 = dot(xg, w3_ref[0])
    sig = jax.nn.sigmoid(h1)
    silu = h1 * sig
    act = (silu * h3).astype(BF)
    a_ref[0] = act
    u_ref[0] = h3 * (sig * (1.0 + h1 * (1.0 - sig)))
    v_ref[0] = silu
    keep_rows(o_scr, dot(act, w2_ref[0]), e, cap, pad)

    @pl.when(e == pl.num_programs(0) - 1)
    def _():
        for s, p_ref in enumerate((p0_ref, p1_ref)):
            slots = lax.broadcasted_iota(jnp.int32, (p_ref.shape[0], q_ref.shape[2]), 0)
            hit = q_ref[s] == slots
            rest = g_ref[s]
            total = None
            for _ in range(3):
                part = rest.astype(BF)
                term = dot(jnp.where(hit, part.astype(F32), 0.0).astype(BF), o_scr[s])
                total = term if total is None else total + term
                rest = rest - part.astype(F32)
            p_ref[...] = total


def bwd_kernel(cap, pad, dya_ref, dyb_ref, tok_ref, gcol_ref, q_ref, w1_ref, w3_ref, w2_ref, u_ref, v_ref, d_ref, dh1_ref, dh3_ref, p0_ref, p1_ref, d_scr, r_scr):
    e = pl.program_id(0)

    @pl.when(e == 0)
    def _():
        store_by_expert(d_scr, [gcol_ref[s] * pick_rows(tok_ref[s], r) for s, r in enumerate((dya_ref, dyb_ref))], cap)

    d = d_scr[e]
    d_ref[0] = d
    da = dot_bt(d, w2_ref[0])
    dh1 = (da * u_ref[0]).astype(BF)
    dh3 = (da * v_ref[0]).astype(BF)
    dh1_ref[0] = dh1
    dh3_ref[0] = dh3
    keep_rows(r_scr, dot_bt(dh1, w1_ref[0]) + dot_bt(dh3, w3_ref[0]), e, cap, pad)

    @pl.when(e == pl.num_programs(0) - 1)
    def _():
        for s, p_ref in enumerate((p0_ref, p1_ref)):
            slots = lax.broadcasted_iota(jnp.int32, (p_ref.shape[0], q_ref.shape[2]), 0)
            p_ref[...] = dot(jnp.where(q_ref[s] == slots, 1.0, 0.0).astype(BF), r_scr[s])


def whole(shape):
    return pl.BlockSpec(shape, lambda e: (0,) * len(shape))


def per_expert(shape):
    return pl.BlockSpec((1,) + shape[1:], lambda e: (e,) + (0,) * (len(shape) - 1))


def of_pair(pair, shape):
    return pl.BlockSpec((PAIR,) + shape[1:], lambda e: (pair,) + (0,) * (len(shape) - 1))


def params():
    return pltpu.CompilerParams(dimension_semantics=("arbitrary",), vmem_limit_bytes=60 * 1024 * 1024)


def forward_pair(pair, xa, xb, tok_col, q_row, g_row, w1, w3, w2, cap, pad, grp_cap):
    experts, hidden, ff = w1.shape
    rows = PAIR * cap
    outs = [((experts, rows, hidden), BF), ((experts, rows, ff), BF), ((experts, rows, ff), F32), ((experts, rows, ff), F32), ((grp_cap, hidden), F32), ((grp_cap, hidden), F32)]
    return pl.pallas_call(
        functools.partial(fwd_kernel, cap, pad),
        grid=(experts,),
        in_specs=[whole(xa.shape), whole(xb.shape), of_pair(pair, tok_col.shape), of_pair(pair, q_row.shape), of_pair(pair, g_row.shape), per_expert(w1.shape), per_expert(w3.shape), per_expert(w2.shape)],
        out_specs=[per_expert(s) if len(s) == 3 else whole(s) for s, _ in outs],
        out_shape=[jax.ShapeDtypeStruct(s, t) for s, t in outs],
        scratch_shapes=[pltpu.VMEM((experts, rows, hidden), BF), pltpu.VMEM((PAIR, experts * pad, hidden), BF)],
        compiler_params=params(),
        cost_estimate=pl.CostEstimate(flops=14 * 10**9, bytes_accessed=50 * 10**6, transcendentals=0),
        name="fwd_pair",
    )(xa, xb, tok_col, q_row, g_row, w1, w3, w2)


def backward_pair(pair, dya, dyb, tok_col, g_col, q_row, w1, w3, w2, u, v, cap, pad, grp_cap):
    experts, hidden, ff = w1.shape
    rows = PAIR * cap
    outs = [((experts, rows, hidden), BF), ((experts, rows, ff), BF), ((experts, rows, ff), BF), ((grp_cap, hidden), F32), ((grp_cap, hidden), F32)]
    return pl.pallas_call(
        functools.partial(bwd_kernel, cap, pad),
        grid=(experts,),
        in_specs=[whole(dya.shape), whole(dyb.shape), of_pair(pair, tok_col.shape), of_pair(pair, g_col.shape), of_pair(pair, q_row.shape), per_expert(w1.shape), per_expert(w3.shape), per_expert(w2.shape), per_expert(u.shape), per_expert(v.shape)],
        out_specs=[per_expert(s) if len(s) == 3 else whole(s) for s, _ in outs],
        out_shape=[jax.ShapeDtypeStruct(s, t) for s, t in outs],
        scratch_shapes=[pltpu.VMEM((experts, rows, hidden), BF), pltpu.VMEM((PAIR, experts * pad, hidden), BF)],
        compiler_params=params(),
        cost_estimate=pl.CostEstimate(flops=14 * 10**9, bytes_accessed=50 * 10**6, transcendentals=0),
        name="bwd_pair",
    )(dya, dyb, tok_col, g_col, q_row, w1, w3, w2, u, v)


def dw_kernel(chunks, *refs):
    ins, (g1_ref, g3_ref, g2_ref) = refs[:5 * chunks], refs[5 * chunks:]

    def joined(k):
        return jnp.concatenate([ins[k * chunks + c][0] for c in range(chunks)], axis=0)

    x, a, d, dh1, dh3 = (joined(k) for k in range(5))
    g1_ref[0] = dot_at(x, dh1)
    g3_ref[0] = dot_at(x, dh3)
    g2_ref[0] = dot_at(a, d)


def weight_grads(xs, acts, ds, dh1s, dh3s):
    chunks = len(xs)
    experts, _, hidden = xs[0].shape
    ff = acts[0].shape[2]
    args = [*xs, *acts, *ds, *dh1s, *dh3s]
    outs = [(experts, hidden, ff), (experts, hidden, ff), (experts, ff, hidden)]
    return pl.pallas_call(
        functools.partial(dw_kernel, chunks),
        grid=(experts,),
        in_specs=[per_expert(a.shape) for a in args],
        out_specs=[per_expert(s) for s in outs],
        out_shape=[jax.ShapeDtypeStruct(s, F32) for s in outs],
        compiler_params=params(),
        cost_estimate=pl.CostEstimate(flops=25 * 10**9, bytes_accessed=120 * 10**6, transcendentals=0),
        name="weight_grads",
    )(*args)


def final_kernel(groups, *refs):
    q_ref, out_ref = refs[groups], refs[groups + 1]
    total = None
    for h in range(groups):
        lanes = lax.broadcasted_iota(jnp.int32, (out_ref.shape[0], refs[h].shape[0]), 1)
        one_hot = jnp.where(q_ref[:, h:h + 1] == lanes, 1.0, 0.0).astype(BF)
        term = dot(one_hot, refs[h][...])
        total = term if total is None else total + term
    out_ref[...] = total.astype(BF)


def collect(parts, q_cols):
    groups = len(parts)
    tokens = q_cols.shape[0]
    hidden = parts[0].shape[1]
    block = tokens // 4
    return pl.pallas_call(
        functools.partial(final_kernel, groups),
        grid=(4,),
        in_specs=[whole(p.shape) for p in parts] + [pl.BlockSpec((block, groups), lambda e: (e, 0))],
        out_specs=pl.BlockSpec((block, hidden), lambda e: (e, 0)),
        out_shape=jax.ShapeDtypeStruct((tokens, hidden), BF),
        compiler_params=params(),
        cost_estimate=pl.CostEstimate(flops=2 * 10**9, bytes_accessed=5 * 10**6, transcendentals=0),
        name="collect",
    )(*parts, q_cols)


def after(earlier, value):
    return lax.optimization_barrier((earlier, value))[1]


def slot_tables(ids, gates, first_exp, experts, group, per_group, cap):
    sources, _, tokens = ids.shape
    eq = ids[:, None] == (first_exp + jnp.arange(experts))[None, :, None, None]
    hit = jnp.any(eq, axis=2)
    gate = jnp.sum(jnp.where(eq, gates[:, None], 0.0), axis=2)
    member = jnp.any(ids // per_group == group, axis=1, keepdims=True)
    pos = count_earlier(jnp.concatenate([hit, member], axis=1).reshape(sources * (experts + 1), tokens))
    pos = pos.reshape(sources, experts + 1, tokens)
    exp_pos, grp_pos = pos[:, :experts], pos[:, experts:]
    taken = hit[:, :, None, :] & (exp_pos[:, :, None, :] == jnp.arange(cap, dtype=F32)[None, None, :, None])
    numbers = jnp.arange(1, tokens + 1, dtype=F32)[None, None, None, :]
    tok = jnp.sum(jnp.where(taken, numbers, 0.0), axis=3) - 1.0
    place = jnp.sum(jnp.where(taken, grp_pos[:, :, None, :] + 1.0, 0.0), axis=3) - 1.0
    weight = jnp.sum(jnp.where(taken, gate[:, :, None, :], 0.0), axis=3)
    return tok, place, weight


def count_earlier(marks):
    tokens = marks.shape[1]
    earlier = (jnp.arange(tokens)[:, None] < jnp.arange(tokens)[None, :]).astype(BF)
    return jnp.dot(marks.astype(BF), earlier, preferred_element_type=F32)


def solution(mesh):
    groups = mesh.shape['grp']
    inner = mesh.shape['ing']
    devices = groups * inner
    tok_spec = P(('dp', 'grp', 'ing'), None)
    weight_spec = P(('grp', 'ing'), None, None)
    grad_spec = P(('dp', 'grp', 'ing'), None, None)

    def hop_y(a):
        return lax.ppermute(a, 'ing', [(0, 1), (1, 0)])

    def hop_g(a, bits):
        return lax.ppermute(a, 'grp', [(g, g ^ bits) for g in range(groups)])

    def device_fn(x_loc, ids_loc, gates_loc, dy_loc, w1, w3, w2):
        tokens, _ = x_loc.shape
        top_k = ids_loc.shape[1]
        experts = w1.shape[0]
        num_exp = experts * devices
        grp_cap = tokens * 2 // groups
        cap = 3 * tokens * top_k // (2 * num_exp)
        pad = -(-cap // 16) * 16
        grp, ing = lax.axis_index('grp'), lax.axis_index('ing')

        per_group = experts * inner
        own = jnp.concatenate([ids_loc.T.astype(F32), gates_loc.T], axis=0)[None]
        pair = jnp.concatenate([own, hop_y(own)], axis=0)
        pair_c = hop_g(pair, 1)
        quad_x = hop_g(jnp.concatenate([pair, pair_c], axis=0), 2)
        routing = jnp.stack([pair[1], pair_c[1], quad_x[1], quad_x[3], pair[0], pair_c[0], quad_x[0], quad_x[2]])

        x_far = hop_y(x_loc)
        dy_far = hop_y(dy_loc)
        x_near_c = hop_g(after(pair_c, x_loc), 1)
        x_near_x = hop_g(after(quad_x, x_loc), 2)
        dy_near_c = hop_g(after(x_near_c, dy_loc), 1)
        x_far_c, x_far_x = hop_g(x_far, 1), hop_g(x_far, 2)
        x_near_xc, x_far_xc = hop_g(x_near_x, 1), hop_g(x_far_x, 1)
        dy_far_c, dy_far_x = hop_g(dy_far, 1), hop_g(dy_far, 2)
        dy_far_xc = hop_g(dy_far_x, 1)
        dy_near_x = hop_g(after(x_far_x, dy_loc), 2)
        dy_near_xc = hop_g(dy_near_x, 1)
        x_pairs = [(x_far, x_far_c), (x_far_x, x_far_xc), (x_loc, x_near_c), (x_near_x, x_near_xc)]
        dy_pairs = [(dy_far, dy_far_c), (dy_far_x, dy_far_xc), (dy_loc, dy_near_c), (dy_near_x, dy_near_xc)]

        ids_rel, gates_rel = routing[:, :top_k].astype(jnp.int32), routing[:, top_k:]
        tok_rel, place_rel, weight_rel = slot_tables(ids_rel, gates_rel, (grp * inner + ing) * experts, experts, grp, per_group, cap)
        own_groups = ids_loc.T[None] // per_group == (grp ^ jnp.arange(groups))[:, None, None]
        own_member = jnp.any(own_groups, axis=1)
        q_cols = jnp.where(own_member, count_earlier(own_member), -1.0).astype(jnp.int32).T
        slots = experts * cap
        tok_cols = tok_rel.astype(jnp.int32).reshape(devices, slots, 1)
        g_cols = weight_rel.reshape(devices, slots, 1)
        spare = ((0, 0), (0, 0), (0, pad - cap))
        q_rows = jnp.pad(place_rel, spare, constant_values=-1.0).astype(jnp.int32).reshape(devices, 1, experts * pad)
        g_rows = jnp.pad(weight_rel, spare).reshape(devices, 1, experts * pad)

        fwd, bwd = [None] * 4, [None] * 4
        last = None
        for step, c in KERNEL_ORDER:
            rows = x_pairs[c] if step == 'f' else dy_pairs[c]
            places = q_rows if last is None else after(last, q_rows)
            if step == 'f':
                fwd[c] = forward_pair(c, *rows, tok_cols, places, g_rows, w1, w3, w2, cap, pad, grp_cap)
                last = fwd[c][4]
            else:
                bwd[c] = backward_pair(c, *rows, tok_cols, g_cols, places, w1, w3, w2, fwd[c][2], fwd[c][3], cap, pad, grp_cap)
                last = bwd[c][3]

        grads = weight_grads([f[0] for f in fwd], [f[1] for f in fwd], [b[0] for b in bwd], [b[1] for b in bwd], [b[2] for b in bwd])

        def combine(results):
            sums = []
            for far, near in ((0, 2), (1, 3)):
                for s in (0, 1):
                    sums.append((results[near][s] + hop_y(results[far][s])).astype(BF))
            return [sums[0]] + [hop_g(sums[k], k) for k in (1, 2, 3)]

        y_out = collect(combine([f[4:6] for f in fwd]), q_cols)
        dx_out = collect(combine([b[3:5] for b in bwd]), q_cols)
        return y_out, dx_out, grads[0], grads[1], grads[2]

    return jax.shard_map(device_fn, mesh=mesh, in_specs=(tok_spec, tok_spec, tok_spec, tok_spec, weight_spec, weight_spec, weight_spec), out_specs=(tok_spec, tok_spec, grad_spec, grad_spec, grad_spec), check_vma=False)
```

```python
import functools

import jax
import jax.numpy as jnp
from jax import lax
from jax.experimental import pallas as pl
from jax.experimental.pallas import tpu as pltpu
from jax.sharding import PartitionSpec as P


BF = jnp.bfloat16
F32 = jnp.float32
PAIR = 2

KERNEL_ORDER = (('f', 0), ('n', 2), ('f', 1), ('b', 0), ('b', 1), ('n', 3))


def dot(a, b):
    return lax.dot_general(a, b, (((1,), (0,)), ((), ())), preferred_element_type=F32)


def dot_bt(a, b):
    return lax.dot_general(a, b, (((1,), (1,)), ((), ())), preferred_element_type=F32)


def dot_at(a, b):
    return lax.dot_general(a, b, (((0,), (0,)), ((), ())), preferred_element_type=F32)


def pick_rows(tok_col, rows_ref):
    tokens = rows_ref.shape[0]
    lanes = lax.broadcasted_iota(jnp.int32, (tok_col.shape[0], tokens), 1)
    one_hot = jnp.where(tok_col == lanes, 1.0, 0.0).astype(BF)
    return dot(one_hot, rows_ref[...])


def store_by_expert(dst_ref, rows, cap):
    for e in range(dst_ref.shape[0]):
        dst_ref[e] = jnp.concatenate([r[e * cap:(e + 1) * cap] for r in rows], axis=0).astype(BF)


def keep_rows(dst_ref, rows, e, cap, pad):
    zeros = jnp.zeros((pad - cap, rows.shape[1]), F32)
    for s in range(PAIR):
        padded = jnp.concatenate([rows[s * cap:(s + 1) * cap], zeros], axis=0).astype(BF)
        dst_ref[s, pl.ds(pl.multiple_of(e * pad, pad), pad), :] = padded


def spread_rows(dst_ref, tok_ref, row_refs, cap, gcol_ref=None):
    picked = [pick_rows(tok_ref[s], r) for s, r in enumerate(row_refs)]
    if gcol_ref is not None:
        picked = [gcol_ref[s] * p for s, p in enumerate(picked)]
    store_by_expert(dst_ref, picked, cap)


def forward_expert(xg, w1_ref, w3_ref):
    h1 = dot(xg, w1_ref[0])
    h3 = dot(xg, w3_ref[0])
    sig = jax.nn.sigmoid(h1)
    silu = h1 * sig
    act = (silu * h3).astype(BF)
    return act, h3 * (sig * (1.0 + h1 * (1.0 - sig))), silu


def group_sums(p_refs, q_ref, rows_scr, g_ref=None):
    for s, p_ref in enumerate(p_refs):
        slots = lax.broadcasted_iota(jnp.int32, (p_ref.shape[0], q_ref.shape[2]), 0)
        hit = q_ref[s] == slots
        if g_ref is None:
            p_ref[...] = dot(jnp.where(hit, 1.0, 0.0).astype(BF), rows_scr[s])
            continue
        rest = g_ref[s]
        total = None
        for _ in range(3):
            part = rest.astype(BF)
            term = dot(jnp.where(hit, part.astype(F32), 0.0).astype(BF), rows_scr[s])
            total = term if total is None else total + term
            rest = rest - part.astype(F32)
        p_ref[...] = total


def fwd_kernel(cap, pad, xa_ref, xb_ref, tok_ref, q_ref, g_ref, w1_ref, w3_ref, w2_ref, xg_ref, a_ref, u_ref, v_ref, p0_ref, p1_ref, xg_scr, o_scr):
    e = pl.program_id(0)

    @pl.when(e == 0)
    def _():
        spread_rows(xg_scr, tok_ref, (xa_ref, xb_ref), cap)

    xg_ref[0] = xg_scr[e]
    act, u_ref[0], v_ref[0] = forward_expert(xg_scr[e], w1_ref, w3_ref)
    a_ref[0] = act
    keep_rows(o_scr, dot(act, w2_ref[0]), e, cap, pad)

    @pl.when(e == pl.num_programs(0) - 1)
    def _():
        group_sums((p0_ref, p1_ref), q_ref, o_scr, g_ref)


def bwd_kernel(cap, pad, dya_ref, dyb_ref, tok_ref, gcol_ref, q_ref, w1_ref, w3_ref, w2_ref, u_ref, v_ref, d_ref, dh1_ref, dh3_ref, p0_ref, p1_ref, d_scr, r_scr):
    e = pl.program_id(0)

    @pl.when(e == 0)
    def _():
        spread_rows(d_scr, tok_ref, (dya_ref, dyb_ref), cap, gcol_ref)

    d_ref[0] = d_scr[e]
    da = dot_bt(d_scr[e], w2_ref[0])
    dh1 = (da * u_ref[0]).astype(BF)
    dh3 = (da * v_ref[0]).astype(BF)
    dh1_ref[0] = dh1
    dh3_ref[0] = dh3
    keep_rows(r_scr, dot_bt(dh1, w1_ref[0]) + dot_bt(dh3, w3_ref[0]), e, cap, pad)

    @pl.when(e == pl.num_programs(0) - 1)
    def _():
        group_sums((p0_ref, p1_ref), q_ref, r_scr)


def near_kernel(cap, pad, xa_ref, xb_ref, dya_ref, dyb_ref, tok_ref, gcol_ref, q_ref, g_ref, w1_ref, w3_ref, w2_ref, xg_ref, a_ref, d_ref, dh1_ref, dh3_ref, y0_ref, y1_ref, z0_ref, z1_ref, xg_scr, d_scr, o_scr, r_scr):
    e = pl.program_id(0)

    @pl.when(e == 0)
    def _():
        spread_rows(xg_scr, tok_ref, (xa_ref, xb_ref), cap)
        spread_rows(d_scr, tok_ref, (dya_ref, dyb_ref), cap, gcol_ref)

    xg_ref[0] = xg_scr[e]
    d_ref[0] = d_scr[e]
    act, u, v = forward_expert(xg_scr[e], w1_ref, w3_ref)
    a_ref[0] = act
    keep_rows(o_scr, dot(act, w2_ref[0]), e, cap, pad)
    da = dot_bt(d_scr[e], w2_ref[0])
    dh1 = (da * u).astype(BF)
    dh3 = (da * v).astype(BF)
    dh1_ref[0] = dh1
    dh3_ref[0] = dh3
    keep_rows(r_scr, dot_bt(dh1, w1_ref[0]) + dot_bt(dh3, w3_ref[0]), e, cap, pad)

    @pl.when(e == pl.num_programs(0) - 1)
    def _():
        group_sums((y0_ref, y1_ref), q_ref, o_scr, g_ref)
        group_sums((z0_ref, z1_ref), q_ref, r_scr)


def whole(shape):
    return pl.BlockSpec(shape, lambda e: (0,) * len(shape))


def per_expert(shape):
    return pl.BlockSpec((1,) + shape[1:], lambda e: (e,) + (0,) * (len(shape) - 1))


def once(shape):
    return pl.BlockSpec(shape, lambda e: (0,) * len(shape), pipeline_mode=pl.Buffered(1))


def of_pair(pair, shape):
    return pl.BlockSpec((PAIR,) + shape[1:], lambda e: (pair,) + (0,) * (len(shape) - 1))


def params():
    return pltpu.CompilerParams(dimension_semantics=("arbitrary",), vmem_limit_bytes=60 * 1024 * 1024)


def forward_pair(pair, xa, xb, tok_col, q_row, g_row, w1, w3, w2, cap, pad, grp_cap):
    experts, hidden, ff = w1.shape
    rows = PAIR * cap
    outs = [((experts, rows, hidden), BF), ((experts, rows, ff), BF), ((experts, rows, ff), F32), ((experts, rows, ff), F32), ((grp_cap, hidden), F32), ((grp_cap, hidden), F32)]
    return pl.pallas_call(
        functools.partial(fwd_kernel, cap, pad),
        grid=(experts,),
        in_specs=[whole(xa.shape), whole(xb.shape), of_pair(pair, tok_col.shape), of_pair(pair, q_row.shape), of_pair(pair, g_row.shape), per_expert(w1.shape), per_expert(w3.shape), per_expert(w2.shape)],
        out_specs=[per_expert(s) if len(s) == 3 else whole(s) for s, _ in outs],
        out_shape=[jax.ShapeDtypeStruct(s, t) for s, t in outs],
        scratch_shapes=[pltpu.VMEM((experts, rows, hidden), BF), pltpu.VMEM((PAIR, experts * pad, hidden), BF)],
        compiler_params=params(),
        cost_estimate=pl.CostEstimate(flops=14 * 10**9, bytes_accessed=50 * 10**6, transcendentals=0),
        name="fwd_pair",
    )(xa, xb, tok_col, q_row, g_row, w1, w3, w2)


def backward_pair(pair, dya, dyb, tok_col, g_col, q_row, w1, w3, w2, u, v, cap, pad, grp_cap):
    experts, hidden, ff = w1.shape
    rows = PAIR * cap
    outs = [((experts, rows, hidden), BF), ((experts, rows, ff), BF), ((experts, rows, ff), BF), ((grp_cap, hidden), F32), ((grp_cap, hidden), F32)]
    return pl.pallas_call(
        functools.partial(bwd_kernel, cap, pad),
        grid=(experts,),
        in_specs=[whole(dya.shape), whole(dyb.shape), of_pair(pair, tok_col.shape), of_pair(pair, g_col.shape), of_pair(pair, q_row.shape), per_expert(w1.shape), per_expert(w3.shape), per_expert(w2.shape), per_expert(u.shape), per_expert(v.shape)],
        out_specs=[per_expert(s) if len(s) == 3 else whole(s) for s, _ in outs],
        out_shape=[jax.ShapeDtypeStruct(s, t) for s, t in outs],
        scratch_shapes=[pltpu.VMEM((experts, rows, hidden), BF), pltpu.VMEM((PAIR, experts * pad, hidden), BF)],
        compiler_params=params(),
        cost_estimate=pl.CostEstimate(flops=14 * 10**9, bytes_accessed=50 * 10**6, transcendentals=0),
        name="bwd_pair",
    )(dya, dyb, tok_col, g_col, q_row, w1, w3, w2, u, v)


def near_pair(pair, xa, xb, dya, dyb, tok_col, g_col, q_row, g_row, w1, w3, w2, cap, pad, grp_cap):
    experts, hidden, ff = w1.shape
    rows = PAIR * cap
    wide, narrow, part = ((experts, rows, hidden), BF), ((experts, rows, ff), BF), ((grp_cap, hidden), F32)
    outs = [wide, narrow, wide, narrow, narrow, part, part, part, part]
    tables = [tok_col, g_col, q_row, g_row]
    return pl.pallas_call(
        functools.partial(near_kernel, cap, pad),
        grid=(experts,),
        in_specs=[once(xa.shape)] * 4 + [of_pair(pair, t.shape) for t in tables] + [per_expert(w1.shape), per_expert(w3.shape), per_expert(w2.shape)],
        out_specs=[per_expert(s) if len(s) == 3 else whole(s) for s, _ in outs],
        out_shape=[jax.ShapeDtypeStruct(s, t) for s, t in outs],
        scratch_shapes=[pltpu.VMEM((experts, rows, hidden), BF)] * 2 + [pltpu.VMEM((PAIR, experts * pad, hidden), BF)] * 2,
        compiler_params=params(),
        cost_estimate=pl.CostEstimate(flops=28 * 10**9, bytes_accessed=70 * 10**6, transcendentals=0),
        name="near_pair",
    )(xa, xb, dya, dyb, *tables, w1, w3, w2)


def dw_kernel(chunks, *refs):
    ins, (g1_ref, g3_ref, g2_ref) = refs[:5 * chunks], refs[5 * chunks:]

    def joined(k):
        return jnp.concatenate([ins[k * chunks + c][0] for c in range(chunks)], axis=0)

    x, a, d, dh1, dh3 = (joined(k) for k in range(5))
    g1_ref[0] = dot_at(x, dh1)
    g3_ref[0] = dot_at(x, dh3)
    g2_ref[0] = dot_at(a, d)


def weight_grads(xs, acts, ds, dh1s, dh3s):
    chunks = len(xs)
    experts, _, hidden = xs[0].shape
    ff = acts[0].shape[2]
    args = [*xs, *acts, *ds, *dh1s, *dh3s]
    outs = [(experts, hidden, ff), (experts, hidden, ff), (experts, ff, hidden)]
    return pl.pallas_call(
        functools.partial(dw_kernel, chunks),
        grid=(experts,),
        in_specs=[per_expert(a.shape) for a in args],
        out_specs=[per_expert(s) for s in outs],
        out_shape=[jax.ShapeDtypeStruct(s, F32) for s in outs],
        compiler_params=params(),
        cost_estimate=pl.CostEstimate(flops=25 * 10**9, bytes_accessed=120 * 10**6, transcendentals=0),
        name="weight_grads",
    )(*args)


def final_kernel(groups, *refs):
    q_ref, out_ref = refs[groups], refs[groups + 1]
    total = None
    for h in range(groups):
        lanes = lax.broadcasted_iota(jnp.int32, (out_ref.shape[0], refs[h].shape[0]), 1)
        one_hot = jnp.where(q_ref[:, h:h + 1] == lanes, 1.0, 0.0).astype(BF)
        term = dot(one_hot, refs[h][...])
        total = term if total is None else total + term
    out_ref[...] = total.astype(BF)


def collect(parts, q_cols):
    groups = len(parts)
    tokens = q_cols.shape[0]
    hidden = parts[0].shape[1]
    block = tokens // 4
    return pl.pallas_call(
        functools.partial(final_kernel, groups),
        grid=(4,),
        in_specs=[whole(p.shape) for p in parts] + [pl.BlockSpec((block, groups), lambda e: (e, 0))],
        out_specs=pl.BlockSpec((block, hidden), lambda e: (e, 0)),
        out_shape=jax.ShapeDtypeStruct((tokens, hidden), BF),
        compiler_params=params(),
        cost_estimate=pl.CostEstimate(flops=2 * 10**9, bytes_accessed=5 * 10**6, transcendentals=0),
        name="collect",
    )(*parts, q_cols)


def after(earlier, value):
    return lax.optimization_barrier((earlier, value))[1]


def slot_tables(ids, gates, first_exp, experts, group, per_group, cap):
    sources, _, tokens = ids.shape
    eq = ids[:, None] == (first_exp + jnp.arange(experts))[None, :, None, None]
    hit = jnp.any(eq, axis=2)
    gate = jnp.sum(jnp.where(eq, gates[:, None], 0.0), axis=2)
    member = jnp.any(ids // per_group == group, axis=1, keepdims=True)
    pos = count_earlier(jnp.concatenate([hit, member], axis=1).reshape(sources * (experts + 1), tokens))
    pos = pos.reshape(sources, experts + 1, tokens)
    exp_pos, grp_pos = pos[:, :experts], pos[:, experts:]
    taken = hit[:, :, None, :] & (exp_pos[:, :, None, :] == jnp.arange(cap, dtype=F32)[None, None, :, None])
    numbers = jnp.arange(1, tokens + 1, dtype=F32)[None, None, None, :]
    tok = jnp.sum(jnp.where(taken, numbers, 0.0), axis=3) - 1.0
    place = jnp.sum(jnp.where(taken, grp_pos[:, :, None, :] + 1.0, 0.0), axis=3) - 1.0
    weight = jnp.sum(jnp.where(taken, gate[:, :, None, :], 0.0), axis=3)
    return tok, place, weight


def count_earlier(marks):
    tokens = marks.shape[1]
    earlier = (jnp.arange(tokens)[:, None] < jnp.arange(tokens)[None, :]).astype(BF)
    return jnp.dot(marks.astype(BF), earlier, preferred_element_type=F32)


def solution(mesh):
    groups = mesh.shape['grp']
    inner = mesh.shape['ing']
    devices = groups * inner
    tok_spec = P(('dp', 'grp', 'ing'), None)
    weight_spec = P(('grp', 'ing'), None, None)
    grad_spec = P(('dp', 'grp', 'ing'), None, None)

    def hop_y(a):
        return lax.ppermute(a, 'ing', [(0, 1), (1, 0)])

    def hop_g(a, bits):
        return lax.ppermute(a, 'grp', [(g, g ^ bits) for g in range(groups)])

    def device_fn(x_loc, ids_loc, gates_loc, dy_loc, w1, w3, w2):
        tokens, _ = x_loc.shape
        top_k = ids_loc.shape[1]
        experts = w1.shape[0]
        num_exp = experts * devices
        grp_cap = tokens * 2 // groups
        cap = 3 * tokens * top_k // (2 * num_exp)
        pad = -(-cap // 16) * 16
        grp, ing = lax.axis_index('grp'), lax.axis_index('ing')

        per_group = experts * inner
        own = jnp.concatenate([ids_loc.T.astype(F32), gates_loc.T], axis=0)[None]
        pair = jnp.concatenate([own, hop_y(own)], axis=0)
        pair_c = hop_g(pair, 1)
        quad_x = hop_g(jnp.concatenate([pair, pair_c], axis=0), 2)
        routing = jnp.stack([pair[1], pair_c[1], quad_x[1], quad_x[3], pair[0], pair_c[0], quad_x[0], quad_x[2]])

        x_far = hop_y(x_loc)
        dy_far = hop_y(dy_loc)
        x_near_c = hop_g(after(pair_c, x_loc), 1)
        x_near_x = hop_g(after(quad_x, x_loc), 2)
        dy_near_c = hop_g(after(x_near_c, dy_loc), 1)
        x_far_c, x_far_x = hop_g(x_far, 1), hop_g(x_far, 2)
        x_near_xc, x_far_xc = hop_g(x_near_x, 1), hop_g(x_far_x, 1)
        dy_far_c, dy_far_x = hop_g(dy_far, 1), hop_g(dy_far, 2)
        dy_far_xc = hop_g(dy_far_x, 1)
        dy_near_x = hop_g(after(x_far_x, dy_loc), 2)
        dy_near_xc = hop_g(dy_near_x, 1)
        x_pairs = [(x_far, x_far_c), (x_far_x, x_far_xc), (x_loc, x_near_c), (x_near_x, x_near_xc)]
        dy_pairs = [(dy_far, dy_far_c), (dy_far_x, dy_far_xc), (dy_loc, dy_near_c), (dy_near_x, dy_near_xc)]

        ids_rel, gates_rel = routing[:, :top_k].astype(jnp.int32), routing[:, top_k:]
        tok_rel, place_rel, weight_rel = slot_tables(ids_rel, gates_rel, (grp * inner + ing) * experts, experts, grp, per_group, cap)
        own_groups = ids_loc.T[None] // per_group == (grp ^ jnp.arange(groups))[:, None, None]
        own_member = jnp.any(own_groups, axis=1)
        q_cols = jnp.where(own_member, count_earlier(own_member), -1.0).astype(jnp.int32).T
        slots = experts * cap
        tok_cols = tok_rel.astype(jnp.int32).reshape(devices, slots, 1)
        g_cols = weight_rel.reshape(devices, slots, 1)
        spare = ((0, 0), (0, 0), (0, pad - cap))
        q_rows = jnp.pad(place_rel, spare, constant_values=-1.0).astype(jnp.int32).reshape(devices, 1, experts * pad)
        g_rows = jnp.pad(weight_rel, spare).reshape(devices, 1, experts * pad)

        xs, acts, ds, dh1s, dh3s, y_sums, dx_sums = ([None] * 4 for _ in range(7))
        saved = {}
        last = None
        for step, c in KERNEL_ORDER:
            places = q_rows if last is None else after(last, q_rows)
            if step == 'n':
                xs[c], acts[c], ds[c], dh1s[c], dh3s[c], *sums = near_pair(c, *x_pairs[c], *dy_pairs[c], tok_cols, g_cols, places, g_rows, w1, w3, w2, cap, pad, grp_cap)
                y_sums[c], dx_sums[c] = sums[:PAIR], sums[PAIR:]
            elif step == 'f':
                xs[c], acts[c], *saved[c], y0, y1 = forward_pair(c, *x_pairs[c], tok_cols, places, g_rows, w1, w3, w2, cap, pad, grp_cap)
                y_sums[c] = (y0, y1)
            else:
                ds[c], dh1s[c], dh3s[c], *dx_sums[c] = backward_pair(c, *dy_pairs[c], tok_cols, g_cols, places, w1, w3, w2, *saved[c], cap, pad, grp_cap)
            last = (y_sums if step == 'f' else dx_sums)[c][0]

        grads = weight_grads(xs, acts, ds, dh1s, dh3s)

        def combine(results):
            sums = []
            for far, near in ((0, 2), (1, 3)):
                for s in (0, 1):
                    sums.append((results[near][s] + hop_y(results[far][s])).astype(BF))
            return [sums[0]] + [hop_g(sums[k], k) for k in (1, 2, 3)]

        y_out = collect(combine(y_sums), q_cols)
        dx_out = collect(combine(dx_sums), q_cols)
        return y_out, dx_out, grads[0], grads[1], grads[2]

    return jax.shard_map(device_fn, mesh=mesh, in_specs=(tok_spec, tok_spec, tok_spec, tok_spec, weight_spec, weight_spec, weight_spec), out_specs=(tok_spec, tok_spec, grad_spec, grad_spec, grad_spec), check_vma=False)
```

```python
import functools

import jax
import jax.numpy as jnp
from jax import lax
from jax.experimental import pallas as pl
from jax.experimental.pallas import tpu as pltpu
from jax.sharding import PartitionSpec as P


BF = jnp.bfloat16
F32 = jnp.float32
ALONE = 1024.0
SENT_SHARE = 7, 8
PAIR = 2

KERNEL_ORDER = (('f', 0), ('n', 2), ('f', 1), ('b', 0), ('b', 1), ('n', 3))


def dot(a, b):
    return lax.dot_general(a, b, (((1,), (0,)), ((), ())), preferred_element_type=F32)


def dot_bt(a, b):
    return lax.dot_general(a, b, (((1,), (1,)), ((), ())), preferred_element_type=F32)


def dot_at(a, b):
    return lax.dot_general(a, b, (((0,), (0,)), ((), ())), preferred_element_type=F32)


def pick_rows(tok_col, rows_ref):
    tokens = rows_ref.shape[0]
    lanes = lax.broadcasted_iota(jnp.int32, (tok_col.shape[0], tokens), 1)
    one_hot = jnp.where(tok_col == lanes, 1.0, 0.0).astype(BF)
    return dot(one_hot, rows_ref[...])


def store_by_expert(dst_ref, rows, cap):
    for e in range(dst_ref.shape[0]):
        dst_ref[e] = jnp.concatenate([r[e * cap:(e + 1) * cap] for r in rows], axis=0).astype(BF)


def keep_rows(dst_ref, rows, e, cap, pad):
    zeros = jnp.zeros((pad - cap, rows.shape[1]), F32)
    for s in range(PAIR):
        padded = jnp.concatenate([rows[s * cap:(s + 1) * cap], zeros], axis=0).astype(BF)
        dst_ref[s, pl.ds(pl.multiple_of(e * pad, pad), pad), :] = padded


def spread_rows(dst_ref, tok_ref, row_refs, cap, gcol_ref=None):
    picked = [pick_rows(tok_ref[s], r) for s, r in enumerate(row_refs)]
    if gcol_ref is not None:
        picked = [gcol_ref[s] * p for s, p in enumerate(picked)]
    store_by_expert(dst_ref, picked, cap)


def forward_expert(xg, w1_ref, w3_ref):
    h1 = dot(xg, w1_ref[0])
    h3 = dot(xg, w3_ref[0])
    sig = jax.nn.sigmoid(h1)
    silu = h1 * sig
    act = (silu * h3).astype(BF)
    return act, h3 * (sig * (1.0 + h1 * (1.0 - sig))), silu


def weighted_rows(hit, weight, rows):
    if weight is None:
        return dot(jnp.where(hit, 1.0, 0.0).astype(BF), rows)
    rest, total = weight, None
    for _ in range(3):
        part = rest.astype(BF)
        term = dot(jnp.where(hit, part.astype(F32), 0.0).astype(BF), rows)
        total = term if total is None else total + term
        rest = rest - part.astype(F32)
    return total


def group_sums(p_refs, q_ref, rows_scr, g_ref=None):
    for s, p_ref in enumerate(p_refs):
        slots = lax.broadcasted_iota(jnp.int32, (p_ref.shape[0], q_ref.shape[2]), 0)
        p_ref[...] = weighted_rows(q_ref[s] == slots, None if g_ref is None else g_ref[s], rows_scr[s])


def fwd_kernel(cap, pad, xa_ref, xb_ref, tok_ref, q_ref, g_ref, w1_ref, w3_ref, w2_ref, xg_ref, a_ref, u_ref, v_ref, p0_ref, p1_ref, xg_scr, o_scr):
    e = pl.program_id(0)

    @pl.when(e == 0)
    def _():
        spread_rows(xg_scr, tok_ref, (xa_ref, xb_ref), cap)

    xg_ref[0] = xg_scr[e]
    act, u_ref[0], v_ref[0] = forward_expert(xg_scr[e], w1_ref, w3_ref)
    a_ref[0] = act
    keep_rows(o_scr, dot(act, w2_ref[0]), e, cap, pad)

    @pl.when(e == pl.num_programs(0) - 1)
    def _():
        group_sums((p0_ref, p1_ref), q_ref, o_scr, g_ref)


def bwd_kernel(cap, pad, dya_ref, dyb_ref, tok_ref, gcol_ref, q_ref, w1_ref, w3_ref, w2_ref, u_ref, v_ref, d_ref, dh1_ref, dh3_ref, p0_ref, p1_ref, d_scr, r_scr):
    e = pl.program_id(0)

    @pl.when(e == 0)
    def _():
        spread_rows(d_scr, tok_ref, (dya_ref, dyb_ref), cap, gcol_ref)

    d_ref[0] = d_scr[e]
    da = dot_bt(d_scr[e], w2_ref[0])
    dh1 = (da * u_ref[0]).astype(BF)
    dh3 = (da * v_ref[0]).astype(BF)
    dh1_ref[0] = dh1
    dh3_ref[0] = dh3
    keep_rows(r_scr, dot_bt(dh1, w1_ref[0]) + dot_bt(dh3, w3_ref[0]), e, cap, pad)

    @pl.when(e == pl.num_programs(0) - 1)
    def _():
        group_sums((p0_ref, p1_ref), q_ref, r_scr)


def unit_rows(u_refs, unit_ref, rows_scr, weight_ref=None):
    for s, u_ref in enumerate(u_refs):
        units = lax.broadcasted_iota(jnp.int32, (u_ref.shape[0], unit_ref.shape[2]), 0)
        u_ref[...] = weighted_rows(unit_ref[s] == units, None if weight_ref is None else weight_ref[s], rows_scr[s]).astype(BF)


def far_fwd_kernel(cap, pad, xa_ref, xb_ref, tok_ref, q_ref, g_ref, unit_ref, form_ref, over_ref, w1_ref, w3_ref, w2_ref, xg_ref, a_ref, u_ref, v_ref, p0_ref, p1_ref, r0_ref, r1_ref, xg_scr, o_scr):
    e = pl.program_id(0)

    @pl.when(e == 0)
    def _():
        spread_rows(xg_scr, tok_ref, (xa_ref, xb_ref), cap)

    xg_ref[0] = xg_scr[e]
    act, u_ref[0], v_ref[0] = forward_expert(xg_scr[e], w1_ref, w3_ref)
    a_ref[0] = act
    keep_rows(o_scr, dot(act, w2_ref[0]), e, cap, pad)
    done = e == pl.num_programs(0) - 1

    @pl.when(done & (over_ref[0] == 0))
    def _():
        unit_rows((r0_ref, r1_ref), unit_ref, o_scr, form_ref)

    @pl.when(done & (over_ref[0] != 0))
    def _():
        group_sums((p0_ref, p1_ref), q_ref, o_scr, g_ref)


def far_bwd_kernel(cap, pad, dya_ref, dyb_ref, tok_ref, gcol_ref, q_ref, unit_ref, over_ref, w1_ref, w3_ref, w2_ref, u_ref, v_ref, d_ref, dh1_ref, dh3_ref, p0_ref, p1_ref, r0_ref, r1_ref, d_scr, r_scr):
    e = pl.program_id(0)

    @pl.when(e == 0)
    def _():
        spread_rows(d_scr, tok_ref, (dya_ref, dyb_ref), cap, gcol_ref)

    d_ref[0] = d_scr[e]
    da = dot_bt(d_scr[e], w2_ref[0])
    dh1 = (da * u_ref[0]).astype(BF)
    dh3 = (da * v_ref[0]).astype(BF)
    dh1_ref[0] = dh1
    dh3_ref[0] = dh3
    keep_rows(r_scr, dot_bt(dh1, w1_ref[0]) + dot_bt(dh3, w3_ref[0]), e, cap, pad)
    done = e == pl.num_programs(0) - 1

    @pl.when(done & (over_ref[0] == 0))
    def _():
        unit_rows((r0_ref, r1_ref), unit_ref, r_scr)

    @pl.when(done & (over_ref[0] != 0))
    def _():
        group_sums((p0_ref, p1_ref), q_ref, r_scr)


def merge_kernel(weighted, n0_ref, n1_ref, r0_ref, r1_ref, place_ref, weight_ref, p0_ref, p1_ref):
    for s, (n_ref, r_ref, p_ref) in enumerate(((n0_ref, r0_ref, p0_ref), (n1_ref, r1_ref, p1_ref))):
        places = lax.broadcasted_iota(jnp.int32, (n_ref.shape[0], r_ref.shape[0]), 0)
        total = weighted_rows(place_ref[s] == places, weight_ref[s] if weighted else None, r_ref[...])
        p_ref[...] = (n_ref[...] + total).astype(BF)


def near_kernel(cap, pad, xa_ref, xb_ref, dya_ref, dyb_ref, tok_ref, gcol_ref, q_ref, g_ref, w1_ref, w3_ref, w2_ref, xg_ref, a_ref, d_ref, dh1_ref, dh3_ref, y0_ref, y1_ref, z0_ref, z1_ref, xg_scr, d_scr, o_scr, r_scr):
    e = pl.program_id(0)

    @pl.when(e == 0)
    def _():
        spread_rows(xg_scr, tok_ref, (xa_ref, xb_ref), cap)
        spread_rows(d_scr, tok_ref, (dya_ref, dyb_ref), cap, gcol_ref)

    xg_ref[0] = xg_scr[e]
    d_ref[0] = d_scr[e]
    act, u, v = forward_expert(xg_scr[e], w1_ref, w3_ref)
    a_ref[0] = act
    keep_rows(o_scr, dot(act, w2_ref[0]), e, cap, pad)
    da = dot_bt(d_scr[e], w2_ref[0])
    dh1 = (da * u).astype(BF)
    dh3 = (da * v).astype(BF)
    dh1_ref[0] = dh1
    dh3_ref[0] = dh3
    keep_rows(r_scr, dot_bt(dh1, w1_ref[0]) + dot_bt(dh3, w3_ref[0]), e, cap, pad)

    @pl.when(e == pl.num_programs(0) - 1)
    def _():
        group_sums((y0_ref, y1_ref), q_ref, o_scr, g_ref)
        group_sums((z0_ref, z1_ref), q_ref, r_scr)


def whole(shape):
    return pl.BlockSpec(shape, lambda e: (0,) * len(shape))


def per_expert(shape):
    return pl.BlockSpec((1,) + shape[1:], lambda e: (e,) + (0,) * (len(shape) - 1))


def once(shape):
    return pl.BlockSpec(shape, lambda e: (0,) * len(shape), pipeline_mode=pl.Buffered(1))


def of_pair(pair, shape):
    return pl.BlockSpec((PAIR,) + shape[1:], lambda e: (pair,) + (0,) * (len(shape) - 1))


def params():
    return pltpu.CompilerParams(dimension_semantics=("arbitrary",), vmem_limit_bytes=60 * 1024 * 1024)


def forward_pair(pair, xa, xb, tok_col, q_row, g_row, w1, w3, w2, cap, pad, grp_cap):
    experts, hidden, ff = w1.shape
    rows = PAIR * cap
    outs = [((experts, rows, hidden), BF), ((experts, rows, ff), BF), ((experts, rows, ff), F32), ((experts, rows, ff), F32), ((grp_cap, hidden), F32), ((grp_cap, hidden), F32)]
    return pl.pallas_call(
        functools.partial(fwd_kernel, cap, pad),
        grid=(experts,),
        in_specs=[whole(xa.shape), whole(xb.shape), of_pair(pair, tok_col.shape), of_pair(pair, q_row.shape), of_pair(pair, g_row.shape), per_expert(w1.shape), per_expert(w3.shape), per_expert(w2.shape)],
        out_specs=[per_expert(s) if len(s) == 3 else whole(s) for s, _ in outs],
        out_shape=[jax.ShapeDtypeStruct(s, t) for s, t in outs],
        scratch_shapes=[pltpu.VMEM((experts, rows, hidden), BF), pltpu.VMEM((PAIR, experts * pad, hidden), BF)],
        compiler_params=params(),
        cost_estimate=pl.CostEstimate(flops=14 * 10**9, bytes_accessed=50 * 10**6, transcendentals=0),
        name="fwd_pair",
    )(xa, xb, tok_col, q_row, g_row, w1, w3, w2)


def backward_pair(pair, dya, dyb, tok_col, g_col, q_row, w1, w3, w2, u, v, cap, pad, grp_cap):
    experts, hidden, ff = w1.shape
    rows = PAIR * cap
    outs = [((experts, rows, hidden), BF), ((experts, rows, ff), BF), ((experts, rows, ff), BF), ((grp_cap, hidden), F32), ((grp_cap, hidden), F32)]
    return pl.pallas_call(
        functools.partial(bwd_kernel, cap, pad),
        grid=(experts,),
        in_specs=[whole(dya.shape), whole(dyb.shape), of_pair(pair, tok_col.shape), of_pair(pair, g_col.shape), of_pair(pair, q_row.shape), per_expert(w1.shape), per_expert(w3.shape), per_expert(w2.shape), per_expert(u.shape), per_expert(v.shape)],
        out_specs=[per_expert(s) if len(s) == 3 else whole(s) for s, _ in outs],
        out_shape=[jax.ShapeDtypeStruct(s, t) for s, t in outs],
        scratch_shapes=[pltpu.VMEM((experts, rows, hidden), BF), pltpu.VMEM((PAIR, experts * pad, hidden), BF)],
        compiler_params=params(),
        cost_estimate=pl.CostEstimate(flops=14 * 10**9, bytes_accessed=50 * 10**6, transcendentals=0),
        name="bwd_pair",
    )(dya, dyb, tok_col, g_col, q_row, w1, w3, w2, u, v)


def flag():
    return pl.BlockSpec(memory_space=pltpu.SMEM)


def far_forward_pair(pair, xa, xb, tok_col, q_row, g_row, unit_row, form_row, over, w1, w3, w2, cap, pad, grp_cap, units):
    experts, hidden, ff = w1.shape
    rows = PAIR * cap
    part, sent = ((grp_cap, hidden), F32), ((units, hidden), BF)
    outs = [((experts, rows, hidden), BF), ((experts, rows, ff), BF), ((experts, rows, ff), F32), ((experts, rows, ff), F32), part, part, sent, sent]
    tables = [tok_col, q_row, g_row, unit_row, form_row]
    return pl.pallas_call(
        functools.partial(far_fwd_kernel, cap, pad),
        grid=(experts,),
        in_specs=[whole(xa.shape), whole(xb.shape)] + [of_pair(pair, t.shape) for t in tables] + [flag(), per_expert(w1.shape), per_expert(w3.shape), per_expert(w2.shape)],
        out_specs=[per_expert(s) if len(s) == 3 else whole(s) for s, _ in outs],
        out_shape=[jax.ShapeDtypeStruct(s, t) for s, t in outs],
        scratch_shapes=[pltpu.VMEM((experts, rows, hidden), BF), pltpu.VMEM((PAIR, experts * pad, hidden), BF)],
        compiler_params=params(),
        cost_estimate=pl.CostEstimate(flops=14 * 10**9, bytes_accessed=50 * 10**6, transcendentals=0),
        name="far_fwd_pair",
    )(xa, xb, *tables, over, w1, w3, w2)


def far_backward_pair(pair, dya, dyb, tok_col, g_col, q_row, unit_row, over, w1, w3, w2, u, v, cap, pad, grp_cap, units):
    experts, hidden, ff = w1.shape
    rows = PAIR * cap
    part, sent = ((grp_cap, hidden), F32), ((units, hidden), BF)
    outs = [((experts, rows, hidden), BF), ((experts, rows, ff), BF), ((experts, rows, ff), BF), part, part, sent, sent]
    tables = [tok_col, g_col, q_row, unit_row]
    return pl.pallas_call(
        functools.partial(far_bwd_kernel, cap, pad),
        grid=(experts,),
        in_specs=[whole(dya.shape), whole(dyb.shape)] + [of_pair(pair, t.shape) for t in tables] + [flag(), per_expert(w1.shape), per_expert(w3.shape), per_expert(w2.shape), per_expert(u.shape), per_expert(v.shape)],
        out_specs=[per_expert(s) if len(s) == 3 else whole(s) for s, _ in outs],
        out_shape=[jax.ShapeDtypeStruct(s, t) for s, t in outs],
        scratch_shapes=[pltpu.VMEM((experts, rows, hidden), BF), pltpu.VMEM((PAIR, experts * pad, hidden), BF)],
        compiler_params=params(),
        cost_estimate=pl.CostEstimate(flops=14 * 10**9, bytes_accessed=50 * 10**6, transcendentals=0),
        name="far_bwd_pair",
    )(dya, dyb, *tables, over, w1, w3, w2, u, v)


def merge_pair(pair, near, sent, place, weight, weighted):
    grp_cap, hidden = near[0].shape
    units = sent[0].shape[0]
    block = hidden // 3
    return pl.pallas_call(
        functools.partial(merge_kernel, weighted),
        grid=(3,),
        in_specs=[pl.BlockSpec((grp_cap, block), lambda n: (0, n))] * 2 + [pl.BlockSpec((units, block), lambda n: (0, n))] * 2 + [of_pair(pair, place.shape), of_pair(pair, weight.shape)],
        out_specs=[pl.BlockSpec((grp_cap, block), lambda n: (0, n))] * 2,
        out_shape=[jax.ShapeDtypeStruct((grp_cap, hidden), BF)] * 2,
        compiler_params=params(),
        cost_estimate=pl.CostEstimate(flops=2 * 10**9, bytes_accessed=8 * 10**6, transcendentals=0),
        name="merge_pair",
    )(*near, *sent, place, weight)


def near_pair(pair, xa, xb, dya, dyb, tok_col, g_col, q_row, g_row, w1, w3, w2, cap, pad, grp_cap):
    experts, hidden, ff = w1.shape
    rows = PAIR * cap
    wide, narrow, part = ((experts, rows, hidden), BF), ((experts, rows, ff), BF), ((grp_cap, hidden), F32)
    outs = [wide, narrow, wide, narrow, narrow, part, part, part, part]
    tables = [tok_col, g_col, q_row, g_row]
    return pl.pallas_call(
        functools.partial(near_kernel, cap, pad),
        grid=(experts,),
        in_specs=[once(xa.shape)] * 4 + [of_pair(pair, t.shape) for t in tables] + [per_expert(w1.shape), per_expert(w3.shape), per_expert(w2.shape)],
        out_specs=[per_expert(s) if len(s) == 3 else whole(s) for s, _ in outs],
        out_shape=[jax.ShapeDtypeStruct(s, t) for s, t in outs],
        scratch_shapes=[pltpu.VMEM((experts, rows, hidden), BF)] * 2 + [pltpu.VMEM((PAIR, experts * pad, hidden), BF)] * 2,
        compiler_params=params(),
        cost_estimate=pl.CostEstimate(flops=28 * 10**9, bytes_accessed=70 * 10**6, transcendentals=0),
        name="near_pair",
    )(xa, xb, dya, dyb, *tables, w1, w3, w2)


def dw_kernel(chunks, *refs):
    ins, (g1_ref, g3_ref, g2_ref) = refs[:5 * chunks], refs[5 * chunks:]

    def joined(k):
        return jnp.concatenate([ins[k * chunks + c][0] for c in range(chunks)], axis=0)

    x, a, d, dh1, dh3 = (joined(k) for k in range(5))
    g1_ref[0] = dot_at(x, dh1)
    g3_ref[0] = dot_at(x, dh3)
    g2_ref[0] = dot_at(a, d)


def weight_grads(xs, acts, ds, dh1s, dh3s):
    chunks = len(xs)
    experts, _, hidden = xs[0].shape
    ff = acts[0].shape[2]
    args = [*xs, *acts, *ds, *dh1s, *dh3s]
    outs = [(experts, hidden, ff), (experts, hidden, ff), (experts, ff, hidden)]
    return pl.pallas_call(
        functools.partial(dw_kernel, chunks),
        grid=(experts,),
        in_specs=[per_expert(a.shape) for a in args],
        out_specs=[per_expert(s) for s in outs],
        out_shape=[jax.ShapeDtypeStruct(s, F32) for s in outs],
        compiler_params=params(),
        cost_estimate=pl.CostEstimate(flops=25 * 10**9, bytes_accessed=120 * 10**6, transcendentals=0),
        name="weight_grads",
    )(*args)


def final_kernel(groups, *refs):
    q_ref, out_ref = refs[groups], refs[groups + 1]
    total = None
    for h in range(groups):
        lanes = lax.broadcasted_iota(jnp.int32, (out_ref.shape[0], refs[h].shape[0]), 1)
        one_hot = jnp.where(q_ref[:, h:h + 1] == lanes, 1.0, 0.0).astype(BF)
        term = dot(one_hot, refs[h][...])
        total = term if total is None else total + term
    out_ref[...] = total.astype(BF)


def collect(parts, q_cols):
    groups = len(parts)
    tokens = q_cols.shape[0]
    hidden = parts[0].shape[1]
    block = tokens // 4
    return pl.pallas_call(
        functools.partial(final_kernel, groups),
        grid=(4,),
        in_specs=[whole(p.shape) for p in parts] + [pl.BlockSpec((block, groups), lambda e: (e, 0))],
        out_specs=pl.BlockSpec((block, hidden), lambda e: (e, 0)),
        out_shape=jax.ShapeDtypeStruct((tokens, hidden), BF),
        compiler_params=params(),
        cost_estimate=pl.CostEstimate(flops=2 * 10**9, bytes_accessed=5 * 10**6, transcendentals=0),
        name="collect",
    )(*parts, q_cols)


def after(earlier, value):
    return lax.optimization_barrier((earlier, value))[1]


def slot_tables(ids, gates, first_exp, experts, group, per_group, cap):
    sources, _, tokens = ids.shape
    eq = ids[:, None] == (first_exp + jnp.arange(experts))[None, :, None, None]
    hit = jnp.any(eq, axis=2)
    gate = jnp.sum(jnp.where(eq, gates[:, None], 0.0), axis=2)
    member = jnp.any(ids // per_group == group, axis=1, keepdims=True)
    pos = count_earlier(jnp.concatenate([hit, member], axis=1).reshape(sources * (experts + 1), tokens))
    pos = pos.reshape(sources, experts + 1, tokens)
    exp_pos, grp_pos = pos[:, :experts], pos[:, experts:]
    taken = hit[:, :, None, :] & (exp_pos[:, :, None, :] == jnp.arange(cap, dtype=F32)[None, None, :, None])
    numbers = jnp.arange(1, tokens + 1, dtype=F32)[None, None, None, :]
    tok = jnp.sum(jnp.where(taken, numbers, 0.0), axis=3) - 1.0
    place = jnp.sum(jnp.where(taken, grp_pos[:, :, None, :] + 1.0, 0.0), axis=3) - 1.0
    weight = jnp.sum(jnp.where(taken, gate[:, :, None, :], 0.0), axis=3)
    here = jnp.sum(hit, axis=1).astype(F32)
    alone = here == jnp.sum(ids // per_group == group, axis=1).astype(F32)
    first = count_earlier(jnp.where(alone, jnp.minimum(here, 1.0), here))
    rank, seen = [], jnp.zeros((sources, tokens), F32)
    for e in range(experts):
        rank.append(seen)
        seen = seen + hit[:, e].astype(F32)
    unit = first[:, None] + jnp.where(alone[:, None], ALONE, jnp.stack(rank, axis=1)) + 1.0
    code = jnp.sum(jnp.where(taken, unit[:, :, None, :], 0.0), axis=3)
    lone = code > ALONE
    return tok, place, weight, jnp.where(lone, code - ALONE, code) - 1.0, lone


def longest_list(ids, per_group, experts, away):
    devices = away.shape[1]
    count = jnp.sum(ids[:, None] // experts == jnp.arange(devices)[None, :, None, None], axis=2)
    half = per_group // experts
    in_group = jnp.repeat(jnp.sum(count.reshape(ids.shape[0], devices // half, half, -1), axis=2), half, axis=1)
    rows = jnp.where(count == in_group, jnp.minimum(count, 1), count)
    return jnp.max(jnp.where(away, jnp.sum(rows, axis=2), 0))


def count_earlier(marks):
    tokens = marks.shape[1]
    earlier = (jnp.arange(tokens)[:, None] < jnp.arange(tokens)[None, :]).astype(BF)
    return jnp.dot(marks.astype(BF), earlier, preferred_element_type=F32)


def solution(mesh):
    groups = mesh.shape['grp']
    inner = mesh.shape['ing']
    devices = groups * inner
    tok_spec = P(('dp', 'grp', 'ing'), None)
    weight_spec = P(('grp', 'ing'), None, None)
    grad_spec = P(('dp', 'grp', 'ing'), None, None)

    def hop_y(a):
        return lax.ppermute(a, 'ing', [(0, 1), (1, 0)])

    def hop_g(a, bits):
        return lax.ppermute(a, 'grp', [(g, g ^ bits) for g in range(groups)])

    def device_fn(x_loc, ids_loc, gates_loc, dy_loc, w1, w3, w2):
        tokens, _ = x_loc.shape
        top_k = ids_loc.shape[1]
        experts = w1.shape[0]
        num_exp = experts * devices
        grp_cap = tokens * 2 // groups
        cap = 3 * tokens * top_k // (2 * num_exp)
        pad = -(-cap // 16) * 16
        grp, ing = lax.axis_index('grp'), lax.axis_index('ing')

        per_group = experts * inner
        own = jnp.concatenate([ids_loc.T.astype(F32), gates_loc.T], axis=0)[None]
        pair = jnp.concatenate([own, hop_y(own)], axis=0)
        pair_c = hop_g(pair, 1)
        quad_x = hop_g(jnp.concatenate([pair, pair_c], axis=0), 2)
        routing = jnp.stack([pair[1], pair_c[1], quad_x[1], quad_x[3], pair[0], pair_c[0], quad_x[0], quad_x[2]])

        x_far = hop_y(x_loc)
        dy_far = hop_y(dy_loc)
        x_near_c = hop_g(after(pair_c, x_loc), 1)
        x_near_x = hop_g(after(quad_x, x_loc), 2)
        dy_near_c = hop_g(after(x_near_c, dy_loc), 1)
        x_far_c, x_far_x = hop_g(x_far, 1), hop_g(x_far, 2)
        x_near_xc, x_far_xc = hop_g(x_near_x, 1), hop_g(x_far_x, 1)
        dy_far_c, dy_far_x = hop_g(dy_far, 1), hop_g(dy_far, 2)
        dy_far_xc = hop_g(dy_far_x, 1)
        dy_near_x = hop_g(after(x_far_x, dy_loc), 2)
        dy_near_xc = hop_g(dy_near_x, 1)
        x_pairs = [(x_far, x_far_c), (x_far_x, x_far_xc), (x_loc, x_near_c), (x_near_x, x_near_xc)]
        dy_pairs = [(dy_far, dy_far_c), (dy_far_x, dy_far_xc), (dy_loc, dy_near_c), (dy_near_x, dy_near_xc)]

        ids_rel, gates_rel = routing[:, :top_k].astype(jnp.int32), routing[:, top_k:]
        units = tokens * SENT_SHARE[0] // SENT_SHARE[1]
        tok_rel, place_rel, weight_rel, unit_rel, lone_rel = slot_tables(ids_rel, gates_rel, (grp * inner + ing) * experts, experts, grp, per_group, cap)
        far = devices // 2
        source_ing = jnp.where(jnp.arange(devices) < far, 1 - ing, ing)
        away = source_ing[:, None] != (jnp.arange(devices) % inner)[None, :]
        over = longest_list(ids_rel, per_group, experts, away) > units
        over_flag = over.astype(jnp.int32).reshape(1)
        flat = [t[:far].reshape(far, 1, -1) for t in (unit_rel, place_rel, jnp.where(lone_rel, 1.0, weight_rel))]
        sent_here = flat[0] == jnp.arange(units, dtype=F32)[None, :, None]
        notes = jnp.stack([jnp.max(jnp.where(sent_here, flat[1], -1.0), axis=2), jnp.max(jnp.where(sent_here, flat[2], 0.0), axis=2)])
        notes = hop_y(notes)
        sent_place = notes[0].astype(jnp.int32).reshape(far, 1, units)
        sent_weight = notes[1].reshape(far, 1, units)
        own_groups = ids_loc.T[None] // per_group == (grp ^ jnp.arange(groups))[:, None, None]
        own_member = jnp.any(own_groups, axis=1)
        q_cols = jnp.where(own_member, count_earlier(own_member), -1.0).astype(jnp.int32).T
        slots = experts * cap
        tok_cols = tok_rel.astype(jnp.int32).reshape(devices, slots, 1)
        g_cols = weight_rel.reshape(devices, slots, 1)
        spare = ((0, 0), (0, 0), (0, pad - cap))
        q_rows = jnp.pad(place_rel, spare, constant_values=-1.0).astype(jnp.int32).reshape(devices, 1, experts * pad)
        g_rows = jnp.pad(weight_rel, spare).reshape(devices, 1, experts * pad)
        unit_rows = jnp.pad(unit_rel[:far], spare, constant_values=-1.0).astype(jnp.int32).reshape(far, 1, experts * pad)
        form_rows = jnp.pad(jnp.where(lone_rel, weight_rel, 1.0)[:far], spare).reshape(far, 1, experts * pad)

        xs, acts, ds, dh1s, dh3s, y_sums, dx_sums, y_sent, dx_sent = ([None] * 4 for _ in range(9))
        saved = {}
        last = None
        for step, c in KERNEL_ORDER:
            places = q_rows if last is None else after(last, q_rows)
            if step == 'n':
                xs[c], acts[c], ds[c], dh1s[c], dh3s[c], *sums = near_pair(c, *x_pairs[c], *dy_pairs[c], tok_cols, g_cols, places, g_rows, w1, w3, w2, cap, pad, grp_cap)
                y_sums[c], dx_sums[c] = sums[:PAIR], sums[PAIR:]
            elif step == 'f' and c < 2:
                xs[c], acts[c], *saved[c], y0, y1, r0, r1 = far_forward_pair(c, *x_pairs[c], tok_cols, places, g_rows, unit_rows, form_rows, over_flag, w1, w3, w2, cap, pad, grp_cap, units)
                y_sums[c], y_sent[c] = (y0, y1), (r0, r1)
            elif step == 'b' and c < 2:
                ds[c], dh1s[c], dh3s[c], z0, z1, r0, r1 = far_backward_pair(c, *dy_pairs[c], tok_cols, g_cols, places, unit_rows, over_flag, w1, w3, w2, *saved[c], cap, pad, grp_cap, units)
                dx_sums[c], dx_sent[c] = (z0, z1), (r0, r1)
            elif step == 'f':
                xs[c], acts[c], *saved[c], y0, y1 = forward_pair(c, *x_pairs[c], tok_cols, places, g_rows, w1, w3, w2, cap, pad, grp_cap)
                y_sums[c] = (y0, y1)
            else:
                ds[c], dh1s[c], dh3s[c], *dx_sums[c] = backward_pair(c, *dy_pairs[c], tok_cols, g_cols, places, w1, w3, w2, *saved[c], cap, pad, grp_cap)
            last = (y_sums if step == 'f' else dx_sums)[c][0]

        grads = weight_grads(xs, acts, ds, dh1s, dh3s)

        def combine(results, sent, weighted):
            sums = []
            for pair, near in ((0, 2), (1, 3)):
                arrived = [hop_y(r) for r in sent[pair]]

                def by_rows(ops):
                    return list(merge_pair(pair, ops[0], ops[1], sent_place, sent_weight, weighted))

                def by_sums(ops):
                    return [(n + hop_y(f)).astype(BF) for n, f in zip(ops[0], ops[2])]

                sums += lax.cond(over, by_sums, by_rows, (list(results[near]), arrived, list(results[pair])))
            return [sums[0]] + [hop_g(sums[k], k) for k in (1, 2, 3)]

        y_parts = combine(y_sums, y_sent, True)
        y_out = collect(y_parts, q_cols)
        dx_out = collect(combine(dx_sums, dx_sent, False), q_cols)
        return y_out, dx_out, grads[0], grads[1], grads[2]

    return jax.shard_map(device_fn, mesh=mesh, in_specs=(tok_spec, tok_spec, tok_spec, tok_spec, weight_spec, weight_spec, weight_spec), out_specs=(tok_spec, tok_spec, grad_spec, grad_spec, grad_spec), check_vma=False)
```

```python
import functools

import jax
import jax.numpy as jnp
from jax import lax
from jax.experimental import pallas as pl
from jax.experimental.pallas import tpu as pltpu
from jax.sharding import PartitionSpec as P


BF = jnp.bfloat16
F32 = jnp.float32
ALONE = 1024.0
SENT_SHARE = 7, 8
PAIR = 2

KERNEL_ORDER = (('f', 0), ('b', 0), ('f', 1), ('b', 1), ('n', 2), ('n', 3))


def dot(a, b):
    return lax.dot_general(a, b, (((1,), (0,)), ((), ())), preferred_element_type=F32)


def dot_bt(a, b):
    return lax.dot_general(a, b, (((1,), (1,)), ((), ())), preferred_element_type=F32)


def dot_at(a, b):
    return lax.dot_general(a, b, (((0,), (0,)), ((), ())), preferred_element_type=F32)


def pick_rows(tok_col, rows_ref):
    tokens = rows_ref.shape[0]
    lanes = lax.broadcasted_iota(jnp.int32, (tok_col.shape[0], tokens), 1)
    one_hot = jnp.where(tok_col == lanes, 1.0, 0.0).astype(BF)
    return dot(one_hot, rows_ref[...])


def store_by_expert(dst_ref, rows, cap):
    for e in range(dst_ref.shape[0]):
        dst_ref[e] = jnp.concatenate([r[e * cap:(e + 1) * cap] for r in rows], axis=0).astype(BF)


def keep_rows(dst_ref, rows, e, cap, pad):
    zeros = jnp.zeros((pad - cap, rows.shape[1]), F32)
    for s in range(PAIR):
        padded = jnp.concatenate([rows[s * cap:(s + 1) * cap], zeros], axis=0).astype(BF)
        dst_ref[s, pl.ds(pl.multiple_of(e * pad, pad), pad), :] = padded


def spread_rows(dst_ref, tok_ref, row_refs, cap, gcol_ref=None):
    picked = [pick_rows(tok_ref[s], r) for s, r in enumerate(row_refs)]
    if gcol_ref is not None:
        picked = [gcol_ref[s] * p for s, p in enumerate(picked)]
    store_by_expert(dst_ref, picked, cap)


def forward_expert(xg, w1_ref, w3_ref):
    h1 = dot(xg, w1_ref[0])
    h3 = dot(xg, w3_ref[0])
    sig = jax.nn.sigmoid(h1)
    silu = h1 * sig
    act = (silu * h3).astype(BF)
    return act, h3 * (sig * (1.0 + h1 * (1.0 - sig))), silu


def weighted_rows(hit, weight, rows):
    if weight is None:
        return dot(jnp.where(hit, 1.0, 0.0).astype(BF), rows)
    rest, total = weight, None
    for _ in range(3):
        part = rest.astype(BF)
        term = dot(jnp.where(hit, part.astype(F32), 0.0).astype(BF), rows)
        total = term if total is None else total + term
        rest = rest - part.astype(F32)
    return total


def group_sums(p_refs, q_ref, rows_scr, g_ref=None):
    for s, p_ref in enumerate(p_refs):
        slots = lax.broadcasted_iota(jnp.int32, (p_ref.shape[0], q_ref.shape[2]), 0)
        p_ref[...] = weighted_rows(q_ref[s] == slots, None if g_ref is None else g_ref[s], rows_scr[s])


def fwd_kernel(cap, pad, xa_ref, xb_ref, tok_ref, q_ref, g_ref, w1_ref, w3_ref, w2_ref, xg_ref, a_ref, u_ref, v_ref, p0_ref, p1_ref, xg_scr, o_scr):
    e = pl.program_id(0)

    @pl.when(e == 0)
    def _():
        spread_rows(xg_scr, tok_ref, (xa_ref, xb_ref), cap)

    xg_ref[0] = xg_scr[e]
    act, u_ref[0], v_ref[0] = forward_expert(xg_scr[e], w1_ref, w3_ref)
    a_ref[0] = act
    keep_rows(o_scr, dot(act, w2_ref[0]), e, cap, pad)

    @pl.when(e == pl.num_programs(0) - 1)
    def _():
        group_sums((p0_ref, p1_ref), q_ref, o_scr, g_ref)


def bwd_kernel(cap, pad, dya_ref, dyb_ref, tok_ref, gcol_ref, q_ref, w1_ref, w3_ref, w2_ref, u_ref, v_ref, d_ref, dh1_ref, dh3_ref, p0_ref, p1_ref, d_scr, r_scr):
    e = pl.program_id(0)

    @pl.when(e == 0)
    def _():
        spread_rows(d_scr, tok_ref, (dya_ref, dyb_ref), cap, gcol_ref)

    d_ref[0] = d_scr[e]
    da = dot_bt(d_scr[e], w2_ref[0])
    dh1 = (da * u_ref[0]).astype(BF)
    dh3 = (da * v_ref[0]).astype(BF)
    dh1_ref[0] = dh1
    dh3_ref[0] = dh3
    keep_rows(r_scr, dot_bt(dh1, w1_ref[0]) + dot_bt(dh3, w3_ref[0]), e, cap, pad)

    @pl.when(e == pl.num_programs(0) - 1)
    def _():
        group_sums((p0_ref, p1_ref), q_ref, r_scr)


def unit_rows(u_refs, unit_ref, rows_scr, weight_ref=None):
    for s, u_ref in enumerate(u_refs):
        units = lax.broadcasted_iota(jnp.int32, (u_ref.shape[0], unit_ref.shape[2]), 0)
        u_ref[...] = weighted_rows(unit_ref[s] == units, None if weight_ref is None else weight_ref[s], rows_scr[s]).astype(BF)


def far_fwd_kernel(cap, pad, xa_ref, xb_ref, tok_ref, q_ref, g_ref, unit_ref, form_ref, over_ref, w1_ref, w3_ref, w2_ref, xg_ref, a_ref, u_ref, v_ref, p0_ref, p1_ref, r0_ref, r1_ref, xg_scr, o_scr):
    e = pl.program_id(0)

    @pl.when(e == 0)
    def _():
        spread_rows(xg_scr, tok_ref, (xa_ref, xb_ref), cap)

    xg_ref[0] = xg_scr[e]
    act, u_ref[0], v_ref[0] = forward_expert(xg_scr[e], w1_ref, w3_ref)
    a_ref[0] = act
    keep_rows(o_scr, dot(act, w2_ref[0]), e, cap, pad)
    done = e == pl.num_programs(0) - 1

    @pl.when(done & (over_ref[0] == 0))
    def _():
        unit_rows((r0_ref, r1_ref), unit_ref, o_scr, form_ref)

    @pl.when(done & (over_ref[0] != 0))
    def _():
        group_sums((p0_ref, p1_ref), q_ref, o_scr, g_ref)


def far_bwd_kernel(cap, pad, dya_ref, dyb_ref, tok_ref, gcol_ref, q_ref, unit_ref, over_ref, w1_ref, w3_ref, w2_ref, u_ref, v_ref, d_ref, dh1_ref, dh3_ref, p0_ref, p1_ref, r0_ref, r1_ref, d_scr, r_scr):
    e = pl.program_id(0)

    @pl.when(e == 0)
    def _():
        spread_rows(d_scr, tok_ref, (dya_ref, dyb_ref), cap, gcol_ref)

    d_ref[0] = d_scr[e]
    da = dot_bt(d_scr[e], w2_ref[0])
    dh1 = (da * u_ref[0]).astype(BF)
    dh3 = (da * v_ref[0]).astype(BF)
    dh1_ref[0] = dh1
    dh3_ref[0] = dh3
    keep_rows(r_scr, dot_bt(dh1, w1_ref[0]) + dot_bt(dh3, w3_ref[0]), e, cap, pad)
    done = e == pl.num_programs(0) - 1

    @pl.when(done & (over_ref[0] == 0))
    def _():
        unit_rows((r0_ref, r1_ref), unit_ref, r_scr)

    @pl.when(done & (over_ref[0] != 0))
    def _():
        group_sums((p0_ref, p1_ref), q_ref, r_scr)


def merge_kernel(weighted, n0_ref, n1_ref, r0_ref, r1_ref, place_ref, weight_ref, p0_ref, p1_ref):
    for s, (n_ref, r_ref, p_ref) in enumerate(((n0_ref, r0_ref, p0_ref), (n1_ref, r1_ref, p1_ref))):
        places = lax.broadcasted_iota(jnp.int32, (n_ref.shape[0], r_ref.shape[0]), 0)
        total = weighted_rows(place_ref[s] == places, weight_ref[s] if weighted else None, r_ref[...])
        p_ref[...] = (n_ref[...] + total).astype(BF)


def near_kernel(cap, pad, xa_ref, xb_ref, dya_ref, dyb_ref, tok_ref, gcol_ref, q_ref, g_ref, w1_ref, w3_ref, w2_ref, xg_ref, a_ref, d_ref, dh1_ref, dh3_ref, y0_ref, y1_ref, z0_ref, z1_ref, xg_scr, d_scr, o_scr, r_scr):
    e = pl.program_id(0)

    @pl.when(e == 0)
    def _():
        spread_rows(xg_scr, tok_ref, (xa_ref, xb_ref), cap)
        spread_rows(d_scr, tok_ref, (dya_ref, dyb_ref), cap, gcol_ref)

    xg_ref[0] = xg_scr[e]
    d_ref[0] = d_scr[e]
    act, u, v = forward_expert(xg_scr[e], w1_ref, w3_ref)
    a_ref[0] = act
    keep_rows(o_scr, dot(act, w2_ref[0]), e, cap, pad)
    da = dot_bt(d_scr[e], w2_ref[0])
    dh1 = (da * u).astype(BF)
    dh3 = (da * v).astype(BF)
    dh1_ref[0] = dh1
    dh3_ref[0] = dh3
    keep_rows(r_scr, dot_bt(dh1, w1_ref[0]) + dot_bt(dh3, w3_ref[0]), e, cap, pad)

    @pl.when(e == pl.num_programs(0) - 1)
    def _():
        group_sums((y0_ref, y1_ref), q_ref, o_scr, g_ref)
        group_sums((z0_ref, z1_ref), q_ref, r_scr)


def whole(shape):
    return pl.BlockSpec(shape, lambda e: (0,) * len(shape))


def per_expert(shape):
    return pl.BlockSpec((1,) + shape[1:], lambda e: (e,) + (0,) * (len(shape) - 1))


def once(shape):
    return pl.BlockSpec(shape, lambda e: (0,) * len(shape), pipeline_mode=pl.Buffered(1))


def of_pair(pair, shape):
    return pl.BlockSpec((PAIR,) + shape[1:], lambda e: (pair,) + (0,) * (len(shape) - 1))


def params():
    return pltpu.CompilerParams(dimension_semantics=("arbitrary",), vmem_limit_bytes=60 * 1024 * 1024)


def forward_pair(pair, xa, xb, tok_col, q_row, g_row, w1, w3, w2, cap, pad, grp_cap):
    experts, hidden, ff = w1.shape
    rows = PAIR * cap
    outs = [((experts, rows, hidden), BF), ((experts, rows, ff), BF), ((experts, rows, ff), F32), ((experts, rows, ff), F32), ((grp_cap, hidden), F32), ((grp_cap, hidden), F32)]
    return pl.pallas_call(
        functools.partial(fwd_kernel, cap, pad),
        grid=(experts,),
        in_specs=[whole(xa.shape), whole(xb.shape), of_pair(pair, tok_col.shape), of_pair(pair, q_row.shape), of_pair(pair, g_row.shape), per_expert(w1.shape), per_expert(w3.shape), per_expert(w2.shape)],
        out_specs=[per_expert(s) if len(s) == 3 else whole(s) for s, _ in outs],
        out_shape=[jax.ShapeDtypeStruct(s, t) for s, t in outs],
        scratch_shapes=[pltpu.VMEM((experts, rows, hidden), BF), pltpu.VMEM((PAIR, experts * pad, hidden), BF)],
        compiler_params=params(),
        cost_estimate=pl.CostEstimate(flops=14 * 10**9, bytes_accessed=50 * 10**6, transcendentals=0),
        name="fwd_pair",
    )(xa, xb, tok_col, q_row, g_row, w1, w3, w2)


def backward_pair(pair, dya, dyb, tok_col, g_col, q_row, w1, w3, w2, u, v, cap, pad, grp_cap):
    experts, hidden, ff = w1.shape
    rows = PAIR * cap
    outs = [((experts, rows, hidden), BF), ((experts, rows, ff), BF), ((experts, rows, ff), BF), ((grp_cap, hidden), F32), ((grp_cap, hidden), F32)]
    return pl.pallas_call(
        functools.partial(bwd_kernel, cap, pad),
        grid=(experts,),
        in_specs=[whole(dya.shape), whole(dyb.shape), of_pair(pair, tok_col.shape), of_pair(pair, g_col.shape), of_pair(pair, q_row.shape), per_expert(w1.shape), per_expert(w3.shape), per_expert(w2.shape), per_expert(u.shape), per_expert(v.shape)],
        out_specs=[per_expert(s) if len(s) == 3 else whole(s) for s, _ in outs],
        out_shape=[jax.ShapeDtypeStruct(s, t) for s, t in outs],
        scratch_shapes=[pltpu.VMEM((experts, rows, hidden), BF), pltpu.VMEM((PAIR, experts * pad, hidden), BF)],
        compiler_params=params(),
        cost_estimate=pl.CostEstimate(flops=14 * 10**9, bytes_accessed=50 * 10**6, transcendentals=0),
        name="bwd_pair",
    )(dya, dyb, tok_col, g_col, q_row, w1, w3, w2, u, v)


def flag():
    return pl.BlockSpec(memory_space=pltpu.SMEM)


def far_forward_pair(pair, xa, xb, tok_col, q_row, g_row, unit_row, form_row, over, w1, w3, w2, cap, pad, grp_cap, units):
    experts, hidden, ff = w1.shape
    rows = PAIR * cap
    part, sent = ((grp_cap, hidden), F32), ((units, hidden), BF)
    outs = [((experts, rows, hidden), BF), ((experts, rows, ff), BF), ((experts, rows, ff), F32), ((experts, rows, ff), F32), part, part, sent, sent]
    tables = [tok_col, q_row, g_row, unit_row, form_row]
    return pl.pallas_call(
        functools.partial(far_fwd_kernel, cap, pad),
        grid=(experts,),
        in_specs=[whole(xa.shape), whole(xb.shape)] + [of_pair(pair, t.shape) for t in tables] + [flag(), per_expert(w1.shape), per_expert(w3.shape), per_expert(w2.shape)],
        out_specs=[per_expert(s) if len(s) == 3 else whole(s) for s, _ in outs],
        out_shape=[jax.ShapeDtypeStruct(s, t) for s, t in outs],
        scratch_shapes=[pltpu.VMEM((experts, rows, hidden), BF), pltpu.VMEM((PAIR, experts * pad, hidden), BF)],
        compiler_params=params(),
        cost_estimate=pl.CostEstimate(flops=14 * 10**9, bytes_accessed=50 * 10**6, transcendentals=0),
        name="far_fwd_pair",
    )(xa, xb, *tables, over, w1, w3, w2)


def far_backward_pair(pair, dya, dyb, tok_col, g_col, q_row, unit_row, over, w1, w3, w2, u, v, cap, pad, grp_cap, units):
    experts, hidden, ff = w1.shape
    rows = PAIR * cap
    part, sent = ((grp_cap, hidden), F32), ((units, hidden), BF)
    outs = [((experts, rows, hidden), BF), ((experts, rows, ff), BF), ((experts, rows, ff), BF), part, part, sent, sent]
    tables = [tok_col, g_col, q_row, unit_row]
    return pl.pallas_call(
        functools.partial(far_bwd_kernel, cap, pad),
        grid=(experts,),
        in_specs=[whole(dya.shape), whole(dyb.shape)] + [of_pair(pair, t.shape) for t in tables] + [flag(), per_expert(w1.shape), per_expert(w3.shape), per_expert(w2.shape), per_expert(u.shape), per_expert(v.shape)],
        out_specs=[per_expert(s) if len(s) == 3 else whole(s) for s, _ in outs],
        out_shape=[jax.ShapeDtypeStruct(s, t) for s, t in outs],
        scratch_shapes=[pltpu.VMEM((experts, rows, hidden), BF), pltpu.VMEM((PAIR, experts * pad, hidden), BF)],
        compiler_params=params(),
        cost_estimate=pl.CostEstimate(flops=14 * 10**9, bytes_accessed=50 * 10**6, transcendentals=0),
        name="far_bwd_pair",
    )(dya, dyb, *tables, over, w1, w3, w2, u, v)


def merge_pair(pair, near, sent, place, weight, weighted):
    grp_cap, hidden = near[0].shape
    units = sent[0].shape[0]
    block = hidden // 3
    return pl.pallas_call(
        functools.partial(merge_kernel, weighted),
        grid=(3,),
        in_specs=[pl.BlockSpec((grp_cap, block), lambda n: (0, n))] * 2 + [pl.BlockSpec((units, block), lambda n: (0, n))] * 2 + [of_pair(pair, place.shape), of_pair(pair, weight.shape)],
        out_specs=[pl.BlockSpec((grp_cap, block), lambda n: (0, n))] * 2,
        out_shape=[jax.ShapeDtypeStruct((grp_cap, hidden), BF)] * 2,
        compiler_params=params(),
        cost_estimate=pl.CostEstimate(flops=2 * 10**9, bytes_accessed=8 * 10**6, transcendentals=0),
        name="merge_pair",
    )(*near, *sent, place, weight)


def near_pair(pair, xa, xb, dya, dyb, tok_col, g_col, q_row, g_row, w1, w3, w2, cap, pad, grp_cap):
    experts, hidden, ff = w1.shape
    rows = PAIR * cap
    wide, narrow, part = ((experts, rows, hidden), BF), ((experts, rows, ff), BF), ((grp_cap, hidden), F32)
    outs = [wide, narrow, wide, narrow, narrow, part, part, part, part]
    tables = [tok_col, g_col, q_row, g_row]
    return pl.pallas_call(
        functools.partial(near_kernel, cap, pad),
        grid=(experts,),
        in_specs=[once(xa.shape)] * 4 + [of_pair(pair, t.shape) for t in tables] + [per_expert(w1.shape), per_expert(w3.shape), per_expert(w2.shape)],
        out_specs=[per_expert(s) if len(s) == 3 else whole(s) for s, _ in outs],
        out_shape=[jax.ShapeDtypeStruct(s, t) for s, t in outs],
        scratch_shapes=[pltpu.VMEM((experts, rows, hidden), BF)] * 2 + [pltpu.VMEM((PAIR, experts * pad, hidden), BF)] * 2,
        compiler_params=params(),
        cost_estimate=pl.CostEstimate(flops=28 * 10**9, bytes_accessed=70 * 10**6, transcendentals=0),
        name="near_pair",
    )(xa, xb, dya, dyb, *tables, w1, w3, w2)


def dw_kernel(chunks, *refs):
    ins, (g1_ref, g3_ref, g2_ref) = refs[:5 * chunks], refs[5 * chunks:]

    def joined(k):
        return jnp.concatenate([ins[k * chunks + c][0] for c in range(chunks)], axis=0)

    x, a, d, dh1, dh3 = (joined(k) for k in range(5))
    g1_ref[0] = dot_at(x, dh1)
    g3_ref[0] = dot_at(x, dh3)
    g2_ref[0] = dot_at(a, d)


def weight_grads(xs, acts, ds, dh1s, dh3s):
    chunks = len(xs)
    experts, _, hidden = xs[0].shape
    ff = acts[0].shape[2]
    args = [*xs, *acts, *ds, *dh1s, *dh3s]
    outs = [(experts, hidden, ff), (experts, hidden, ff), (experts, ff, hidden)]
    return pl.pallas_call(
        functools.partial(dw_kernel, chunks),
        grid=(experts,),
        in_specs=[per_expert(a.shape) for a in args],
        out_specs=[per_expert(s) for s in outs],
        out_shape=[jax.ShapeDtypeStruct(s, F32) for s in outs],
        compiler_params=params(),
        cost_estimate=pl.CostEstimate(flops=25 * 10**9, bytes_accessed=120 * 10**6, transcendentals=0),
        name="weight_grads",
    )(*args)


def final_kernel(groups, *refs):
    q_ref, out_ref = refs[groups], refs[groups + 1]
    total = None
    for h in range(groups):
        lanes = lax.broadcasted_iota(jnp.int32, (out_ref.shape[0], refs[h].shape[0]), 1)
        one_hot = jnp.where(q_ref[:, h:h + 1] == lanes, 1.0, 0.0).astype(BF)
        term = dot(one_hot, refs[h][...])
        total = term if total is None else total + term
    out_ref[...] = total.astype(BF)


def collect(parts, q_cols):
    groups = len(parts)
    tokens = q_cols.shape[0]
    hidden = parts[0].shape[1]
    block = tokens // 4
    return pl.pallas_call(
        functools.partial(final_kernel, groups),
        grid=(4,),
        in_specs=[whole(p.shape) for p in parts] + [pl.BlockSpec((block, groups), lambda e: (e, 0))],
        out_specs=pl.BlockSpec((block, hidden), lambda e: (e, 0)),
        out_shape=jax.ShapeDtypeStruct((tokens, hidden), BF),
        compiler_params=params(),
        cost_estimate=pl.CostEstimate(flops=2 * 10**9, bytes_accessed=5 * 10**6, transcendentals=0),
        name="collect",
    )(*parts, q_cols)


def after(earlier, value):
    return lax.optimization_barrier((earlier, value))[1]


def slot_tables(ids, gates, first_exp, experts, group, per_group, cap):
    sources, _, tokens = ids.shape
    eq = ids[:, None] == (first_exp + jnp.arange(experts))[None, :, None, None]
    hit = jnp.any(eq, axis=2)
    gate = jnp.sum(jnp.where(eq, gates[:, None], 0.0), axis=2)
    member = jnp.any(ids // per_group == group, axis=1, keepdims=True)
    pos = count_earlier(jnp.concatenate([hit, member], axis=1).reshape(sources * (experts + 1), tokens))
    pos = pos.reshape(sources, experts + 1, tokens)
    exp_pos, grp_pos = pos[:, :experts], pos[:, experts:]
    taken = hit[:, :, None, :] & (exp_pos[:, :, None, :] == jnp.arange(cap, dtype=F32)[None, None, :, None])
    numbers = jnp.arange(1, tokens + 1, dtype=F32)[None, None, None, :]
    tok = jnp.sum(jnp.where(taken, numbers, 0.0), axis=3) - 1.0
    place = jnp.sum(jnp.where(taken, grp_pos[:, :, None, :] + 1.0, 0.0), axis=3) - 1.0
    weight = jnp.sum(jnp.where(taken, gate[:, :, None, :], 0.0), axis=3)
    here = jnp.sum(hit, axis=1).astype(F32)
    alone = here == jnp.sum(ids // per_group == group, axis=1).astype(F32)
    first = count_earlier(jnp.where(alone, jnp.minimum(here, 1.0), here))
    rank, seen = [], jnp.zeros((sources, tokens), F32)
    for e in range(experts):
        rank.append(seen)
        seen = seen + hit[:, e].astype(F32)
    unit = first[:, None] + jnp.where(alone[:, None], ALONE, jnp.stack(rank, axis=1)) + 1.0
    code = jnp.sum(jnp.where(taken, unit[:, :, None, :], 0.0), axis=3)
    lone = code > ALONE
    return tok, place, weight, jnp.where(lone, code - ALONE, code) - 1.0, lone


def longest_list(ids, per_group, experts, away):
    devices = away.shape[1]
    count = jnp.sum(ids[:, None] // experts == jnp.arange(devices)[None, :, None, None], axis=2)
    half = per_group // experts
    in_group = jnp.repeat(jnp.sum(count.reshape(ids.shape[0], devices // half, half, -1), axis=2), half, axis=1)
    rows = jnp.where(count == in_group, jnp.minimum(count, 1), count)
    return jnp.max(jnp.where(away, jnp.sum(rows, axis=2), 0))


def count_earlier(marks):
    tokens = marks.shape[1]
    earlier = (jnp.arange(tokens)[:, None] < jnp.arange(tokens)[None, :]).astype(BF)
    return jnp.dot(marks.astype(BF), earlier, preferred_element_type=F32)


def solution(mesh):
    groups = mesh.shape['grp']
    inner = mesh.shape['ing']
    devices = groups * inner
    tok_spec = P(('dp', 'grp', 'ing'), None)
    weight_spec = P(('grp', 'ing'), None, None)
    grad_spec = P(('dp', 'grp', 'ing'), None, None)

    def hop_y(a):
        return lax.ppermute(a, 'ing', [(0, 1), (1, 0)])

    def hop_g(a, bits):
        return lax.ppermute(a, 'grp', [(g, g ^ bits) for g in range(groups)])

    def device_fn(x_loc, ids_loc, gates_loc, dy_loc, w1, w3, w2):
        tokens, _ = x_loc.shape
        top_k = ids_loc.shape[1]
        experts = w1.shape[0]
        num_exp = experts * devices
        grp_cap = tokens * 2 // groups
        cap = 3 * tokens * top_k // (2 * num_exp)
        pad = -(-cap // 16) * 16
        grp, ing = lax.axis_index('grp'), lax.axis_index('ing')

        per_group = experts * inner
        own = jnp.concatenate([ids_loc.T.astype(F32), gates_loc.T], axis=0)[None]
        pair = jnp.concatenate([own, hop_y(own)], axis=0)
        pair_c = hop_g(pair, 1)
        quad_x = hop_g(jnp.concatenate([pair, pair_c], axis=0), 2)
        routing = jnp.stack([pair[1], pair_c[1], quad_x[1], quad_x[3], pair[0], pair_c[0], quad_x[0], quad_x[2]])

        x_far = hop_y(x_loc)
        dy_far = hop_y(dy_loc)
        x_near_c = hop_g(after(pair_c, x_loc), 1)
        x_near_x = hop_g(x_loc, 2)
        dy_near_c = hop_g(after(x_near_c, dy_loc), 1)
        x_far_c, x_far_x = hop_g(x_far, 1), hop_g(x_far, 2)
        x_near_xc, x_far_xc = hop_g(x_near_x, 1), hop_g(x_far_x, 1)
        dy_far_c, dy_far_x = hop_g(dy_far, 1), hop_g(dy_far, 2)
        dy_far_xc = hop_g(dy_far_x, 1)
        dy_near_x = hop_g(dy_loc, 2)
        dy_near_xc = hop_g(dy_near_x, 1)
        x_pairs = [(x_far, x_far_c), (x_far_x, x_far_xc), (x_loc, x_near_c), (x_near_x, x_near_xc)]
        dy_pairs = [(dy_far, dy_far_c), (dy_far_x, dy_far_xc), (dy_loc, dy_near_c), (dy_near_x, dy_near_xc)]

        ids_rel, gates_rel = routing[:, :top_k].astype(jnp.int32), routing[:, top_k:]
        units = tokens * SENT_SHARE[0] // SENT_SHARE[1]
        tok_rel, place_rel, weight_rel, unit_rel, lone_rel = slot_tables(ids_rel, gates_rel, (grp * inner + ing) * experts, experts, grp, per_group, cap)
        far = devices // 2
        source_ing = jnp.where(jnp.arange(devices) < far, 1 - ing, ing)
        away = source_ing[:, None] != (jnp.arange(devices) % inner)[None, :]
        over = longest_list(ids_rel, per_group, experts, away) > units
        over_flag = over.astype(jnp.int32).reshape(1)
        flat = [t[:far].reshape(far, 1, -1) for t in (unit_rel, place_rel, jnp.where(lone_rel, 1.0, weight_rel))]
        sent_here = flat[0] == jnp.arange(units, dtype=F32)[None, :, None]
        notes = jnp.stack([jnp.max(jnp.where(sent_here, flat[1], -1.0), axis=2), jnp.max(jnp.where(sent_here, flat[2], 0.0), axis=2)])
        notes = hop_y(notes)
        sent_place = notes[0].astype(jnp.int32).reshape(far, 1, units)
        sent_weight = notes[1].reshape(far, 1, units)
        own_groups = ids_loc.T[None] // per_group == (grp ^ jnp.arange(groups))[:, None, None]
        own_member = jnp.any(own_groups, axis=1)
        q_cols = jnp.where(own_member, count_earlier(own_member), -1.0).astype(jnp.int32).T
        slots = experts * cap
        tok_cols = tok_rel.astype(jnp.int32).reshape(devices, slots, 1)
        g_cols = weight_rel.reshape(devices, slots, 1)
        spare = ((0, 0), (0, 0), (0, pad - cap))
        q_rows = jnp.pad(place_rel, spare, constant_values=-1.0).astype(jnp.int32).reshape(devices, 1, experts * pad)
        g_rows = jnp.pad(weight_rel, spare).reshape(devices, 1, experts * pad)
        unit_rows = jnp.pad(unit_rel[:far], spare, constant_values=-1.0).astype(jnp.int32).reshape(far, 1, experts * pad)
        form_rows = jnp.pad(jnp.where(lone_rel, weight_rel, 1.0)[:far], spare).reshape(far, 1, experts * pad)

        xs, acts, ds, dh1s, dh3s, y_sums, dx_sums, y_sent, dx_sent = ([None] * 4 for _ in range(9))
        saved = {}
        last = None
        for step, c in KERNEL_ORDER:
            places = q_rows if last is None else after(last, q_rows)
            if step == 'n':
                xs[c], acts[c], ds[c], dh1s[c], dh3s[c], *sums = near_pair(c, *x_pairs[c], *dy_pairs[c], tok_cols, g_cols, places, g_rows, w1, w3, w2, cap, pad, grp_cap)
                y_sums[c], dx_sums[c] = sums[:PAIR], sums[PAIR:]
            elif step == 'f' and c < 2:
                xs[c], acts[c], *saved[c], y0, y1, r0, r1 = far_forward_pair(c, *x_pairs[c], tok_cols, places, g_rows, unit_rows, form_rows, over_flag, w1, w3, w2, cap, pad, grp_cap, units)
                y_sums[c], y_sent[c] = (y0, y1), (r0, r1)
            elif step == 'b' and c < 2:
                ds[c], dh1s[c], dh3s[c], z0, z1, r0, r1 = far_backward_pair(c, *dy_pairs[c], tok_cols, g_cols, places, unit_rows, over_flag, w1, w3, w2, *saved[c], cap, pad, grp_cap, units)
                dx_sums[c], dx_sent[c] = (z0, z1), (r0, r1)
            elif step == 'f':
                xs[c], acts[c], *saved[c], y0, y1 = forward_pair(c, *x_pairs[c], tok_cols, places, g_rows, w1, w3, w2, cap, pad, grp_cap)
                y_sums[c] = (y0, y1)
            else:
                ds[c], dh1s[c], dh3s[c], *dx_sums[c] = backward_pair(c, *dy_pairs[c], tok_cols, g_cols, places, w1, w3, w2, *saved[c], cap, pad, grp_cap)
            last = (y_sums if step == 'f' else dx_sums)[c][0]

        grads = weight_grads(xs, acts, ds, dh1s, dh3s)

        def combine(results, sent, weighted):
            sums = []
            for pair, near in ((0, 2), (1, 3)):
                arrived = [hop_y(r) for r in sent[pair]]

                def by_rows(ops):
                    return list(merge_pair(pair, ops[0], ops[1], sent_place, sent_weight, weighted))

                def by_sums(ops):
                    return [(n + hop_y(f)).astype(BF) for n, f in zip(ops[0], ops[2])]

                sums += lax.cond(over, by_sums, by_rows, (list(results[near]), arrived, list(results[pair])))
            return [sums[0]] + [hop_g(sums[k], k) for k in (1, 2, 3)]

        y_parts = combine(y_sums, y_sent, True)
        y_out = collect(y_parts, q_cols)
        dx_out = collect(combine(dx_sums, dx_sent, False), q_cols)
        return y_out, dx_out, grads[0], grads[1], grads[2]

    return jax.shard_map(device_fn, mesh=mesh, in_specs=(tok_spec, tok_spec, tok_spec, tok_spec, weight_spec, weight_spec, weight_spec), out_specs=(tok_spec, tok_spec, grad_spec, grad_spec, grad_spec), check_vma=False)
```

```python
import functools

import jax
import jax.numpy as jnp
from jax import lax
from jax.experimental import pallas as pl
from jax.experimental.pallas import tpu as pltpu
from jax.sharding import PartitionSpec as P


BF = jnp.bfloat16
F32 = jnp.float32
ALONE = 1024.0
SENT_SHARE = 7, 8
PAIR = 2

KERNEL_ORDER = (('f', 0), ('b', 0), ('m', 1), ('n', 2), ('n', 3))


def dot(a, b):
    return lax.dot_general(a, b, (((1,), (0,)), ((), ())), preferred_element_type=F32)


def dot_bt(a, b):
    return lax.dot_general(a, b, (((1,), (1,)), ((), ())), preferred_element_type=F32)


def dot_at(a, b):
    return lax.dot_general(a, b, (((0,), (0,)), ((), ())), preferred_element_type=F32)


def pick_rows(tok_col, rows_ref):
    tokens = rows_ref.shape[0]
    lanes = lax.broadcasted_iota(jnp.int32, (tok_col.shape[0], tokens), 1)
    one_hot = jnp.where(tok_col == lanes, 1.0, 0.0).astype(BF)
    return dot(one_hot, rows_ref[...])


def store_by_expert(dst_ref, rows, cap):
    for e in range(dst_ref.shape[0]):
        dst_ref[e] = jnp.concatenate([r[e * cap:(e + 1) * cap] for r in rows], axis=0).astype(BF)


def keep_rows(dst_ref, rows, e, cap, pad):
    zeros = jnp.zeros((pad - cap, rows.shape[1]), F32)
    for s in range(PAIR):
        padded = jnp.concatenate([rows[s * cap:(s + 1) * cap], zeros], axis=0).astype(BF)
        dst_ref[s, pl.ds(pl.multiple_of(e * pad, pad), pad), :] = padded


def spread_rows(dst_ref, tok_ref, row_refs, cap, gcol_ref=None):
    picked = [pick_rows(tok_ref[s], r) for s, r in enumerate(row_refs)]
    if gcol_ref is not None:
        picked = [gcol_ref[s] * p for s, p in enumerate(picked)]
    store_by_expert(dst_ref, picked, cap)


def forward_expert(xg, w1_ref, w3_ref):
    h1 = dot(xg, w1_ref[0])
    h3 = dot(xg, w3_ref[0])
    sig = jax.nn.sigmoid(h1)
    silu = h1 * sig
    act = (silu * h3).astype(BF)
    return act, h3 * (sig * (1.0 + h1 * (1.0 - sig))), silu


def weighted_rows(hit, weight, rows):
    if weight is None:
        return dot(jnp.where(hit, 1.0, 0.0).astype(BF), rows)
    rest, total = weight, None
    for _ in range(3):
        part = rest.astype(BF)
        term = dot(jnp.where(hit, part.astype(F32), 0.0).astype(BF), rows)
        total = term if total is None else total + term
        rest = rest - part.astype(F32)
    return total


def group_sums(p_refs, q_ref, rows_scr, g_ref=None):
    for s, p_ref in enumerate(p_refs):
        slots = lax.broadcasted_iota(jnp.int32, (p_ref.shape[0], q_ref.shape[2]), 0)
        p_ref[...] = weighted_rows(q_ref[s] == slots, None if g_ref is None else g_ref[s], rows_scr[s])


def unit_rows(u_refs, unit_ref, rows_scr, weight_ref=None):
    for s, u_ref in enumerate(u_refs):
        units = lax.broadcasted_iota(jnp.int32, (u_ref.shape[0], unit_ref.shape[2]), 0)
        u_ref[...] = weighted_rows(unit_ref[s] == units, None if weight_ref is None else weight_ref[s], rows_scr[s]).astype(BF)


def far_fwd_kernel(cap, pad, xa_ref, xb_ref, tok_ref, q_ref, g_ref, unit_ref, form_ref, over_ref, w1_ref, w3_ref, w2_ref, xg_ref, a_ref, u_ref, v_ref, p0_ref, p1_ref, r0_ref, r1_ref, xg_scr, o_scr):
    e = pl.program_id(0)

    @pl.when(e == 0)
    def _():
        spread_rows(xg_scr, tok_ref, (xa_ref, xb_ref), cap)

    xg_ref[0] = xg_scr[e]
    act, u_ref[0], v_ref[0] = forward_expert(xg_scr[e], w1_ref, w3_ref)
    a_ref[0] = act
    keep_rows(o_scr, dot(act, w2_ref[0]), e, cap, pad)
    done = e == pl.num_programs(0) - 1

    @pl.when(done & (over_ref[0] == 0))
    def _():
        unit_rows((r0_ref, r1_ref), unit_ref, o_scr, form_ref)

    @pl.when(done & (over_ref[0] != 0))
    def _():
        group_sums((p0_ref, p1_ref), q_ref, o_scr, g_ref)


def far_bwd_kernel(cap, pad, dya_ref, dyb_ref, tok_ref, gcol_ref, q_ref, unit_ref, over_ref, w1_ref, w3_ref, w2_ref, u_ref, v_ref, d_ref, dh1_ref, dh3_ref, p0_ref, p1_ref, r0_ref, r1_ref, d_scr, r_scr):
    e = pl.program_id(0)

    @pl.when(e == 0)
    def _():
        spread_rows(d_scr, tok_ref, (dya_ref, dyb_ref), cap, gcol_ref)

    d_ref[0] = d_scr[e]
    da = dot_bt(d_scr[e], w2_ref[0])
    dh1 = (da * u_ref[0]).astype(BF)
    dh3 = (da * v_ref[0]).astype(BF)
    dh1_ref[0] = dh1
    dh3_ref[0] = dh3
    keep_rows(r_scr, dot_bt(dh1, w1_ref[0]) + dot_bt(dh3, w3_ref[0]), e, cap, pad)
    done = e == pl.num_programs(0) - 1

    @pl.when(done & (over_ref[0] == 0))
    def _():
        unit_rows((r0_ref, r1_ref), unit_ref, r_scr)

    @pl.when(done & (over_ref[0] != 0))
    def _():
        group_sums((p0_ref, p1_ref), q_ref, r_scr)


def merge_kernel(weighted, count, *refs):
    near, sent, places, weights, outs = (refs[k * count:(k + 1) * count] for k in range(5))
    for n_ref, r_ref, place_ref, weight_ref, p_ref in zip(near, sent, places, weights, outs):
        slots = lax.broadcasted_iota(jnp.int32, (n_ref.shape[0], r_ref.shape[0]), 0)
        total = weighted_rows(place_ref[0] == slots, weight_ref[0] if weighted else None, r_ref[...])
        p_ref[...] = (n_ref[...] + total).astype(BF)


def both_ways(cap, pad, e, w1_ref, w3_ref, w2_ref, xg_ref, a_ref, d_ref, dh1_ref, dh3_ref, xg_scr, d_scr, o_scr, r_scr):
    xg_ref[0] = xg_scr[e]
    d_ref[0] = d_scr[e]
    act, u, v = forward_expert(xg_scr[e], w1_ref, w3_ref)
    a_ref[0] = act
    keep_rows(o_scr, dot(act, w2_ref[0]), e, cap, pad)
    da = dot_bt(d_scr[e], w2_ref[0])
    dh1 = (da * u).astype(BF)
    dh3 = (da * v).astype(BF)
    dh1_ref[0] = dh1
    dh3_ref[0] = dh3
    keep_rows(r_scr, dot_bt(dh1, w1_ref[0]) + dot_bt(dh3, w3_ref[0]), e, cap, pad)


def near_kernel(cap, pad, xa_ref, xb_ref, dya_ref, dyb_ref, tok_ref, gcol_ref, q_ref, g_ref, w1_ref, w3_ref, w2_ref, xg_ref, a_ref, d_ref, dh1_ref, dh3_ref, y0_ref, y1_ref, z0_ref, z1_ref, xg_scr, d_scr, o_scr, r_scr):
    e = pl.program_id(0)

    @pl.when(e == 0)
    def _():
        spread_rows(xg_scr, tok_ref, (xa_ref, xb_ref), cap)
        spread_rows(d_scr, tok_ref, (dya_ref, dyb_ref), cap, gcol_ref)

    both_ways(cap, pad, e, w1_ref, w3_ref, w2_ref, xg_ref, a_ref, d_ref, dh1_ref, dh3_ref, xg_scr, d_scr, o_scr, r_scr)

    @pl.when(e == pl.num_programs(0) - 1)
    def _():
        group_sums((y0_ref, y1_ref), q_ref, o_scr, g_ref)
        group_sums((z0_ref, z1_ref), q_ref, r_scr)


def far_both_kernel(cap, pad, xa_ref, xb_ref, dya_ref, dyb_ref, tok_ref, gcol_ref, q_ref, g_ref, unit_ref, form_ref, over_ref, w1_ref, w3_ref, w2_ref, xg_ref, a_ref, d_ref, dh1_ref, dh3_ref, y0_ref, y1_ref, z0_ref, z1_ref, ry0_ref, ry1_ref, rz0_ref, rz1_ref, xg_scr, d_scr, o_scr, r_scr):
    e = pl.program_id(0)

    @pl.when(e == 0)
    def _():
        spread_rows(xg_scr, tok_ref, (xa_ref, xb_ref), cap)
        spread_rows(d_scr, tok_ref, (dya_ref, dyb_ref), cap, gcol_ref)

    both_ways(cap, pad, e, w1_ref, w3_ref, w2_ref, xg_ref, a_ref, d_ref, dh1_ref, dh3_ref, xg_scr, d_scr, o_scr, r_scr)
    done = e == pl.num_programs(0) - 1

    @pl.when(done & (over_ref[0] == 0))
    def _():
        unit_rows((ry0_ref, ry1_ref), unit_ref, o_scr, form_ref)
        unit_rows((rz0_ref, rz1_ref), unit_ref, r_scr)

    @pl.when(done & (over_ref[0] != 0))
    def _():
        group_sums((y0_ref, y1_ref), q_ref, o_scr, g_ref)
        group_sums((z0_ref, z1_ref), q_ref, r_scr)


def whole(shape):
    return pl.BlockSpec(shape, lambda e: (0,) * len(shape))


def per_expert(shape):
    return pl.BlockSpec((1,) + shape[1:], lambda e: (e,) + (0,) * (len(shape) - 1))


def once(shape):
    return pl.BlockSpec(shape, lambda e: (0,) * len(shape), pipeline_mode=pl.Buffered(1))


def of_pair(pair, shape):
    return pl.BlockSpec((PAIR,) + shape[1:], lambda e: (pair,) + (0,) * (len(shape) - 1))


def params():
    return pltpu.CompilerParams(dimension_semantics=("arbitrary",), vmem_limit_bytes=60 * 1024 * 1024)


def flag():
    return pl.BlockSpec(memory_space=pltpu.SMEM)


def far_forward_pair(pair, xa, xb, tok_col, q_row, g_row, unit_row, form_row, over, w1, w3, w2, cap, pad, grp_cap, units):
    experts, hidden, ff = w1.shape
    rows = PAIR * cap
    part, sent = ((grp_cap, hidden), F32), ((units, hidden), BF)
    outs = [((experts, rows, hidden), BF), ((experts, rows, ff), BF), ((experts, rows, ff), F32), ((experts, rows, ff), F32), part, part, sent, sent]
    tables = [tok_col, q_row, g_row, unit_row, form_row]
    return pl.pallas_call(
        functools.partial(far_fwd_kernel, cap, pad),
        grid=(experts,),
        in_specs=[whole(xa.shape), whole(xb.shape)] + [of_pair(pair, t.shape) for t in tables] + [flag(), per_expert(w1.shape), per_expert(w3.shape), per_expert(w2.shape)],
        out_specs=[per_expert(s) if len(s) == 3 else whole(s) for s, _ in outs],
        out_shape=[jax.ShapeDtypeStruct(s, t) for s, t in outs],
        scratch_shapes=[pltpu.VMEM((experts, rows, hidden), BF), pltpu.VMEM((PAIR, experts * pad, hidden), BF)],
        compiler_params=params(),
        cost_estimate=pl.CostEstimate(flops=14 * 10**9, bytes_accessed=50 * 10**6, transcendentals=0),
        name="far_fwd_pair",
    )(xa, xb, *tables, over, w1, w3, w2)


def far_backward_pair(pair, dya, dyb, tok_col, g_col, q_row, unit_row, over, w1, w3, w2, u, v, cap, pad, grp_cap, units):
    experts, hidden, ff = w1.shape
    rows = PAIR * cap
    part, sent = ((grp_cap, hidden), F32), ((units, hidden), BF)
    outs = [((experts, rows, hidden), BF), ((experts, rows, ff), BF), ((experts, rows, ff), BF), part, part, sent, sent]
    tables = [tok_col, g_col, q_row, unit_row]
    return pl.pallas_call(
        functools.partial(far_bwd_kernel, cap, pad),
        grid=(experts,),
        in_specs=[whole(dya.shape), whole(dyb.shape)] + [of_pair(pair, t.shape) for t in tables] + [flag(), per_expert(w1.shape), per_expert(w3.shape), per_expert(w2.shape), per_expert(u.shape), per_expert(v.shape)],
        out_specs=[per_expert(s) if len(s) == 3 else whole(s) for s, _ in outs],
        out_shape=[jax.ShapeDtypeStruct(s, t) for s, t in outs],
        scratch_shapes=[pltpu.VMEM((experts, rows, hidden), BF), pltpu.VMEM((PAIR, experts * pad, hidden), BF)],
        compiler_params=params(),
        cost_estimate=pl.CostEstimate(flops=14 * 10**9, bytes_accessed=50 * 10**6, transcendentals=0),
        name="far_bwd_pair",
    )(dya, dyb, *tables, over, w1, w3, w2, u, v)


def far_both_pair(pair, xa, xb, dya, dyb, tok_col, g_col, q_row, g_row, unit_row, form_row, over, w1, w3, w2, cap, pad, grp_cap, units):
    experts, hidden, ff = w1.shape
    rows = PAIR * cap
    wide, narrow, part, sent = ((experts, rows, hidden), BF), ((experts, rows, ff), BF), ((grp_cap, hidden), F32), ((units, hidden), BF)
    outs = [wide, narrow, wide, narrow, narrow] + [part] * 4 + [sent] * 4
    tables = [tok_col, g_col, q_row, g_row, unit_row, form_row]
    return pl.pallas_call(
        functools.partial(far_both_kernel, cap, pad),
        grid=(experts,),
        in_specs=[once(xa.shape)] * 4 + [of_pair(pair, t.shape) for t in tables] + [flag(), per_expert(w1.shape), per_expert(w3.shape), per_expert(w2.shape)],
        out_specs=[per_expert(s) if len(s) == 3 else once(s) for s, _ in outs],
        out_shape=[jax.ShapeDtypeStruct(s, t) for s, t in outs],
        scratch_shapes=[pltpu.VMEM((experts, rows, hidden), BF)] * 2 + [pltpu.VMEM((PAIR, experts * pad, hidden), BF)] * 2,
        compiler_params=params(),
        cost_estimate=pl.CostEstimate(flops=28 * 10**9, bytes_accessed=70 * 10**6, transcendentals=0),
        name="far_both_pair",
    )(xa, xb, dya, dyb, *tables, over, w1, w3, w2)


def merge_sources(sources, near, sent, place, weight, weighted):
    grp_cap, hidden = near[0].shape
    units, count = sent[0].shape[0], len(sources)
    block = hidden // 3
    notes = [pl.BlockSpec((1, 1, units), functools.partial(lambda k, n: (k, 0, 0), k)) for k in sources]
    return pl.pallas_call(
        functools.partial(merge_kernel, weighted, count),
        grid=(3,),
        in_specs=[pl.BlockSpec((grp_cap, block), lambda n: (0, n))] * count + [pl.BlockSpec((units, block), lambda n: (0, n))] * count + notes * 2,
        out_specs=[pl.BlockSpec((grp_cap, block), lambda n: (0, n))] * count,
        out_shape=[jax.ShapeDtypeStruct((grp_cap, hidden), BF)] * count,
        compiler_params=params(),
        cost_estimate=pl.CostEstimate(flops=count * 10**9, bytes_accessed=count * 4 * 10**6, transcendentals=0),
        name="merge_sources",
    )(*near, *sent, *[place] * count, *[weight] * count)


def near_pair(pair, xa, xb, dya, dyb, tok_col, g_col, q_row, g_row, w1, w3, w2, cap, pad, grp_cap):
    experts, hidden, ff = w1.shape
    rows = PAIR * cap
    wide, narrow, part = ((experts, rows, hidden), BF), ((experts, rows, ff), BF), ((grp_cap, hidden), F32)
    outs = [wide, narrow, wide, narrow, narrow, part, part, part, part]
    tables = [tok_col, g_col, q_row, g_row]
    return pl.pallas_call(
        functools.partial(near_kernel, cap, pad),
        grid=(experts,),
        in_specs=[once(xa.shape)] * 4 + [of_pair(pair, t.shape) for t in tables] + [per_expert(w1.shape), per_expert(w3.shape), per_expert(w2.shape)],
        out_specs=[per_expert(s) if len(s) == 3 else whole(s) for s, _ in outs],
        out_shape=[jax.ShapeDtypeStruct(s, t) for s, t in outs],
        scratch_shapes=[pltpu.VMEM((experts, rows, hidden), BF)] * 2 + [pltpu.VMEM((PAIR, experts * pad, hidden), BF)] * 2,
        compiler_params=params(),
        cost_estimate=pl.CostEstimate(flops=28 * 10**9, bytes_accessed=70 * 10**6, transcendentals=0),
        name="near_pair",
    )(xa, xb, dya, dyb, *tables, w1, w3, w2)


def dw_kernel(chunks, *refs):
    ins, (g1_ref, g3_ref, g2_ref) = refs[:5 * chunks], refs[5 * chunks:]

    def joined(k):
        return jnp.concatenate([ins[k * chunks + c][0] for c in range(chunks)], axis=0)

    x, a, d, dh1, dh3 = (joined(k) for k in range(5))
    g1_ref[0] = dot_at(x, dh1)
    g3_ref[0] = dot_at(x, dh3)
    g2_ref[0] = dot_at(a, d)


def weight_grads(xs, acts, ds, dh1s, dh3s):
    chunks = len(xs)
    experts, _, hidden = xs[0].shape
    ff = acts[0].shape[2]
    args = [*xs, *acts, *ds, *dh1s, *dh3s]
    outs = [(experts, hidden, ff), (experts, hidden, ff), (experts, ff, hidden)]
    return pl.pallas_call(
        functools.partial(dw_kernel, chunks),
        grid=(experts,),
        in_specs=[per_expert(a.shape) for a in args],
        out_specs=[per_expert(s) for s in outs],
        out_shape=[jax.ShapeDtypeStruct(s, F32) for s in outs],
        compiler_params=params(),
        cost_estimate=pl.CostEstimate(flops=25 * 10**9, bytes_accessed=120 * 10**6, transcendentals=0),
        name="weight_grads",
    )(*args)


def final_kernel(groups, *refs):
    q_ref, out_ref = refs[groups], refs[groups + 1]
    total = None
    for h in range(groups):
        lanes = lax.broadcasted_iota(jnp.int32, (out_ref.shape[0], refs[h].shape[0]), 1)
        one_hot = jnp.where(q_ref[:, h:h + 1] == lanes, 1.0, 0.0).astype(BF)
        term = dot(one_hot, refs[h][...])
        total = term if total is None else total + term
    out_ref[...] = total.astype(BF)


def collect(parts, q_cols):
    groups = len(parts)
    tokens = q_cols.shape[0]
    hidden = parts[0].shape[1]
    block = tokens // 4
    return pl.pallas_call(
        functools.partial(final_kernel, groups),
        grid=(4,),
        in_specs=[whole(p.shape) for p in parts] + [pl.BlockSpec((block, groups), lambda e: (e, 0))],
        out_specs=pl.BlockSpec((block, hidden), lambda e: (e, 0)),
        out_shape=jax.ShapeDtypeStruct((tokens, hidden), BF),
        compiler_params=params(),
        cost_estimate=pl.CostEstimate(flops=2 * 10**9, bytes_accessed=5 * 10**6, transcendentals=0),
        name="collect",
    )(*parts, q_cols)


def after(earlier, value):
    return lax.optimization_barrier((earlier, value))[1]


def slot_tables(ids, gates, first_exp, experts, group, per_group, cap):
    sources, _, tokens = ids.shape
    eq = ids[:, None] == (first_exp + jnp.arange(experts))[None, :, None, None]
    hit = jnp.any(eq, axis=2)
    gate = jnp.sum(jnp.where(eq, gates[:, None], 0.0), axis=2)
    member = jnp.any(ids // per_group == group, axis=1, keepdims=True)
    pos = count_earlier(jnp.concatenate([hit, member], axis=1).reshape(sources * (experts + 1), tokens))
    pos = pos.reshape(sources, experts + 1, tokens)
    exp_pos, grp_pos = pos[:, :experts], pos[:, experts:]
    taken = hit[:, :, None, :] & (exp_pos[:, :, None, :] == jnp.arange(cap, dtype=F32)[None, None, :, None])
    numbers = jnp.arange(1, tokens + 1, dtype=F32)[None, None, None, :]
    tok = jnp.sum(jnp.where(taken, numbers, 0.0), axis=3) - 1.0
    place = jnp.sum(jnp.where(taken, grp_pos[:, :, None, :] + 1.0, 0.0), axis=3) - 1.0
    weight = jnp.sum(jnp.where(taken, gate[:, :, None, :], 0.0), axis=3)
    here = jnp.sum(hit, axis=1).astype(F32)
    alone = here == jnp.sum(ids // per_group == group, axis=1).astype(F32)
    first = count_earlier(jnp.where(alone, jnp.minimum(here, 1.0), here))
    rank, seen = [], jnp.zeros((sources, tokens), F32)
    for e in range(experts):
        rank.append(seen)
        seen = seen + hit[:, e].astype(F32)
    unit = first[:, None] + jnp.where(alone[:, None], ALONE, jnp.stack(rank, axis=1)) + 1.0
    code = jnp.sum(jnp.where(taken, unit[:, :, None, :], 0.0), axis=3)
    lone = code > ALONE
    return tok, place, weight, jnp.where(lone, code - ALONE, code) - 1.0, lone


def longest_list(ids, per_group, experts, away):
    devices = away.shape[1]
    count = jnp.sum(ids[:, None] // experts == jnp.arange(devices)[None, :, None, None], axis=2)
    half = per_group // experts
    in_group = jnp.repeat(jnp.sum(count.reshape(ids.shape[0], devices // half, half, -1), axis=2), half, axis=1)
    rows = jnp.where(count == in_group, jnp.minimum(count, 1), count)
    return jnp.max(jnp.where(away, jnp.sum(rows, axis=2), 0))


def count_earlier(marks):
    tokens = marks.shape[1]
    earlier = (jnp.arange(tokens)[:, None] < jnp.arange(tokens)[None, :]).astype(BF)
    return jnp.dot(marks.astype(BF), earlier, preferred_element_type=F32)


def solution(mesh):
    groups = mesh.shape['grp']
    inner = mesh.shape['ing']
    devices = groups * inner
    tok_spec = P(('dp', 'grp', 'ing'), None)
    weight_spec = P(('grp', 'ing'), None, None)
    grad_spec = P(('dp', 'grp', 'ing'), None, None)

    def hop_y(a):
        return lax.ppermute(a, 'ing', [(0, 1), (1, 0)])

    def hop_g(a, bits):
        return lax.ppermute(a, 'grp', [(g, g ^ bits) for g in range(groups)])

    def device_fn(x_loc, ids_loc, gates_loc, dy_loc, w1, w3, w2):
        tokens, _ = x_loc.shape
        top_k = ids_loc.shape[1]
        experts = w1.shape[0]
        num_exp = experts * devices
        grp_cap = tokens * 2 // groups
        cap = 3 * tokens * top_k // (2 * num_exp)
        pad = -(-cap // 16) * 16
        grp, ing = lax.axis_index('grp'), lax.axis_index('ing')

        per_group = experts * inner
        own = jnp.concatenate([ids_loc.T.astype(F32), gates_loc.T], axis=0)[None]
        pair = jnp.concatenate([own, hop_y(own)], axis=0)
        pair_c = hop_g(pair, 1)
        quad_x = hop_g(jnp.concatenate([pair, pair_c], axis=0), 2)
        routing = jnp.stack([pair[1], pair_c[1], quad_x[1], quad_x[3], pair[0], pair_c[0], quad_x[0], quad_x[2]])

        x_far = hop_y(x_loc)
        dy_far = hop_y(dy_loc)
        x_near_c = hop_g(after(pair_c, x_loc), 1)
        x_near_x = hop_g(x_loc, 2)
        dy_near_c = hop_g(after(x_near_c, dy_loc), 1)
        x_far_c, x_far_x = hop_g(x_far, 1), hop_g(x_far, 2)
        x_near_xc, x_far_xc = hop_g(x_near_x, 1), hop_g(x_far_x, 1)
        dy_far_c, dy_far_x = hop_g(dy_far, 1), hop_g(dy_far, 2)
        dy_far_xc = hop_g(dy_far_x, 1)
        dy_near_x = hop_g(dy_loc, 2)
        dy_near_xc = hop_g(dy_near_x, 1)
        x_pairs = [(x_far, x_far_c), (x_far_x, x_far_xc), (x_loc, x_near_c), (x_near_x, x_near_xc)]
        dy_pairs = [(dy_far, dy_far_c), (dy_far_x, dy_far_xc), (dy_loc, dy_near_c), (dy_near_x, dy_near_xc)]

        ids_rel, gates_rel = routing[:, :top_k].astype(jnp.int32), routing[:, top_k:]
        units = tokens * SENT_SHARE[0] // SENT_SHARE[1]
        tok_rel, place_rel, weight_rel, unit_rel, lone_rel = slot_tables(ids_rel, gates_rel, (grp * inner + ing) * experts, experts, grp, per_group, cap)
        far = devices // 2
        source_ing = jnp.where(jnp.arange(devices) < far, 1 - ing, ing)
        away = source_ing[:, None] != (jnp.arange(devices) % inner)[None, :]
        over = longest_list(ids_rel, per_group, experts, away) > units
        over_flag = over.astype(jnp.int32).reshape(1)
        flat = [t[:far].reshape(far, 1, -1) for t in (unit_rel, place_rel, jnp.where(lone_rel, 1.0, weight_rel))]
        sent_here = flat[0] == jnp.arange(units, dtype=F32)[None, :, None]
        notes = jnp.stack([jnp.max(jnp.where(sent_here, flat[1], -1.0), axis=2), jnp.max(jnp.where(sent_here, flat[2], 0.0), axis=2)])
        notes = hop_y(notes)
        sent_place = notes[0].astype(jnp.int32).reshape(far, 1, units)
        sent_weight = notes[1].reshape(far, 1, units)
        own_groups = ids_loc.T[None] // per_group == (grp ^ jnp.arange(groups))[:, None, None]
        own_member = jnp.any(own_groups, axis=1)
        q_cols = jnp.where(own_member, count_earlier(own_member), -1.0).astype(jnp.int32).T
        slots = experts * cap
        tok_cols = tok_rel.astype(jnp.int32).reshape(devices, slots, 1)
        g_cols = weight_rel.reshape(devices, slots, 1)
        spare = ((0, 0), (0, 0), (0, pad - cap))
        q_rows = jnp.pad(place_rel, spare, constant_values=-1.0).astype(jnp.int32).reshape(devices, 1, experts * pad)
        g_rows = jnp.pad(weight_rel, spare).reshape(devices, 1, experts * pad)
        unit_rows = jnp.pad(unit_rel[:far], spare, constant_values=-1.0).astype(jnp.int32).reshape(far, 1, experts * pad)
        form_rows = jnp.pad(jnp.where(lone_rel, weight_rel, 1.0)[:far], spare).reshape(far, 1, experts * pad)

        xs, acts, ds, dh1s, dh3s, y_sums, dx_sums, y_sent, dx_sent = ([None] * 4 for _ in range(9))
        saved = {}
        last = None
        for step, c in KERNEL_ORDER:
            places = q_rows if last is None else after(last, q_rows)
            if step == 'n':
                xs[c], acts[c], ds[c], dh1s[c], dh3s[c], *sums = near_pair(c, *x_pairs[c], *dy_pairs[c], tok_cols, g_cols, places, g_rows, w1, w3, w2, cap, pad, grp_cap)
                y_sums[c], dx_sums[c] = sums[:PAIR], sums[PAIR:]
            elif step == 'm':
                xs[c], acts[c], ds[c], dh1s[c], dh3s[c], *sums = far_both_pair(c, *x_pairs[c], *dy_pairs[c], tok_cols, g_cols, places, g_rows, unit_rows, form_rows, over_flag, w1, w3, w2, cap, pad, grp_cap, units)
                y_sums[c], dx_sums[c], y_sent[c], dx_sent[c] = (sums[k:k + PAIR] for k in range(0, 4 * PAIR, PAIR))
            elif step == 'f':
                xs[c], acts[c], *saved[c], y0, y1, r0, r1 = far_forward_pair(c, *x_pairs[c], tok_cols, places, g_rows, unit_rows, form_rows, over_flag, w1, w3, w2, cap, pad, grp_cap, units)
                y_sums[c], y_sent[c] = (y0, y1), (r0, r1)
            else:
                ds[c], dh1s[c], dh3s[c], z0, z1, r0, r1 = far_backward_pair(c, *dy_pairs[c], tok_cols, g_cols, places, unit_rows, over_flag, w1, w3, w2, *saved[c], cap, pad, grp_cap, units)
                dx_sums[c], dx_sent[c] = (z0, z1), (r0, r1)
            last = (y_sums if step == 'f' else dx_sums)[c][0]

        grads = weight_grads(xs, acts, ds, dh1s, dh3s)

        def combine(results, sent, weighted, split):
            near = [*results[2], *results[3]]
            full = [*results[0], *results[1]]
            arrived = [hop_y(r) for r in (*sent[0], *sent[1])]
            sums = []
            for sources in split:

                def by_rows(ops):
                    return list(merge_sources(sources, ops[0], ops[1], sent_place, sent_weight, weighted))

                def by_sums(ops):
                    return [(n + hop_y(f)).astype(BF) for n, f in zip(ops[0], ops[2])]

                sums += lax.cond(over, by_sums, by_rows, tuple([rows[k] for k in sources] for rows in (near, arrived, full)))
            return [sums[0]] + [hop_g(sums[k], k) for k in (1, 2, 3)]

        y_parts = combine(y_sums, y_sent, True, ((0, 1), (2, 3)))
        y_out = collect(y_parts, q_cols)
        dx_out = collect(combine(dx_sums, dx_sent, False, ((0, 1), (2,), (3,))), q_cols)
        return y_out, dx_out, grads[0], grads[1], grads[2]

    return jax.shard_map(device_fn, mesh=mesh, in_specs=(tok_spec, tok_spec, tok_spec, tok_spec, weight_spec, weight_spec, weight_spec), out_specs=(tok_spec, tok_spec, grad_spec, grad_spec, grad_spec), check_vma=False)
```

```python
import functools

import jax
import jax.numpy as jnp
from jax import lax
from jax.experimental import pallas as pl
from jax.experimental.pallas import tpu as pltpu
from jax.sharding import PartitionSpec as P


BF = jnp.bfloat16
F32 = jnp.float32
ALONE = 1024.0
SENT_SHARE = 27, 32
PAIR = 2

KERNEL_ORDER = (('f', 0), ('b', 0), ('m', 1), ('n', 2), ('n', 3))


def dot(a, b):
    return lax.dot_general(a, b, (((1,), (0,)), ((), ())), preferred_element_type=F32)


def dot_bt(a, b):
    return lax.dot_general(a, b, (((1,), (1,)), ((), ())), preferred_element_type=F32)


def dot_at(a, b):
    return lax.dot_general(a, b, (((0,), (0,)), ((), ())), preferred_element_type=F32)


def pick_rows(tok_col, rows_ref):
    tokens = rows_ref.shape[0]
    lanes = lax.broadcasted_iota(jnp.int32, (tok_col.shape[0], tokens), 1)
    one_hot = jnp.where(tok_col == lanes, 1.0, 0.0).astype(BF)
    return dot(one_hot, rows_ref[...])


def store_by_expert(dst_ref, rows, cap):
    for e in range(dst_ref.shape[0]):
        dst_ref[e] = jnp.concatenate([r[e * cap:(e + 1) * cap] for r in rows], axis=0).astype(BF)


def keep_rows(dst_ref, rows, e, cap, pad):
    zeros = jnp.zeros((pad - cap, rows.shape[1]), F32)
    for s in range(PAIR):
        padded = jnp.concatenate([rows[s * cap:(s + 1) * cap], zeros], axis=0).astype(BF)
        dst_ref[s, pl.ds(pl.multiple_of(e * pad, pad), pad), :] = padded


def spread_rows(dst_ref, tok_ref, row_refs, cap, gcol_ref=None):
    picked = [pick_rows(tok_ref[s], r) for s, r in enumerate(row_refs)]
    if gcol_ref is not None:
        picked = [gcol_ref[s] * p for s, p in enumerate(picked)]
    store_by_expert(dst_ref, picked, cap)


def forward_expert(xg, w1_ref, w3_ref):
    h1 = dot(xg, w1_ref[0])
    h3 = dot(xg, w3_ref[0])
    sig = jax.nn.sigmoid(h1)
    silu = h1 * sig
    act = (silu * h3).astype(BF)
    return act, h3 * (sig * (1.0 + h1 * (1.0 - sig))), silu


def mixers(hit, weight):
    if weight is None:
        return [jnp.where(hit, 1.0, 0.0).astype(BF)]
    terms = []
    for _ in range(3):
        part = weight.astype(BF)
        terms.append(jnp.where(hit, part.astype(F32), 0.0).astype(BF))
        weight = weight - part.astype(F32)
    return terms


def weighted_rows(hit, weight, rows):
    total = None
    for term in mixers(hit, weight):
        product = dot(term, rows)
        total = product if total is None else total + product
    return total


def group_sums(p_refs, q_ref, rows_scr, g_ref=None):
    for s, p_ref in enumerate(p_refs):
        slots = lax.broadcasted_iota(jnp.int32, (p_ref.shape[0], q_ref.shape[2]), 0)
        p_ref[...] = weighted_rows(q_ref[s] == slots, None if g_ref is None else g_ref[s], rows_scr[s])


def unit_rows(u_refs, unit_ref, rows_scr, weight_ref=None):
    for s, u_ref in enumerate(u_refs):
        units = lax.broadcasted_iota(jnp.int32, (u_ref.shape[0], unit_ref.shape[2]), 0)
        u_ref[...] = weighted_rows(unit_ref[s] == units, None if weight_ref is None else weight_ref[s], rows_scr[s]).astype(BF)


def far_fwd_kernel(cap, pad, xa_ref, xb_ref, tok_ref, q_ref, g_ref, unit_ref, form_ref, over_ref, w1_ref, w3_ref, w2_ref, xg_ref, a_ref, u_ref, v_ref, p0_ref, p1_ref, r0_ref, r1_ref, xg_scr, o_scr):
    e = pl.program_id(0)

    @pl.when(e == 0)
    def _():
        spread_rows(xg_scr, tok_ref, (xa_ref, xb_ref), cap)

    xg_ref[0] = xg_scr[e]
    act, u_ref[0], v_ref[0] = forward_expert(xg_scr[e], w1_ref, w3_ref)
    a_ref[0] = act
    keep_rows(o_scr, dot(act, w2_ref[0]), e, cap, pad)
    done = e == pl.num_programs(0) - 1

    @pl.when(done & (over_ref[0] == 0))
    def _():
        unit_rows((r0_ref, r1_ref), unit_ref, o_scr, form_ref)

    @pl.when(done & (over_ref[0] != 0))
    def _():
        group_sums((p0_ref, p1_ref), q_ref, o_scr, g_ref)


def far_bwd_kernel(cap, pad, dya_ref, dyb_ref, tok_ref, gcol_ref, q_ref, unit_ref, over_ref, w1_ref, w3_ref, w2_ref, u_ref, v_ref, d_ref, dh1_ref, dh3_ref, p0_ref, p1_ref, r0_ref, r1_ref, d_scr, r_scr):
    e = pl.program_id(0)

    @pl.when(e == 0)
    def _():
        spread_rows(d_scr, tok_ref, (dya_ref, dyb_ref), cap, gcol_ref)

    d_ref[0] = d_scr[e]
    da = dot_bt(d_scr[e], w2_ref[0])
    dh1 = (da * u_ref[0]).astype(BF)
    dh3 = (da * v_ref[0]).astype(BF)
    dh1_ref[0] = dh1
    dh3_ref[0] = dh3
    keep_rows(r_scr, dot_bt(dh1, w1_ref[0]) + dot_bt(dh3, w3_ref[0]), e, cap, pad)
    done = e == pl.num_programs(0) - 1

    @pl.when(done & (over_ref[0] == 0))
    def _():
        unit_rows((r0_ref, r1_ref), unit_ref, r_scr)

    @pl.when(done & (over_ref[0] != 0))
    def _():
        group_sums((p0_ref, p1_ref), q_ref, r_scr)


def merge_kernel(weighted, count, *refs):
    near, sent, places, weights, outs = (refs[k * count:(k + 1) * count] for k in range(5))
    mix_ref = refs[5 * count]

    @pl.when(pl.program_id(0) == 0)
    def _():
        for s, (place_ref, weight_ref) in enumerate(zip(places, weights)):
            hit = place_ref[0] == lax.broadcasted_iota(jnp.int32, mix_ref.shape[2:], 0)
            for k, term in enumerate(mixers(hit, weight_ref[0] if weighted else None)):
                mix_ref[s, k] = term

    for s, (n_ref, r_ref, p_ref) in enumerate(zip(near, sent, outs)):
        total = n_ref[...]
        for k in range(mix_ref.shape[1]):
            total = total + dot(mix_ref[s, k], r_ref[...])
        p_ref[...] = total.astype(BF)


def both_ways(cap, pad, e, w1_ref, w3_ref, w2_ref, xg_ref, a_ref, d_ref, dh1_ref, dh3_ref, xg_scr, d_scr, o_scr, r_scr):
    xg_ref[0] = xg_scr[e]
    d_ref[0] = d_scr[e]
    act, u, v = forward_expert(xg_scr[e], w1_ref, w3_ref)
    a_ref[0] = act
    keep_rows(o_scr, dot(act, w2_ref[0]), e, cap, pad)
    da = dot_bt(d_scr[e], w2_ref[0])
    dh1 = (da * u).astype(BF)
    dh3 = (da * v).astype(BF)
    dh1_ref[0] = dh1
    dh3_ref[0] = dh3
    keep_rows(r_scr, dot_bt(dh1, w1_ref[0]) + dot_bt(dh3, w3_ref[0]), e, cap, pad)


def near_kernel(cap, pad, xa_ref, xb_ref, dya_ref, dyb_ref, tok_ref, gcol_ref, q_ref, g_ref, w1_ref, w3_ref, w2_ref, xg_ref, a_ref, d_ref, dh1_ref, dh3_ref, y0_ref, y1_ref, z0_ref, z1_ref, xg_scr, d_scr, o_scr, r_scr):
    e = pl.program_id(0)

    @pl.when(e == 0)
    def _():
        spread_rows(xg_scr, tok_ref, (xa_ref, xb_ref), cap)
        spread_rows(d_scr, tok_ref, (dya_ref, dyb_ref), cap, gcol_ref)

    both_ways(cap, pad, e, w1_ref, w3_ref, w2_ref, xg_ref, a_ref, d_ref, dh1_ref, dh3_ref, xg_scr, d_scr, o_scr, r_scr)

    @pl.when(e == pl.num_programs(0) - 1)
    def _():
        group_sums((y0_ref, y1_ref), q_ref, o_scr, g_ref)
        group_sums((z0_ref, z1_ref), q_ref, r_scr)


def far_both_kernel(cap, pad, xa_ref, xb_ref, dya_ref, dyb_ref, tok_ref, gcol_ref, q_ref, g_ref, unit_ref, form_ref, over_ref, w1_ref, w3_ref, w2_ref, xg_ref, a_ref, d_ref, dh1_ref, dh3_ref, y0_ref, y1_ref, z0_ref, z1_ref, ry0_ref, ry1_ref, rz0_ref, rz1_ref, xg_scr, d_scr, o_scr, r_scr):
    e = pl.program_id(0)

    @pl.when(e == 0)
    def _():
        spread_rows(xg_scr, tok_ref, (xa_ref, xb_ref), cap)
        spread_rows(d_scr, tok_ref, (dya_ref, dyb_ref), cap, gcol_ref)

    both_ways(cap, pad, e, w1_ref, w3_ref, w2_ref, xg_ref, a_ref, d_ref, dh1_ref, dh3_ref, xg_scr, d_scr, o_scr, r_scr)
    done = e == pl.num_programs(0) - 1

    @pl.when(done & (over_ref[0] == 0))
    def _():
        unit_rows((ry0_ref, ry1_ref), unit_ref, o_scr, form_ref)
        unit_rows((rz0_ref, rz1_ref), unit_ref, r_scr)

    @pl.when(done & (over_ref[0] != 0))
    def _():
        group_sums((y0_ref, y1_ref), q_ref, o_scr, g_ref)
        group_sums((z0_ref, z1_ref), q_ref, r_scr)


def whole(shape):
    return pl.BlockSpec(shape, lambda e: (0,) * len(shape))


def per_expert(shape):
    return pl.BlockSpec((1,) + shape[1:], lambda e: (e,) + (0,) * (len(shape) - 1))


def once(shape):
    return pl.BlockSpec(shape, lambda e: (0,) * len(shape), pipeline_mode=pl.Buffered(1))


def of_pair(pair, shape):
    return pl.BlockSpec((PAIR,) + shape[1:], lambda e: (pair,) + (0,) * (len(shape) - 1))


def params():
    return pltpu.CompilerParams(dimension_semantics=("arbitrary",), vmem_limit_bytes=60 * 1024 * 1024)


def flag():
    return pl.BlockSpec(memory_space=pltpu.SMEM)


def far_forward_pair(pair, xa, xb, tok_col, q_row, g_row, unit_row, form_row, over, w1, w3, w2, cap, pad, grp_cap, units):
    experts, hidden, ff = w1.shape
    rows = PAIR * cap
    part, sent = ((grp_cap, hidden), F32), ((units, hidden), BF)
    outs = [((experts, rows, hidden), BF), ((experts, rows, ff), BF), ((experts, rows, ff), F32), ((experts, rows, ff), F32), part, part, sent, sent]
    tables = [tok_col, q_row, g_row, unit_row, form_row]
    return pl.pallas_call(
        functools.partial(far_fwd_kernel, cap, pad),
        grid=(experts,),
        in_specs=[whole(xa.shape), whole(xb.shape)] + [of_pair(pair, t.shape) for t in tables] + [flag(), per_expert(w1.shape), per_expert(w3.shape), per_expert(w2.shape)],
        out_specs=[per_expert(s) if len(s) == 3 else whole(s) for s, _ in outs],
        out_shape=[jax.ShapeDtypeStruct(s, t) for s, t in outs],
        scratch_shapes=[pltpu.VMEM((experts, rows, hidden), BF), pltpu.VMEM((PAIR, experts * pad, hidden), BF)],
        compiler_params=params(),
        cost_estimate=pl.CostEstimate(flops=14 * 10**9, bytes_accessed=50 * 10**6, transcendentals=0),
        name="far_fwd_pair",
    )(xa, xb, *tables, over, w1, w3, w2)


def far_backward_pair(pair, dya, dyb, tok_col, g_col, q_row, unit_row, over, w1, w3, w2, u, v, cap, pad, grp_cap, units):
    experts, hidden, ff = w1.shape
    rows = PAIR * cap
    part, sent = ((grp_cap, hidden), F32), ((units, hidden), BF)
    outs = [((experts, rows, hidden), BF), ((experts, rows, ff), BF), ((experts, rows, ff), BF), part, part, sent, sent]
    tables = [tok_col, g_col, q_row, unit_row]
    return pl.pallas_call(
        functools.partial(far_bwd_kernel, cap, pad),
        grid=(experts,),
        in_specs=[whole(dya.shape), whole(dyb.shape)] + [of_pair(pair, t.shape) for t in tables] + [flag(), per_expert(w1.shape), per_expert(w3.shape), per_expert(w2.shape), per_expert(u.shape), per_expert(v.shape)],
        out_specs=[per_expert(s) if len(s) == 3 else whole(s) for s, _ in outs],
        out_shape=[jax.ShapeDtypeStruct(s, t) for s, t in outs],
        scratch_shapes=[pltpu.VMEM((experts, rows, hidden), BF), pltpu.VMEM((PAIR, experts * pad, hidden), BF)],
        compiler_params=params(),
        cost_estimate=pl.CostEstimate(flops=14 * 10**9, bytes_accessed=50 * 10**6, transcendentals=0),
        name="far_bwd_pair",
    )(dya, dyb, *tables, over, w1, w3, w2, u, v)


def far_both_pair(pair, xa, xb, dya, dyb, tok_col, g_col, q_row, g_row, unit_row, form_row, over, w1, w3, w2, cap, pad, grp_cap, units):
    experts, hidden, ff = w1.shape
    rows = PAIR * cap
    wide, narrow, part, sent = ((experts, rows, hidden), BF), ((experts, rows, ff), BF), ((grp_cap, hidden), F32), ((units, hidden), BF)
    outs = [wide, narrow, wide, narrow, narrow] + [part] * 4 + [sent] * 4
    tables = [tok_col, g_col, q_row, g_row, unit_row, form_row]
    return pl.pallas_call(
        functools.partial(far_both_kernel, cap, pad),
        grid=(experts,),
        in_specs=[once(xa.shape)] * 4 + [of_pair(pair, t.shape) for t in tables] + [flag(), per_expert(w1.shape), per_expert(w3.shape), per_expert(w2.shape)],
        out_specs=[per_expert(s) if len(s) == 3 else once(s) for s, _ in outs],
        out_shape=[jax.ShapeDtypeStruct(s, t) for s, t in outs],
        scratch_shapes=[pltpu.VMEM((experts, rows, hidden), BF)] * 2 + [pltpu.VMEM((PAIR, experts * pad, hidden), BF)] * 2,
        compiler_params=params(),
        cost_estimate=pl.CostEstimate(flops=28 * 10**9, bytes_accessed=70 * 10**6, transcendentals=0),
        name="far_both_pair",
    )(xa, xb, dya, dyb, *tables, over, w1, w3, w2)


def merge_sources(sources, near, sent, place, weight, weighted):
    grp_cap, hidden = near[0].shape
    units, count = sent[0].shape[0], len(sources)
    block = hidden // 3
    notes = [pl.BlockSpec((1, 1, units), functools.partial(lambda k, n: (k, 0, 0), k)) for k in sources]
    return pl.pallas_call(
        functools.partial(merge_kernel, weighted, count),
        grid=(3,),
        in_specs=[pl.BlockSpec((grp_cap, block), lambda n: (0, n))] * count + [pl.BlockSpec((units, block), lambda n: (0, n))] * count + notes * 2,
        out_specs=[pl.BlockSpec((grp_cap, block), lambda n: (0, n))] * count,
        out_shape=[jax.ShapeDtypeStruct((grp_cap, hidden), BF)] * count,
        scratch_shapes=[pltpu.VMEM((count, 3 if weighted else 1, grp_cap, units), BF)],
        compiler_params=params(),
        cost_estimate=pl.CostEstimate(flops=count * 10**9, bytes_accessed=count * 4 * 10**6, transcendentals=0),
        name="merge_sources",
    )(*near, *sent, *[place] * count, *[weight] * count)


def near_pair(pair, xa, xb, dya, dyb, tok_col, g_col, q_row, g_row, w1, w3, w2, cap, pad, grp_cap):
    experts, hidden, ff = w1.shape
    rows = PAIR * cap
    wide, narrow, part = ((experts, rows, hidden), BF), ((experts, rows, ff), BF), ((grp_cap, hidden), F32)
    outs = [wide, narrow, wide, narrow, narrow, part, part, part, part]
    tables = [tok_col, g_col, q_row, g_row]
    return pl.pallas_call(
        functools.partial(near_kernel, cap, pad),
        grid=(experts,),
        in_specs=[once(xa.shape)] * 4 + [of_pair(pair, t.shape) for t in tables] + [per_expert(w1.shape), per_expert(w3.shape), per_expert(w2.shape)],
        out_specs=[per_expert(s) if len(s) == 3 else whole(s) for s, _ in outs],
        out_shape=[jax.ShapeDtypeStruct(s, t) for s, t in outs],
        scratch_shapes=[pltpu.VMEM((experts, rows, hidden), BF)] * 2 + [pltpu.VMEM((PAIR, experts * pad, hidden), BF)] * 2,
        compiler_params=params(),
        cost_estimate=pl.CostEstimate(flops=28 * 10**9, bytes_accessed=70 * 10**6, transcendentals=0),
        name="near_pair",
    )(xa, xb, dya, dyb, *tables, w1, w3, w2)


def dw_kernel(chunks, *refs):
    ins, (g1_ref, g3_ref, g2_ref) = refs[:5 * chunks], refs[5 * chunks:]

    def joined(k):
        return jnp.concatenate([ins[k * chunks + c][0] for c in range(chunks)], axis=0)

    x, a, d, dh1, dh3 = (joined(k) for k in range(5))
    g1_ref[0] = dot_at(x, dh1)
    g3_ref[0] = dot_at(x, dh3)
    g2_ref[0] = dot_at(a, d)


def weight_grads(xs, acts, ds, dh1s, dh3s):
    chunks = len(xs)
    experts, _, hidden = xs[0].shape
    ff = acts[0].shape[2]
    args = [*xs, *acts, *ds, *dh1s, *dh3s]
    outs = [(experts, hidden, ff), (experts, hidden, ff), (experts, ff, hidden)]
    return pl.pallas_call(
        functools.partial(dw_kernel, chunks),
        grid=(experts,),
        in_specs=[per_expert(a.shape) for a in args],
        out_specs=[per_expert(s) for s in outs],
        out_shape=[jax.ShapeDtypeStruct(s, F32) for s in outs],
        compiler_params=params(),
        cost_estimate=pl.CostEstimate(flops=25 * 10**9, bytes_accessed=120 * 10**6, transcendentals=0),
        name="weight_grads",
    )(*args)


def final_kernel(groups, *refs):
    q_ref, out_ref = refs[groups], refs[groups + 1]
    total = None
    for h in range(groups):
        lanes = lax.broadcasted_iota(jnp.int32, (out_ref.shape[0], refs[h].shape[0]), 1)
        one_hot = jnp.where(q_ref[:, h:h + 1] == lanes, 1.0, 0.0).astype(BF)
        term = dot(one_hot, refs[h][...])
        total = term if total is None else total + term
    out_ref[...] = total.astype(BF)


def collect(parts, q_cols):
    groups = len(parts)
    tokens = q_cols.shape[0]
    hidden = parts[0].shape[1]
    block = tokens // 4
    return pl.pallas_call(
        functools.partial(final_kernel, groups),
        grid=(4,),
        in_specs=[whole(p.shape) for p in parts] + [pl.BlockSpec((block, groups), lambda e: (e, 0))],
        out_specs=pl.BlockSpec((block, hidden), lambda e: (e, 0)),
        out_shape=jax.ShapeDtypeStruct((tokens, hidden), BF),
        compiler_params=params(),
        cost_estimate=pl.CostEstimate(flops=2 * 10**9, bytes_accessed=5 * 10**6, transcendentals=0),
        name="collect",
    )(*parts, q_cols)


def after(earlier, value):
    return lax.optimization_barrier((earlier, value))[1]


def slot_tables(ids, gates, first_exp, experts, group, per_group, cap):
    sources, _, tokens = ids.shape
    eq = ids[:, None] == (first_exp + jnp.arange(experts))[None, :, None, None]
    hit = jnp.any(eq, axis=2)
    gate = jnp.sum(jnp.where(eq, gates[:, None], 0.0), axis=2)
    member = jnp.any(ids // per_group == group, axis=1, keepdims=True)
    pos = count_earlier(jnp.concatenate([hit, member], axis=1).reshape(sources * (experts + 1), tokens))
    pos = pos.reshape(sources, experts + 1, tokens)
    exp_pos, grp_pos = pos[:, :experts], pos[:, experts:]
    taken = hit[:, :, None, :] & (exp_pos[:, :, None, :] == jnp.arange(cap, dtype=F32)[None, None, :, None])
    numbers = jnp.arange(1, tokens + 1, dtype=F32)[None, None, None, :]
    tok = jnp.sum(jnp.where(taken, numbers, 0.0), axis=3) - 1.0
    place = jnp.sum(jnp.where(taken, grp_pos[:, :, None, :] + 1.0, 0.0), axis=3) - 1.0
    weight = jnp.sum(jnp.where(taken, gate[:, :, None, :], 0.0), axis=3)
    here = jnp.sum(hit, axis=1).astype(F32)
    alone = here == jnp.sum(ids // per_group == group, axis=1).astype(F32)
    first = count_earlier(jnp.where(alone, jnp.minimum(here, 1.0), here))
    rank, seen = [], jnp.zeros((sources, tokens), F32)
    for e in range(experts):
        rank.append(seen)
        seen = seen + hit[:, e].astype(F32)
    unit = first[:, None] + jnp.where(alone[:, None], ALONE, jnp.stack(rank, axis=1)) + 1.0
    code = jnp.sum(jnp.where(taken, unit[:, :, None, :], 0.0), axis=3)
    lone = code > ALONE
    return tok, place, weight, jnp.where(lone, code - ALONE, code) - 1.0, lone


def longest_list(ids, per_group, experts, away):
    devices = away.shape[1]
    count = jnp.sum(ids[:, None] // experts == jnp.arange(devices)[None, :, None, None], axis=2)
    half = per_group // experts
    in_group = jnp.repeat(jnp.sum(count.reshape(ids.shape[0], devices // half, half, -1), axis=2), half, axis=1)
    rows = jnp.where(count == in_group, jnp.minimum(count, 1), count)
    return jnp.max(jnp.where(away, jnp.sum(rows, axis=2), 0))


def count_earlier(marks):
    tokens = marks.shape[1]
    earlier = (jnp.arange(tokens)[:, None] < jnp.arange(tokens)[None, :]).astype(BF)
    return jnp.dot(marks.astype(BF), earlier, preferred_element_type=F32)


def solution(mesh):
    groups = mesh.shape['grp']
    inner = mesh.shape['ing']
    devices = groups * inner
    tok_spec = P(('dp', 'grp', 'ing'), None)
    weight_spec = P(('grp', 'ing'), None, None)
    grad_spec = P(('dp', 'grp', 'ing'), None, None)

    def hop_y(a):
        return lax.ppermute(a, 'ing', [(0, 1), (1, 0)])

    def hop_g(a, bits):
        return lax.ppermute(a, 'grp', [(g, g ^ bits) for g in range(groups)])

    def device_fn(x_loc, ids_loc, gates_loc, dy_loc, w1, w3, w2):
        tokens, _ = x_loc.shape
        top_k = ids_loc.shape[1]
        experts = w1.shape[0]
        num_exp = experts * devices
        grp_cap = tokens * 2 // groups
        cap = 3 * tokens * top_k // (2 * num_exp)
        pad = -(-cap // 16) * 16
        grp, ing = lax.axis_index('grp'), lax.axis_index('ing')

        per_group = experts * inner
        own = jnp.concatenate([ids_loc.T.astype(F32), gates_loc.T], axis=0)[None]
        pair = jnp.concatenate([own, hop_y(own)], axis=0)
        pair_c = hop_g(pair, 1)
        quad_x = hop_g(jnp.concatenate([pair, pair_c], axis=0), 2)
        routing = jnp.stack([pair[1], pair_c[1], quad_x[1], quad_x[3], pair[0], pair_c[0], quad_x[0], quad_x[2]])

        x_far = hop_y(x_loc)
        dy_far = hop_y(dy_loc)
        x_near_c = hop_g(after(pair_c, x_loc), 1)
        x_near_x = hop_g(x_loc, 2)
        dy_near_c = hop_g(after(x_near_c, dy_loc), 1)
        x_far_c, x_far_x = hop_g(x_far, 1), hop_g(x_far, 2)
        x_near_xc, x_far_xc = hop_g(x_near_x, 1), hop_g(x_far_x, 1)
        dy_far_c, dy_far_x = hop_g(dy_far, 1), hop_g(dy_far, 2)
        dy_far_xc = hop_g(dy_far_x, 1)
        dy_near_x = hop_g(dy_loc, 2)
        dy_near_xc = hop_g(dy_near_x, 1)
        x_pairs = [(x_far, x_far_c), (x_far_x, x_far_xc), (x_loc, x_near_c), (x_near_x, x_near_xc)]
        dy_pairs = [(dy_far, dy_far_c), (dy_far_x, dy_far_xc), (dy_loc, dy_near_c), (dy_near_x, dy_near_xc)]

        ids_rel, gates_rel = routing[:, :top_k].astype(jnp.int32), routing[:, top_k:]
        units = tokens * SENT_SHARE[0] // SENT_SHARE[1]
        tok_rel, place_rel, weight_rel, unit_rel, lone_rel = slot_tables(ids_rel, gates_rel, (grp * inner + ing) * experts, experts, grp, per_group, cap)
        far = devices // 2
        source_ing = jnp.where(jnp.arange(devices) < far, 1 - ing, ing)
        away = source_ing[:, None] != (jnp.arange(devices) % inner)[None, :]
        over = longest_list(ids_rel, per_group, experts, away) > units
        over_flag = over.astype(jnp.int32).reshape(1)
        flat = [t[:far].reshape(far, 1, -1) for t in (unit_rel, place_rel, jnp.where(lone_rel, 1.0, weight_rel))]
        sent_here = flat[0] == jnp.arange(units, dtype=F32)[None, :, None]
        notes = jnp.stack([jnp.max(jnp.where(sent_here, flat[1], -1.0), axis=2), jnp.max(jnp.where(sent_here, flat[2], 0.0), axis=2)])
        notes = hop_y(notes)
        sent_place = notes[0].astype(jnp.int32).reshape(far, 1, units)
        sent_weight = notes[1].reshape(far, 1, units)
        own_groups = ids_loc.T[None] // per_group == (grp ^ jnp.arange(groups))[:, None, None]
        own_member = jnp.any(own_groups, axis=1)
        q_cols = jnp.where(own_member, count_earlier(own_member), -1.0).astype(jnp.int32).T
        slots = experts * cap
        tok_cols = tok_rel.astype(jnp.int32).reshape(devices, slots, 1)
        g_cols = weight_rel.reshape(devices, slots, 1)
        spare = ((0, 0), (0, 0), (0, pad - cap))
        q_rows = jnp.pad(place_rel, spare, constant_values=-1.0).astype(jnp.int32).reshape(devices, 1, experts * pad)
        g_rows = jnp.pad(weight_rel, spare).reshape(devices, 1, experts * pad)
        unit_rows = jnp.pad(unit_rel[:far], spare, constant_values=-1.0).astype(jnp.int32).reshape(far, 1, experts * pad)
        form_rows = jnp.pad(jnp.where(lone_rel, weight_rel, 1.0)[:far], spare).reshape(far, 1, experts * pad)

        xs, acts, ds, dh1s, dh3s, y_sums, dx_sums, y_sent, dx_sent = ([None] * 4 for _ in range(9))
        saved = {}
        last = None
        for step, c in KERNEL_ORDER:
            places = q_rows if last is None else after(last, q_rows)
            if step == 'n':
                xs[c], acts[c], ds[c], dh1s[c], dh3s[c], *sums = near_pair(c, *x_pairs[c], *dy_pairs[c], tok_cols, g_cols, places, g_rows, w1, w3, w2, cap, pad, grp_cap)
                y_sums[c], dx_sums[c] = sums[:PAIR], sums[PAIR:]
            elif step == 'm':
                xs[c], acts[c], ds[c], dh1s[c], dh3s[c], *sums = far_both_pair(c, *x_pairs[c], *dy_pairs[c], tok_cols, g_cols, places, g_rows, unit_rows, form_rows, over_flag, w1, w3, w2, cap, pad, grp_cap, units)
                y_sums[c], dx_sums[c], y_sent[c], dx_sent[c] = (sums[k:k + PAIR] for k in range(0, 4 * PAIR, PAIR))
            elif step == 'f':
                xs[c], acts[c], *saved[c], y0, y1, r0, r1 = far_forward_pair(c, *x_pairs[c], tok_cols, places, g_rows, unit_rows, form_rows, over_flag, w1, w3, w2, cap, pad, grp_cap, units)
                y_sums[c], y_sent[c] = (y0, y1), (r0, r1)
            else:
                ds[c], dh1s[c], dh3s[c], z0, z1, r0, r1 = far_backward_pair(c, *dy_pairs[c], tok_cols, g_cols, places, unit_rows, over_flag, w1, w3, w2, *saved[c], cap, pad, grp_cap, units)
                dx_sums[c], dx_sent[c] = (z0, z1), (r0, r1)
            last = (y_sums if step == 'f' else dx_sums)[c][0]

        grads = weight_grads(xs, acts, ds, dh1s, dh3s)

        def combine(results, sent, weighted, split):
            near = [*results[2], *results[3]]
            full = [*results[0], *results[1]]
            arrived = [hop_y(r) for r in (*sent[0], *sent[1])]
            sums = []
            for sources in split:

                def by_rows(ops):
                    return list(merge_sources(sources, ops[0], ops[1], sent_place, sent_weight, weighted))

                def by_sums(ops):
                    return [(n + hop_y(f)).astype(BF) for n, f in zip(ops[0], ops[2])]

                sums += lax.cond(over, by_sums, by_rows, tuple([rows[k] for k in sources] for rows in (near, arrived, full)))
            return [sums[0]] + [hop_g(sums[k], k) for k in (1, 2, 3)]

        y_parts = combine(y_sums, y_sent, True, ((0, 1), (2,), (3,)))
        y_out = collect(y_parts, q_cols)
        dx_parts = combine(dx_sums, dx_sent, False, ((0, 1), (2, 3)))
        dx_out = collect(dx_parts, q_cols)
        return y_out, dx_out, grads[0], grads[1], grads[2]

    return jax.shard_map(device_fn, mesh=mesh, in_specs=(tok_spec, tok_spec, tok_spec, tok_spec, weight_spec, weight_spec, weight_spec), out_specs=(tok_spec, tok_spec, grad_spec, grad_spec, grad_spec), check_vma=False)
```

```python
import functools

import jax
import jax.numpy as jnp
from jax import lax
from jax.experimental import pallas as pl
from jax.experimental.pallas import tpu as pltpu
from jax.sharding import PartitionSpec as P


BF = jnp.bfloat16
F32 = jnp.float32
ALONE = 1024.0
SENT_SHARE = 27, 32
STEP = 2
PAIR = 2

KERNEL_ORDER = (('f', 0), ('b', 0), ('m', 1), ('n', 2), ('n', 3))


def dot(a, b):
    return lax.dot_general(a, b, (((1,), (0,)), ((), ())), preferred_element_type=F32)


def dot_bt(a, b):
    return lax.dot_general(a, b, (((1,), (1,)), ((), ())), preferred_element_type=F32)


def dot_at(a, b):
    return lax.dot_general(a, b, (((0,), (0,)), ((), ())), preferred_element_type=F32)


def pick_rows(tok_col, rows_ref):
    tokens = rows_ref.shape[0]
    lanes = lax.broadcasted_iota(jnp.int32, (tok_col.shape[0], tokens), 1)
    one_hot = jnp.where(tok_col == lanes, 1.0, 0.0).astype(BF)
    return dot(one_hot, rows_ref[...])


def store_by_expert(dst_ref, rows, cap):
    for e in range(dst_ref.shape[0]):
        dst_ref[e] = jnp.concatenate([r[e * cap:(e + 1) * cap] for r in rows], axis=0).astype(BF)


def keep_rows(dst_ref, rows, e, cap, pad):
    zeros = jnp.zeros((pad - cap, rows.shape[1]), F32)
    for s in range(PAIR):
        padded = jnp.concatenate([rows[s * cap:(s + 1) * cap], zeros], axis=0).astype(BF)
        dst_ref[s, pl.ds(pl.multiple_of(e * pad, pad), pad), :] = padded


def spread_rows(dst_ref, tok_ref, row_refs, cap, gcol_ref=None):
    picked = [pick_rows(tok_ref[s], r) for s, r in enumerate(row_refs)]
    if gcol_ref is not None:
        picked = [gcol_ref[s] * p for s, p in enumerate(picked)]
    store_by_expert(dst_ref, picked, cap)


def forward_expert(xg, w1, w3):
    h1 = dot(xg, w1)
    h3 = dot(xg, w3)
    sig = jax.nn.sigmoid(h1)
    silu = h1 * sig
    act = (silu * h3).astype(BF)
    return act, h3 * (sig * (1.0 + h1 * (1.0 - sig))), silu


def mixers(hit, weight):
    if weight is None:
        return [jnp.where(hit, 1.0, 0.0).astype(BF)]
    terms = []
    for _ in range(3):
        part = weight.astype(BF)
        terms.append(jnp.where(hit, part.astype(F32), 0.0).astype(BF))
        weight = weight - part.astype(F32)
    return terms


def weighted_rows(hit, weight, rows):
    total = None
    for term in mixers(hit, weight):
        product = dot(term, rows)
        total = product if total is None else total + product
    return total


def group_sums(p_refs, q_ref, rows_scr, g_ref=None):
    for s, p_ref in enumerate(p_refs):
        slots = lax.broadcasted_iota(jnp.int32, (p_ref.shape[0], q_ref.shape[2]), 0)
        p_ref[...] = weighted_rows(q_ref[s] == slots, None if g_ref is None else g_ref[s], rows_scr[s])


def unit_rows(u_refs, unit_ref, rows_scr, weight_ref=None):
    for s, u_ref in enumerate(u_refs):
        units = lax.broadcasted_iota(jnp.int32, (u_ref.shape[0], unit_ref.shape[2]), 0)
        u_ref[...] = weighted_rows(unit_ref[s] == units, None if weight_ref is None else weight_ref[s], rows_scr[s]).astype(BF)


def far_fwd_kernel(cap, pad, xa_ref, xb_ref, tok_ref, q_ref, g_ref, unit_ref, form_ref, over_ref, w1_ref, w3_ref, w2_ref, xg_ref, a_ref, u_ref, v_ref, p0_ref, p1_ref, r0_ref, r1_ref, xg_scr, o_scr):
    e = pl.program_id(0)

    @pl.when(e == 0)
    def _():
        spread_rows(xg_scr, tok_ref, (xa_ref, xb_ref), cap)

    for k in range(STEP):
        xg_ref[k] = xg_scr[e * STEP + k]
        act, u_ref[k], v_ref[k] = forward_expert(xg_scr[e * STEP + k], w1_ref[k], w3_ref[k])
        a_ref[k] = act
        keep_rows(o_scr, dot(act, w2_ref[k]), e * STEP + k, cap, pad)
    done = e == pl.num_programs(0) - 1

    @pl.when(done & (over_ref[0] == 0))
    def _():
        unit_rows((r0_ref, r1_ref), unit_ref, o_scr, form_ref)

    @pl.when(done & (over_ref[0] != 0))
    def _():
        group_sums((p0_ref, p1_ref), q_ref, o_scr, g_ref)


def far_bwd_kernel(cap, pad, dya_ref, dyb_ref, tok_ref, gcol_ref, q_ref, unit_ref, over_ref, w1_ref, w3_ref, w2_ref, u_ref, v_ref, d_ref, dh1_ref, dh3_ref, p0_ref, p1_ref, r0_ref, r1_ref, d_scr, r_scr):
    e = pl.program_id(0)

    @pl.when(e == 0)
    def _():
        spread_rows(d_scr, tok_ref, (dya_ref, dyb_ref), cap, gcol_ref)

    for k in range(STEP):
        d_ref[k] = d_scr[e * STEP + k]
        da = dot_bt(d_scr[e * STEP + k], w2_ref[k])
        dh1 = (da * u_ref[k]).astype(BF)
        dh3 = (da * v_ref[k]).astype(BF)
        dh1_ref[k] = dh1
        dh3_ref[k] = dh3
        keep_rows(r_scr, dot_bt(dh1, w1_ref[k]) + dot_bt(dh3, w3_ref[k]), e * STEP + k, cap, pad)
    done = e == pl.num_programs(0) - 1

    @pl.when(done & (over_ref[0] == 0))
    def _():
        unit_rows((r0_ref, r1_ref), unit_ref, r_scr)

    @pl.when(done & (over_ref[0] != 0))
    def _():
        group_sums((p0_ref, p1_ref), q_ref, r_scr)


def merge_kernel(weighted, count, *refs):
    near, sent, places, weights, outs = (refs[k * count:(k + 1) * count] for k in range(5))
    mix_ref = refs[5 * count]

    @pl.when(pl.program_id(0) == 0)
    def _():
        for s, (place_ref, weight_ref) in enumerate(zip(places, weights)):
            hit = place_ref[0] == lax.broadcasted_iota(jnp.int32, mix_ref.shape[2:], 0)
            for k, term in enumerate(mixers(hit, weight_ref[0] if weighted else None)):
                mix_ref[s, k] = term

    for s, (n_ref, r_ref, p_ref) in enumerate(zip(near, sent, outs)):
        total = n_ref[...]
        for k in range(mix_ref.shape[1]):
            total = total + dot(mix_ref[s, k], r_ref[...])
        p_ref[...] = total.astype(BF)


def both_ways(cap, pad, step, w1_ref, w3_ref, w2_ref, xg_ref, a_ref, d_ref, dh1_ref, dh3_ref, xg_scr, d_scr, o_scr, r_scr):
    for k in range(STEP):
        e = step * STEP + k
        xg_ref[k] = xg_scr[e]
        d_ref[k] = d_scr[e]
        act, u, v = forward_expert(xg_scr[e], w1_ref[k], w3_ref[k])
        a_ref[k] = act
        keep_rows(o_scr, dot(act, w2_ref[k]), e, cap, pad)
        da = dot_bt(d_scr[e], w2_ref[k])
        dh1 = (da * u).astype(BF)
        dh3 = (da * v).astype(BF)
        dh1_ref[k] = dh1
        dh3_ref[k] = dh3
        keep_rows(r_scr, dot_bt(dh1, w1_ref[k]) + dot_bt(dh3, w3_ref[k]), e, cap, pad)


def near_kernel(cap, pad, xa_ref, xb_ref, dya_ref, dyb_ref, tok_ref, gcol_ref, q_ref, g_ref, w1_ref, w3_ref, w2_ref, xg_ref, a_ref, d_ref, dh1_ref, dh3_ref, y0_ref, y1_ref, z0_ref, z1_ref, xg_scr, d_scr, o_scr, r_scr):
    e = pl.program_id(0)

    @pl.when(e == 0)
    def _():
        spread_rows(xg_scr, tok_ref, (xa_ref, xb_ref), cap)
        spread_rows(d_scr, tok_ref, (dya_ref, dyb_ref), cap, gcol_ref)

    both_ways(cap, pad, e, w1_ref, w3_ref, w2_ref, xg_ref, a_ref, d_ref, dh1_ref, dh3_ref, xg_scr, d_scr, o_scr, r_scr)

    @pl.when(e == pl.num_programs(0) - 1)
    def _():
        group_sums((y0_ref, y1_ref), q_ref, o_scr, g_ref)
        group_sums((z0_ref, z1_ref), q_ref, r_scr)


def far_both_kernel(cap, pad, xa_ref, xb_ref, dya_ref, dyb_ref, tok_ref, gcol_ref, q_ref, g_ref, unit_ref, form_ref, over_ref, w1_ref, w3_ref, w2_ref, xg_ref, a_ref, d_ref, dh1_ref, dh3_ref, y0_ref, y1_ref, z0_ref, z1_ref, ry0_ref, ry1_ref, rz0_ref, rz1_ref, xg_scr, d_scr, o_scr, r_scr):
    e = pl.program_id(0)

    @pl.when(e == 0)
    def _():
        spread_rows(xg_scr, tok_ref, (xa_ref, xb_ref), cap)
        spread_rows(d_scr, tok_ref, (dya_ref, dyb_ref), cap, gcol_ref)

    both_ways(cap, pad, e, w1_ref, w3_ref, w2_ref, xg_ref, a_ref, d_ref, dh1_ref, dh3_ref, xg_scr, d_scr, o_scr, r_scr)
    done = e == pl.num_programs(0) - 1

    @pl.when(done & (over_ref[0] == 0))
    def _():
        unit_rows((ry0_ref, ry1_ref), unit_ref, o_scr, form_ref)
        unit_rows((rz0_ref, rz1_ref), unit_ref, r_scr)

    @pl.when(done & (over_ref[0] != 0))
    def _():
        group_sums((y0_ref, y1_ref), q_ref, o_scr, g_ref)
        group_sums((z0_ref, z1_ref), q_ref, r_scr)


def whole(shape):
    return pl.BlockSpec(shape, lambda e: (0,) * len(shape))


def per_step(shape):
    return pl.BlockSpec((STEP,) + shape[1:], lambda e: (e,) + (0,) * (len(shape) - 1))


def per_expert(shape):
    return pl.BlockSpec((1,) + shape[1:], lambda e: (e,) + (0,) * (len(shape) - 1))


def once(shape):
    return pl.BlockSpec(shape, lambda e: (0,) * len(shape), pipeline_mode=pl.Buffered(1))


def of_pair(pair, shape):
    return pl.BlockSpec((PAIR,) + shape[1:], lambda e: (pair,) + (0,) * (len(shape) - 1), pipeline_mode=pl.Buffered(1))


def params(limit=60 * 1024 * 1024):
    return pltpu.CompilerParams(dimension_semantics=("arbitrary",), vmem_limit_bytes=limit)


def flag():
    return pl.BlockSpec(memory_space=pltpu.SMEM)


def far_forward_pair(pair, xa, xb, tok_col, q_row, g_row, unit_row, form_row, over, w1, w3, w2, cap, pad, grp_cap, units):
    experts, hidden, ff = w1.shape
    rows = PAIR * cap
    part, sent = ((grp_cap, hidden), F32), ((units, hidden), BF)
    outs = [((experts, rows, hidden), BF), ((experts, rows, ff), BF), ((experts, rows, ff), F32), ((experts, rows, ff), F32), part, part, sent, sent]
    tables = [tok_col, q_row, g_row, unit_row, form_row]
    return pl.pallas_call(
        functools.partial(far_fwd_kernel, cap, pad),
        grid=(experts // STEP,),
        in_specs=[once(xa.shape)] * 2 + [of_pair(pair, t.shape) for t in tables] + [flag(), per_step(w1.shape), per_step(w3.shape), per_step(w2.shape)],
        out_specs=[per_step(s) if len(s) == 3 else once(s) for s, _ in outs],
        out_shape=[jax.ShapeDtypeStruct(s, t) for s, t in outs],
        scratch_shapes=[pltpu.VMEM((experts, rows, hidden), BF), pltpu.VMEM((PAIR, experts * pad, hidden), BF)],
        compiler_params=params(67043328),
        cost_estimate=pl.CostEstimate(flops=14 * 10**9, bytes_accessed=50 * 10**6, transcendentals=0),
        name="far_fwd_pair",
    )(xa, xb, *tables, over, w1, w3, w2)


def far_backward_pair(pair, dya, dyb, tok_col, g_col, q_row, unit_row, over, w1, w3, w2, u, v, cap, pad, grp_cap, units):
    experts, hidden, ff = w1.shape
    rows = PAIR * cap
    part, sent = ((grp_cap, hidden), F32), ((units, hidden), BF)
    outs = [((experts, rows, hidden), BF), ((experts, rows, ff), BF), ((experts, rows, ff), BF), part, part, sent, sent]
    tables = [tok_col, g_col, q_row, unit_row]
    return pl.pallas_call(
        functools.partial(far_bwd_kernel, cap, pad),
        grid=(experts // STEP,),
        in_specs=[once(dya.shape)] * 2 + [of_pair(pair, t.shape) for t in tables] + [flag(), per_step(w1.shape), per_step(w3.shape), per_step(w2.shape), per_step(u.shape), per_step(v.shape)],
        out_specs=[per_step(s) if len(s) == 3 else once(s) for s, _ in outs],
        out_shape=[jax.ShapeDtypeStruct(s, t) for s, t in outs],
        scratch_shapes=[pltpu.VMEM((experts, rows, hidden), BF), pltpu.VMEM((PAIR, experts * pad, hidden), BF)],
        compiler_params=params(67043328),
        cost_estimate=pl.CostEstimate(flops=14 * 10**9, bytes_accessed=50 * 10**6, transcendentals=0),
        name="far_bwd_pair",
    )(dya, dyb, *tables, over, w1, w3, w2, u, v)


def far_both_pair(pair, xa, xb, dya, dyb, tok_col, g_col, q_row, g_row, unit_row, form_row, over, w1, w3, w2, cap, pad, grp_cap, units):
    experts, hidden, ff = w1.shape
    rows = PAIR * cap
    wide, narrow, part, sent = ((experts, rows, hidden), BF), ((experts, rows, ff), BF), ((grp_cap, hidden), F32), ((units, hidden), BF)
    outs = [wide, narrow, wide, narrow, narrow] + [part] * 4 + [sent] * 4
    tables = [tok_col, g_col, q_row, g_row, unit_row, form_row]
    return pl.pallas_call(
        functools.partial(far_both_kernel, cap, pad),
        grid=(experts // STEP,),
        in_specs=[once(xa.shape)] * 4 + [of_pair(pair, t.shape) for t in tables] + [flag(), per_step(w1.shape), per_step(w3.shape), per_step(w2.shape)],
        out_specs=[per_step(s) if len(s) == 3 else once(s) for s, _ in outs],
        out_shape=[jax.ShapeDtypeStruct(s, t) for s, t in outs],
        scratch_shapes=[pltpu.VMEM((experts, rows, hidden), BF)] * 2 + [pltpu.VMEM((PAIR, experts * pad, hidden), BF)] * 2,
        compiler_params=params(67043328),
        cost_estimate=pl.CostEstimate(flops=28 * 10**9, bytes_accessed=70 * 10**6, transcendentals=0),
        name="far_both_pair",
    )(xa, xb, dya, dyb, *tables, over, w1, w3, w2)


def merge_sources(sources, near, sent, place, weight, weighted):
    grp_cap, hidden = near[0].shape
    units, count = sent[0].shape[0], len(sources)
    block = hidden // 3
    notes = [pl.BlockSpec((1, 1, units), functools.partial(lambda k, n: (k, 0, 0), k)) for k in sources]
    return pl.pallas_call(
        functools.partial(merge_kernel, weighted, count),
        grid=(3,),
        in_specs=[pl.BlockSpec((grp_cap, block), lambda n: (0, n))] * count + [pl.BlockSpec((units, block), lambda n: (0, n))] * count + notes * 2,
        out_specs=[pl.BlockSpec((grp_cap, block), lambda n: (0, n))] * count,
        out_shape=[jax.ShapeDtypeStruct((grp_cap, hidden), BF)] * count,
        scratch_shapes=[pltpu.VMEM((count, 3 if weighted else 1, grp_cap, units), BF)],
        compiler_params=params(),
        cost_estimate=pl.CostEstimate(flops=count * 10**9, bytes_accessed=count * 4 * 10**6, transcendentals=0),
        name="merge_sources",
    )(*near, *sent, *[place] * count, *[weight] * count)


def near_pair(pair, xa, xb, dya, dyb, tok_col, g_col, q_row, g_row, w1, w3, w2, cap, pad, grp_cap):
    experts, hidden, ff = w1.shape
    rows = PAIR * cap
    wide, narrow, part = ((experts, rows, hidden), BF), ((experts, rows, ff), BF), ((grp_cap, hidden), F32)
    outs = [wide, narrow, wide, narrow, narrow, part, part, part, part]
    tables = [tok_col, g_col, q_row, g_row]
    return pl.pallas_call(
        functools.partial(near_kernel, cap, pad),
        grid=(experts // STEP,),
        in_specs=[once(xa.shape)] * 4 + [of_pair(pair, t.shape) for t in tables] + [per_step(w1.shape), per_step(w3.shape), per_step(w2.shape)],
        out_specs=[per_step(s) if len(s) == 3 else once(s) for s, _ in outs],
        out_shape=[jax.ShapeDtypeStruct(s, t) for s, t in outs],
        scratch_shapes=[pltpu.VMEM((experts, rows, hidden), BF)] * 2 + [pltpu.VMEM((PAIR, experts * pad, hidden), BF)] * 2,
        compiler_params=params(67043328),
        cost_estimate=pl.CostEstimate(flops=28 * 10**9, bytes_accessed=70 * 10**6, transcendentals=0),
        name="near_pair",
    )(xa, xb, dya, dyb, *tables, w1, w3, w2)


def dw_kernel(chunks, *refs):
    ins, (g1_ref, g3_ref, g2_ref) = refs[:5 * chunks], refs[5 * chunks:]

    def joined(k):
        return jnp.concatenate([ins[k * chunks + c][0] for c in range(chunks)], axis=0)

    x, a, d, dh1, dh3 = (joined(k) for k in range(5))
    g1_ref[0] = dot_at(x, dh1)
    g3_ref[0] = dot_at(x, dh3)
    g2_ref[0] = dot_at(a, d)


def weight_grads(xs, acts, ds, dh1s, dh3s):
    chunks = len(xs)
    experts, _, hidden = xs[0].shape
    ff = acts[0].shape[2]
    args = [*xs, *acts, *ds, *dh1s, *dh3s]
    outs = [(experts, hidden, ff), (experts, hidden, ff), (experts, ff, hidden)]
    return pl.pallas_call(
        functools.partial(dw_kernel, chunks),
        grid=(experts,),
        in_specs=[per_expert(a.shape) for a in args],
        out_specs=[per_expert(s) for s in outs],
        out_shape=[jax.ShapeDtypeStruct(s, F32) for s in outs],
        compiler_params=params(),
        cost_estimate=pl.CostEstimate(flops=25 * 10**9, bytes_accessed=120 * 10**6, transcendentals=0),
        name="weight_grads",
    )(*args)


def final_kernel(groups, *refs):
    q_ref, out_ref = refs[groups], refs[groups + 1]
    total = None
    for h in range(groups):
        lanes = lax.broadcasted_iota(jnp.int32, (out_ref.shape[0], refs[h].shape[0]), 1)
        one_hot = jnp.where(q_ref[:, h:h + 1] == lanes, 1.0, 0.0).astype(BF)
        term = dot(one_hot, refs[h][...])
        total = term if total is None else total + term
    out_ref[...] = total.astype(BF)


def collect(parts, q_cols):
    groups = len(parts)
    tokens = q_cols.shape[0]
    hidden = parts[0].shape[1]
    block = tokens // 4
    return pl.pallas_call(
        functools.partial(final_kernel, groups),
        grid=(4,),
        in_specs=[whole(p.shape) for p in parts] + [pl.BlockSpec((block, groups), lambda e: (e, 0))],
        out_specs=pl.BlockSpec((block, hidden), lambda e: (e, 0)),
        out_shape=jax.ShapeDtypeStruct((tokens, hidden), BF),
        compiler_params=params(),
        cost_estimate=pl.CostEstimate(flops=2 * 10**9, bytes_accessed=5 * 10**6, transcendentals=0),
        name="collect",
    )(*parts, q_cols)


def after(earlier, value):
    return lax.optimization_barrier((earlier, value))[1]


def slot_tables(ids, gates, first_exp, experts, group, per_group, cap):
    sources, _, tokens = ids.shape
    eq = ids[:, None] == (first_exp + jnp.arange(experts))[None, :, None, None]
    hit = jnp.any(eq, axis=2)
    gate = jnp.sum(jnp.where(eq, gates[:, None], 0.0), axis=2)
    member = jnp.any(ids // per_group == group, axis=1, keepdims=True)
    pos = count_earlier(jnp.concatenate([hit, member], axis=1).reshape(sources * (experts + 1), tokens))
    pos = pos.reshape(sources, experts + 1, tokens)
    exp_pos, grp_pos = pos[:, :experts], pos[:, experts:]
    taken = hit[:, :, None, :] & (exp_pos[:, :, None, :] == jnp.arange(cap, dtype=F32)[None, None, :, None])
    numbers = jnp.arange(1, tokens + 1, dtype=F32)[None, None, None, :]
    tok = jnp.sum(jnp.where(taken, numbers, 0.0), axis=3) - 1.0
    place = jnp.sum(jnp.where(taken, grp_pos[:, :, None, :] + 1.0, 0.0), axis=3) - 1.0
    weight = jnp.sum(jnp.where(taken, gate[:, :, None, :], 0.0), axis=3)
    here = jnp.sum(hit, axis=1).astype(F32)
    alone = here == jnp.sum(ids // per_group == group, axis=1).astype(F32)
    first = count_earlier(jnp.where(alone, jnp.minimum(here, 1.0), here))
    rank, seen = [], jnp.zeros((sources, tokens), F32)
    for e in range(experts):
        rank.append(seen)
        seen = seen + hit[:, e].astype(F32)
    unit = first[:, None] + jnp.where(alone[:, None], ALONE, jnp.stack(rank, axis=1)) + 1.0
    code = jnp.sum(jnp.where(taken, unit[:, :, None, :], 0.0), axis=3)
    lone = code > ALONE
    return tok, place, weight, jnp.where(lone, code - ALONE, code) - 1.0, lone


def longest_list(ids, per_group, experts, away):
    devices = away.shape[1]
    count = jnp.sum(ids[:, None] // experts == jnp.arange(devices)[None, :, None, None], axis=2)
    half = per_group // experts
    in_group = jnp.repeat(jnp.sum(count.reshape(ids.shape[0], devices // half, half, -1), axis=2), half, axis=1)
    rows = jnp.where(count == in_group, jnp.minimum(count, 1), count)
    return jnp.max(jnp.where(away, jnp.sum(rows, axis=2), 0))


def count_earlier(marks):
    tokens = marks.shape[1]
    earlier = (jnp.arange(tokens)[:, None] < jnp.arange(tokens)[None, :]).astype(BF)
    return jnp.dot(marks.astype(BF), earlier, preferred_element_type=F32)


def solution(mesh):
    groups = mesh.shape['grp']
    inner = mesh.shape['ing']
    devices = groups * inner
    tok_spec = P(('dp', 'grp', 'ing'), None)
    weight_spec = P(('grp', 'ing'), None, None)
    grad_spec = P(('dp', 'grp', 'ing'), None, None)

    def hop_y(a):
        return lax.ppermute(a, 'ing', [(0, 1), (1, 0)])

    def hop_g(a, bits):
        return lax.ppermute(a, 'grp', [(g, g ^ bits) for g in range(groups)])

    def device_fn(x_loc, ids_loc, gates_loc, dy_loc, w1, w3, w2):
        tokens, _ = x_loc.shape
        top_k = ids_loc.shape[1]
        experts = w1.shape[0]
        num_exp = experts * devices
        grp_cap = tokens * 2 // groups
        cap = 3 * tokens * top_k // (2 * num_exp)
        pad = -(-cap // 16) * 16
        grp, ing = lax.axis_index('grp'), lax.axis_index('ing')

        per_group = experts * inner
        own = jnp.concatenate([ids_loc.T.astype(F32), gates_loc.T], axis=0)[None]
        pair = jnp.concatenate([own, hop_y(own)], axis=0)
        pair_c = hop_g(pair, 1)
        quad_x = hop_g(jnp.concatenate([pair, pair_c], axis=0), 2)
        routing = jnp.stack([pair[1], pair_c[1], quad_x[1], quad_x[3], pair[0], pair_c[0], quad_x[0], quad_x[2]])

        x_far = hop_y(x_loc)
        dy_far = hop_y(dy_loc)
        x_near_c = hop_g(after(pair_c, x_loc), 1)
        x_near_x = hop_g(x_loc, 2)
        dy_near_c = hop_g(after(x_near_c, dy_loc), 1)
        x_far_c, x_far_x = hop_g(x_far, 1), hop_g(x_far, 2)
        x_near_xc, x_far_xc = hop_g(x_near_x, 1), hop_g(x_far_x, 1)
        dy_far_c, dy_far_x = hop_g(dy_far, 1), hop_g(dy_far, 2)
        dy_far_xc = hop_g(dy_far_x, 1)
        dy_near_x = hop_g(dy_loc, 2)
        dy_near_xc = hop_g(dy_near_x, 1)
        x_pairs = [(x_far, x_far_c), (x_far_x, x_far_xc), (x_loc, x_near_c), (x_near_x, x_near_xc)]
        dy_pairs = [(dy_far, dy_far_c), (dy_far_x, dy_far_xc), (dy_loc, dy_near_c), (dy_near_x, dy_near_xc)]

        ids_rel, gates_rel = routing[:, :top_k].astype(jnp.int32), routing[:, top_k:]
        units = tokens * SENT_SHARE[0] // SENT_SHARE[1]
        tok_rel, place_rel, weight_rel, unit_rel, lone_rel = slot_tables(ids_rel, gates_rel, (grp * inner + ing) * experts, experts, grp, per_group, cap)
        far = devices // 2
        source_ing = jnp.where(jnp.arange(devices) < far, 1 - ing, ing)
        away = source_ing[:, None] != (jnp.arange(devices) % inner)[None, :]
        over = longest_list(ids_rel, per_group, experts, away) > units
        over_flag = over.astype(jnp.int32).reshape(1)
        flat = [t[:far].reshape(far, 1, -1) for t in (unit_rel, place_rel, jnp.where(lone_rel, 1.0, weight_rel))]
        sent_here = flat[0] == jnp.arange(units, dtype=F32)[None, :, None]
        notes = jnp.stack([jnp.max(jnp.where(sent_here, flat[1], -1.0), axis=2), jnp.max(jnp.where(sent_here, flat[2], 0.0), axis=2)])
        notes = hop_y(notes)
        sent_place = notes[0].astype(jnp.int32).reshape(far, 1, units)
        sent_weight = notes[1].reshape(far, 1, units)
        own_groups = ids_loc.T[None] // per_group == (grp ^ jnp.arange(groups))[:, None, None]
        own_member = jnp.any(own_groups, axis=1)
        q_cols = jnp.where(own_member, count_earlier(own_member), -1.0).astype(jnp.int32).T
        slots = experts * cap
        tok_cols = tok_rel.astype(jnp.int32).reshape(devices, slots, 1)
        g_cols = weight_rel.reshape(devices, slots, 1)
        spare = ((0, 0), (0, 0), (0, pad - cap))
        q_rows = jnp.pad(place_rel, spare, constant_values=-1.0).astype(jnp.int32).reshape(devices, 1, experts * pad)
        g_rows = jnp.pad(weight_rel, spare).reshape(devices, 1, experts * pad)
        unit_rows = jnp.pad(unit_rel[:far], spare, constant_values=-1.0).astype(jnp.int32).reshape(far, 1, experts * pad)
        form_rows = jnp.pad(jnp.where(lone_rel, weight_rel, 1.0)[:far], spare).reshape(far, 1, experts * pad)

        xs, acts, ds, dh1s, dh3s, y_sums, dx_sums, y_sent, dx_sent = ([None] * 4 for _ in range(9))
        saved = {}
        last = None
        for step, c in KERNEL_ORDER:
            places = q_rows if last is None else after(last, q_rows)
            if step == 'n':
                xs[c], acts[c], ds[c], dh1s[c], dh3s[c], *sums = near_pair(c, *x_pairs[c], *dy_pairs[c], tok_cols, g_cols, places, g_rows, w1, w3, w2, cap, pad, grp_cap)
                y_sums[c], dx_sums[c] = sums[:PAIR], sums[PAIR:]
            elif step == 'm':
                xs[c], acts[c], ds[c], dh1s[c], dh3s[c], *sums = far_both_pair(c, *x_pairs[c], *dy_pairs[c], tok_cols, g_cols, places, g_rows, unit_rows, form_rows, over_flag, w1, w3, w2, cap, pad, grp_cap, units)
                y_sums[c], dx_sums[c], y_sent[c], dx_sent[c] = (sums[k:k + PAIR] for k in range(0, 4 * PAIR, PAIR))
            elif step == 'f':
                xs[c], acts[c], *saved[c], y0, y1, r0, r1 = far_forward_pair(c, *x_pairs[c], tok_cols, places, g_rows, unit_rows, form_rows, over_flag, w1, w3, w2, cap, pad, grp_cap, units)
                y_sums[c], y_sent[c] = (y0, y1), (r0, r1)
            else:
                ds[c], dh1s[c], dh3s[c], z0, z1, r0, r1 = far_backward_pair(c, *dy_pairs[c], tok_cols, g_cols, places, unit_rows, over_flag, w1, w3, w2, *saved[c], cap, pad, grp_cap, units)
                dx_sums[c], dx_sent[c] = (z0, z1), (r0, r1)
            last = (y_sums if step == 'f' else dx_sums)[c][0]

        grads = weight_grads(xs, acts, ds, dh1s, dh3s)

        def combine(results, sent, weighted, split):
            near = [*results[2], *results[3]]
            full = [*results[0], *results[1]]
            arrived = [hop_y(r) for r in (*sent[0], *sent[1])]
            sums = []
            for sources in split:

                def by_rows(ops):
                    return list(merge_sources(sources, ops[0], ops[1], sent_place, sent_weight, weighted))

                def by_sums(ops):
                    return [(n + hop_y(f)).astype(BF) for n, f in zip(ops[0], ops[2])]

                sums += lax.cond(over, by_sums, by_rows, tuple([rows[k] for k in sources] for rows in (near, arrived, full)))
            return [sums[0]] + [hop_g(sums[k], k) for k in (1, 2, 3)]

        y_parts = combine(y_sums, y_sent, True, ((0, 1), (2,), (3,)))
        y_out = collect(y_parts, q_cols)
        dx_parts = combine(dx_sums, dx_sent, False, ((0, 1), (2, 3)))
        dx_out = collect(dx_parts, q_cols)
        return y_out, dx_out, grads[0], grads[1], grads[2]

    return jax.shard_map(device_fn, mesh=mesh, in_specs=(tok_spec, tok_spec, tok_spec, tok_spec, weight_spec, weight_spec, weight_spec), out_specs=(tok_spec, tok_spec, grad_spec, grad_spec, grad_spec), check_vma=False)
```

```python
import functools

import jax
import jax.numpy as jnp
from jax import lax
from jax.experimental import pallas as pl
from jax.experimental.pallas import tpu as pltpu
from jax.sharding import PartitionSpec as P


BF = jnp.bfloat16
F32 = jnp.float32
ALONE = 1024.0
SENT_SHARE = 27, 32
PAIR = 2

KERNEL_ORDER = (('f', 0), ('b', 0), ('m', 1), ('n', 2), ('n', 3))


def dot(a, b):
    return lax.dot_general(a, b, (((1,), (0,)), ((), ())), preferred_element_type=F32)


def dot_bt(a, b):
    return lax.dot_general(a, b, (((1,), (1,)), ((), ())), preferred_element_type=F32)


def dot_at(a, b):
    return lax.dot_general(a, b, (((0,), (0,)), ((), ())), preferred_element_type=F32)


def pick_rows(tok_col, rows_ref):
    tokens = rows_ref.shape[0]
    lanes = lax.broadcasted_iota(jnp.int32, (tok_col.shape[0], tokens), 1)
    one_hot = jnp.where(tok_col == lanes, 1.0, 0.0).astype(BF)
    return dot(one_hot, rows_ref[...])


def store_by_expert(dst_ref, rows, cap):
    for e in range(dst_ref.shape[0]):
        dst_ref[e] = jnp.concatenate([r[e * cap:(e + 1) * cap] for r in rows], axis=0).astype(BF)


def keep_rows(dst_ref, rows, e, cap, pad):
    zeros = jnp.zeros((pad - cap, rows.shape[1]), F32)
    for s in range(PAIR):
        padded = jnp.concatenate([rows[s * cap:(s + 1) * cap], zeros], axis=0).astype(BF)
        dst_ref[s, pl.ds(pl.multiple_of(e * pad, pad), pad), :] = padded


def spread_rows(dst_ref, tok_ref, row_refs, cap, gcol_ref=None):
    picked = [pick_rows(tok_ref[s], r) for s, r in enumerate(row_refs)]
    if gcol_ref is not None:
        picked = [gcol_ref[s] * p for s, p in enumerate(picked)]
    store_by_expert(dst_ref, picked, cap)


def forward_expert(xg, w1_ref, w3_ref):
    h1 = dot(xg, w1_ref[0])
    h3 = dot(xg, w3_ref[0])
    sig = jax.nn.sigmoid(h1)
    silu = h1 * sig
    act = (silu * h3).astype(BF)
    return act, h3 * (sig * (1.0 + h1 * (1.0 - sig))), silu


def mixers(hit, weight):
    if weight is None:
        return [jnp.where(hit, 1.0, 0.0).astype(BF)]
    terms = []
    for _ in range(3):
        part = weight.astype(BF)
        terms.append(jnp.where(hit, part.astype(F32), 0.0).astype(BF))
        weight = weight - part.astype(F32)
    return terms


def weighted_rows(hit, weight, rows):
    total = None
    for term in mixers(hit, weight):
        product = dot(term, rows)
        total = product if total is None else total + product
    return total


def group_sums(p_refs, q_ref, rows_scr, g_ref=None):
    for s, p_ref in enumerate(p_refs):
        slots = lax.broadcasted_iota(jnp.int32, (p_ref.shape[0], q_ref.shape[2]), 0)
        p_ref[...] = weighted_rows(q_ref[s] == slots, None if g_ref is None else g_ref[s], rows_scr[s])


def unit_rows(u_refs, unit_ref, rows_scr, weight_ref=None):
    for s, u_ref in enumerate(u_refs):
        units = lax.broadcasted_iota(jnp.int32, (u_ref.shape[0], unit_ref.shape[2]), 0)
        u_ref[...] = weighted_rows(unit_ref[s] == units, None if weight_ref is None else weight_ref[s], rows_scr[s]).astype(BF)


def far_fwd_kernel(cap, pad, xa_ref, xb_ref, tok_ref, q_ref, g_ref, unit_ref, form_ref, over_ref, w1_ref, w3_ref, w2_ref, xg_ref, a_ref, u_ref, v_ref, p0_ref, p1_ref, r0_ref, r1_ref, xg_scr, o_scr):
    e = pl.program_id(0)

    @pl.when(e == 0)
    def _():
        spread_rows(xg_scr, tok_ref, (xa_ref, xb_ref), cap)

    xg_ref[0] = xg_scr[e]
    act, u_ref[0], v_ref[0] = forward_expert(xg_scr[e], w1_ref, w3_ref)
    a_ref[0] = act
    keep_rows(o_scr, dot(act, w2_ref[0]), e, cap, pad)
    done = e == pl.num_programs(0) - 1

    @pl.when(done & (over_ref[0] == 0))
    def _():
        unit_rows((r0_ref, r1_ref), unit_ref, o_scr, form_ref)

    @pl.when(done & (over_ref[0] != 0))
    def _():
        group_sums((p0_ref, p1_ref), q_ref, o_scr, g_ref)


def far_bwd_kernel(cap, pad, dya_ref, dyb_ref, tok_ref, gcol_ref, q_ref, unit_ref, over_ref, w1_ref, w3_ref, w2_ref, u_ref, v_ref, d_ref, dh1_ref, dh3_ref, p0_ref, p1_ref, r0_ref, r1_ref, d_scr, r_scr):
    e = pl.program_id(0)

    @pl.when(e == 0)
    def _():
        spread_rows(d_scr, tok_ref, (dya_ref, dyb_ref), cap, gcol_ref)

    d_ref[0] = d_scr[e]
    da = dot_bt(d_scr[e], w2_ref[0])
    dh1 = (da * u_ref[0]).astype(BF)
    dh3 = (da * v_ref[0]).astype(BF)
    dh1_ref[0] = dh1
    dh3_ref[0] = dh3
    keep_rows(r_scr, dot_bt(dh1, w1_ref[0]) + dot_bt(dh3, w3_ref[0]), e, cap, pad)
    done = e == pl.num_programs(0) - 1

    @pl.when(done & (over_ref[0] == 0))
    def _():
        unit_rows((r0_ref, r1_ref), unit_ref, r_scr)

    @pl.when(done & (over_ref[0] != 0))
    def _():
        group_sums((p0_ref, p1_ref), q_ref, r_scr)


def merge_kernel(weighted, count, *refs):
    near, sent, places, weights, outs = (refs[k * count:(k + 1) * count] for k in range(5))
    mix_ref = refs[5 * count]

    @pl.when(pl.program_id(0) == 0)
    def _():
        for s, (place_ref, weight_ref) in enumerate(zip(places, weights)):
            hit = place_ref[0] == lax.broadcasted_iota(jnp.int32, mix_ref.shape[2:], 0)
            for k, term in enumerate(mixers(hit, weight_ref[0] if weighted else None)):
                mix_ref[s, k] = term

    for s, (n_ref, r_ref, p_ref) in enumerate(zip(near, sent, outs)):
        total = n_ref[...]
        for k in range(mix_ref.shape[1]):
            total = total + dot(mix_ref[s, k], r_ref[...])
        p_ref[...] = total.astype(BF)


def both_ways(cap, pad, e, w1_ref, w3_ref, w2_ref, xg_ref, a_ref, d_ref, dh1_ref, dh3_ref, xg_scr, d_scr, o_scr, r_scr):
    xg_ref[0] = xg_scr[e]
    d_ref[0] = d_scr[e]
    act, u, v = forward_expert(xg_scr[e], w1_ref, w3_ref)
    a_ref[0] = act
    keep_rows(o_scr, dot(act, w2_ref[0]), e, cap, pad)
    da = dot_bt(d_scr[e], w2_ref[0])
    dh1 = (da * u).astype(BF)
    dh3 = (da * v).astype(BF)
    dh1_ref[0] = dh1
    dh3_ref[0] = dh3
    keep_rows(r_scr, dot_bt(dh1, w1_ref[0]) + dot_bt(dh3, w3_ref[0]), e, cap, pad)


def near_kernel(cap, pad, xa_ref, xb_ref, dya_ref, dyb_ref, tok_ref, gcol_ref, q_ref, g_ref, w1_ref, w3_ref, w2_ref, xg_ref, a_ref, d_ref, dh1_ref, dh3_ref, y0_ref, y1_ref, z0_ref, z1_ref, xg_scr, d_scr, o_scr, r_scr):
    e = pl.program_id(0)

    @pl.when(e == 0)
    def _():
        spread_rows(xg_scr, tok_ref, (xa_ref, xb_ref), cap)
        spread_rows(d_scr, tok_ref, (dya_ref, dyb_ref), cap, gcol_ref)

    both_ways(cap, pad, e, w1_ref, w3_ref, w2_ref, xg_ref, a_ref, d_ref, dh1_ref, dh3_ref, xg_scr, d_scr, o_scr, r_scr)

    @pl.when(e == pl.num_programs(0) - 1)
    def _():
        group_sums((y0_ref, y1_ref), q_ref, o_scr, g_ref)
        group_sums((z0_ref, z1_ref), q_ref, r_scr)


def far_both_kernel(cap, pad, xa_ref, xb_ref, dya_ref, dyb_ref, tok_ref, gcol_ref, q_ref, g_ref, unit_ref, form_ref, over_ref, w1_ref, w3_ref, w2_ref, xg_ref, a_ref, d_ref, dh1_ref, dh3_ref, y0_ref, y1_ref, z0_ref, z1_ref, ry0_ref, ry1_ref, rz0_ref, rz1_ref, xg_scr, d_scr, o_scr, r_scr):
    e = pl.program_id(0)

    @pl.when(e == 0)
    def _():
        spread_rows(xg_scr, tok_ref, (xa_ref, xb_ref), cap)
        spread_rows(d_scr, tok_ref, (dya_ref, dyb_ref), cap, gcol_ref)

    both_ways(cap, pad, e, w1_ref, w3_ref, w2_ref, xg_ref, a_ref, d_ref, dh1_ref, dh3_ref, xg_scr, d_scr, o_scr, r_scr)
    done = e == pl.num_programs(0) - 1

    @pl.when(done & (over_ref[0] == 0))
    def _():
        unit_rows((ry0_ref, ry1_ref), unit_ref, o_scr, form_ref)
        unit_rows((rz0_ref, rz1_ref), unit_ref, r_scr)

    @pl.when(done & (over_ref[0] != 0))
    def _():
        group_sums((y0_ref, y1_ref), q_ref, o_scr, g_ref)
        group_sums((z0_ref, z1_ref), q_ref, r_scr)


def whole(shape):
    return pl.BlockSpec(shape, lambda e: (0,) * len(shape))


def per_expert(shape):
    return pl.BlockSpec((1,) + shape[1:], lambda e: (e,) + (0,) * (len(shape) - 1))


def once(shape):
    return pl.BlockSpec(shape, lambda e: (0,) * len(shape), pipeline_mode=pl.Buffered(1))


def of_pair(pair, shape):
    return pl.BlockSpec((PAIR,) + shape[1:], lambda e: (pair,) + (0,) * (len(shape) - 1))


def params():
    return pltpu.CompilerParams(dimension_semantics=("arbitrary",), vmem_limit_bytes=60 * 1024 * 1024)


def flag():
    return pl.BlockSpec(memory_space=pltpu.SMEM)


def far_forward_pair(pair, xa, xb, tok_col, q_row, g_row, unit_row, form_row, over, w1, w3, w2, cap, pad, grp_cap, units):
    experts, hidden, ff = w1.shape
    rows = PAIR * cap
    part, sent = ((grp_cap, hidden), F32), ((units, hidden), BF)
    outs = [((experts, rows, hidden), BF), ((experts, rows, ff), BF), ((experts, rows, ff), F32), ((experts, rows, ff), F32), part, part, sent, sent]
    tables = [tok_col, q_row, g_row, unit_row, form_row]
    return pl.pallas_call(
        functools.partial(far_fwd_kernel, cap, pad),
        grid=(experts,),
        in_specs=[whole(xa.shape), whole(xb.shape)] + [of_pair(pair, t.shape) for t in tables] + [flag(), per_expert(w1.shape), per_expert(w3.shape), per_expert(w2.shape)],
        out_specs=[per_expert(s) if len(s) == 3 else whole(s) for s, _ in outs],
        out_shape=[jax.ShapeDtypeStruct(s, t) for s, t in outs],
        scratch_shapes=[pltpu.VMEM((experts, rows, hidden), BF), pltpu.VMEM((PAIR, experts * pad, hidden), BF)],
        compiler_params=params(),
        cost_estimate=pl.CostEstimate(flops=14 * 10**9, bytes_accessed=50 * 10**6, transcendentals=0),
        name="far_fwd_pair",
    )(xa, xb, *tables, over, w1, w3, w2)


def far_backward_pair(pair, dya, dyb, tok_col, g_col, q_row, unit_row, over, w1, w3, w2, u, v, cap, pad, grp_cap, units):
    experts, hidden, ff = w1.shape
    rows = PAIR * cap
    part, sent = ((grp_cap, hidden), F32), ((units, hidden), BF)
    outs = [((experts, rows, hidden), BF), ((experts, rows, ff), BF), ((experts, rows, ff), BF), part, part, sent, sent]
    tables = [tok_col, g_col, q_row, unit_row]
    return pl.pallas_call(
        functools.partial(far_bwd_kernel, cap, pad),
        grid=(experts,),
        in_specs=[whole(dya.shape), whole(dyb.shape)] + [of_pair(pair, t.shape) for t in tables] + [flag(), per_expert(w1.shape), per_expert(w3.shape), per_expert(w2.shape), per_expert(u.shape), per_expert(v.shape)],
        out_specs=[per_expert(s) if len(s) == 3 else whole(s) for s, _ in outs],
        out_shape=[jax.ShapeDtypeStruct(s, t) for s, t in outs],
        scratch_shapes=[pltpu.VMEM((experts, rows, hidden), BF), pltpu.VMEM((PAIR, experts * pad, hidden), BF)],
        compiler_params=params(),
        cost_estimate=pl.CostEstimate(flops=14 * 10**9, bytes_accessed=50 * 10**6, transcendentals=0),
        name="far_bwd_pair",
    )(dya, dyb, *tables, over, w1, w3, w2, u, v)


def far_both_pair(pair, xa, xb, dya, dyb, tok_col, g_col, q_row, g_row, unit_row, form_row, over, w1, w3, w2, cap, pad, grp_cap, units):
    experts, hidden, ff = w1.shape
    rows = PAIR * cap
    wide, narrow, part, sent = ((experts, rows, hidden), BF), ((experts, rows, ff), BF), ((grp_cap, hidden), F32), ((units, hidden), BF)
    outs = [wide, narrow, wide, narrow, narrow] + [part] * 4 + [sent] * 4
    tables = [tok_col, g_col, q_row, g_row, unit_row, form_row]
    return pl.pallas_call(
        functools.partial(far_both_kernel, cap, pad),
        grid=(experts,),
        in_specs=[once(xa.shape)] * 4 + [of_pair(pair, t.shape) for t in tables] + [flag(), per_expert(w1.shape), per_expert(w3.shape), per_expert(w2.shape)],
        out_specs=[per_expert(s) if len(s) == 3 else once(s) for s, _ in outs],
        out_shape=[jax.ShapeDtypeStruct(s, t) for s, t in outs],
        scratch_shapes=[pltpu.VMEM((experts, rows, hidden), BF)] * 2 + [pltpu.VMEM((PAIR, experts * pad, hidden), BF)] * 2,
        compiler_params=params(),
        cost_estimate=pl.CostEstimate(flops=28 * 10**9, bytes_accessed=70 * 10**6, transcendentals=0),
        name="far_both_pair",
    )(xa, xb, dya, dyb, *tables, over, w1, w3, w2)


def merge_sources(sources, near, sent, place, weight, weighted):
    grp_cap, hidden = near[0].shape
    units, count = sent[0].shape[0], len(sources)
    block = hidden // 3
    notes = [pl.BlockSpec((1, 1, units), functools.partial(lambda k, n: (k, 0, 0), k)) for k in sources]
    return pl.pallas_call(
        functools.partial(merge_kernel, weighted, count),
        grid=(3,),
        in_specs=[pl.BlockSpec((grp_cap, block), lambda n: (0, n))] * count + [pl.BlockSpec((units, block), lambda n: (0, n))] * count + notes * 2,
        out_specs=[pl.BlockSpec((grp_cap, block), lambda n: (0, n))] * count,
        out_shape=[jax.ShapeDtypeStruct((grp_cap, hidden), BF)] * count,
        scratch_shapes=[pltpu.VMEM((count, 3 if weighted else 1, grp_cap, units), BF)],
        compiler_params=params(),
        cost_estimate=pl.CostEstimate(flops=count * 10**9, bytes_accessed=count * 4 * 10**6, transcendentals=0),
        name="merge_sources",
    )(*near, *sent, *[place] * count, *[weight] * count)


def near_pair(pair, xa, xb, dya, dyb, tok_col, g_col, q_row, g_row, w1, w3, w2, cap, pad, grp_cap):
    experts, hidden, ff = w1.shape
    rows = PAIR * cap
    wide, narrow, part = ((experts, rows, hidden), BF), ((experts, rows, ff), BF), ((grp_cap, hidden), F32)
    outs = [wide, narrow, wide, narrow, narrow, part, part, part, part]
    tables = [tok_col, g_col, q_row, g_row]
    return pl.pallas_call(
        functools.partial(near_kernel, cap, pad),
        grid=(experts,),
        in_specs=[once(xa.shape)] * 4 + [of_pair(pair, t.shape) for t in tables] + [per_expert(w1.shape), per_expert(w3.shape), per_expert(w2.shape)],
        out_specs=[per_expert(s) if len(s) == 3 else whole(s) for s, _ in outs],
        out_shape=[jax.ShapeDtypeStruct(s, t) for s, t in outs],
        scratch_shapes=[pltpu.VMEM((experts, rows, hidden), BF)] * 2 + [pltpu.VMEM((PAIR, experts * pad, hidden), BF)] * 2,
        compiler_params=params(),
        cost_estimate=pl.CostEstimate(flops=28 * 10**9, bytes_accessed=70 * 10**6, transcendentals=0),
        name="near_pair",
    )(xa, xb, dya, dyb, *tables, w1, w3, w2)


def dw_kernel(chunks, *refs):
    ins, (g1_ref, g3_ref, g2_ref) = refs[:5 * chunks], refs[5 * chunks:]

    def joined(k):
        return jnp.concatenate([ins[k * chunks + c][0] for c in range(chunks)], axis=0)

    x, a, d, dh1, dh3 = (joined(k) for k in range(5))
    g1_ref[0] = dot_at(x, dh1)
    g3_ref[0] = dot_at(x, dh3)
    g2_ref[0] = dot_at(a, d)


def weight_grads(xs, acts, ds, dh1s, dh3s):
    chunks = len(xs)
    experts, _, hidden = xs[0].shape
    ff = acts[0].shape[2]
    args = [*xs, *acts, *ds, *dh1s, *dh3s]
    outs = [(experts, hidden, ff), (experts, hidden, ff), (experts, ff, hidden)]
    return pl.pallas_call(
        functools.partial(dw_kernel, chunks),
        grid=(experts,),
        in_specs=[per_expert(a.shape) for a in args],
        out_specs=[per_expert(s) for s in outs],
        out_shape=[jax.ShapeDtypeStruct(s, F32) for s in outs],
        compiler_params=params(),
        cost_estimate=pl.CostEstimate(flops=25 * 10**9, bytes_accessed=120 * 10**6, transcendentals=0),
        name="weight_grads",
    )(*args)


def final_kernel(groups, *refs):
    q_ref, out_ref, pick_ref = refs[groups:]

    @pl.when(pl.program_id(0) == 0)
    def _():
        lanes = lax.broadcasted_iota(jnp.int32, pick_ref.shape[1:], 1)
        for h in range(groups):
            pick_ref[h] = jnp.where(q_ref[:, h:h + 1] == lanes, 1.0, 0.0).astype(BF)

    total = dot(pick_ref[0], refs[0][...])
    for h in range(1, groups):
        total = total + dot(pick_ref[h], refs[h][...])
    out_ref[...] = total.astype(BF)


def collect(parts, q_cols):
    groups = len(parts)
    tokens = q_cols.shape[0]
    grp_cap, hidden = parts[0].shape
    block = hidden // 3
    return pl.pallas_call(
        functools.partial(final_kernel, groups),
        grid=(3,),
        in_specs=[pl.BlockSpec((grp_cap, block), lambda n: (0, n))] * groups + [whole(q_cols.shape)],
        out_specs=pl.BlockSpec((tokens, block), lambda n: (0, n)),
        out_shape=jax.ShapeDtypeStruct((tokens, hidden), BF),
        scratch_shapes=[pltpu.VMEM((groups, tokens, grp_cap), BF)],
        compiler_params=params(),
        cost_estimate=pl.CostEstimate(flops=2 * 10**9, bytes_accessed=5 * 10**6, transcendentals=0),
        name="collect",
    )(*parts, q_cols)


def after(earlier, value):
    return lax.optimization_barrier((earlier, value))[1]


def slot_tables(ids, gates, first_exp, experts, group, per_group, cap):
    sources, _, tokens = ids.shape
    eq = ids[:, None] == (first_exp + jnp.arange(experts))[None, :, None, None]
    hit = jnp.any(eq, axis=2)
    gate = jnp.sum(jnp.where(eq, gates[:, None], 0.0), axis=2)
    member = jnp.any(ids // per_group == group, axis=1, keepdims=True)
    pos = count_earlier(jnp.concatenate([hit, member], axis=1).reshape(sources * (experts + 1), tokens))
    pos = pos.reshape(sources, experts + 1, tokens)
    exp_pos, grp_pos = pos[:, :experts], pos[:, experts:]
    taken = hit[:, :, None, :] & (exp_pos[:, :, None, :] == jnp.arange(cap, dtype=F32)[None, None, :, None])
    numbers = jnp.arange(1, tokens + 1, dtype=F32)[None, None, None, :]
    tok = jnp.sum(jnp.where(taken, numbers, 0.0), axis=3) - 1.0
    place = jnp.sum(jnp.where(taken, grp_pos[:, :, None, :] + 1.0, 0.0), axis=3) - 1.0
    weight = jnp.sum(jnp.where(taken, gate[:, :, None, :], 0.0), axis=3)
    here = jnp.sum(hit, axis=1).astype(F32)
    alone = here == jnp.sum(ids // per_group == group, axis=1).astype(F32)
    first = count_earlier(jnp.where(alone, jnp.minimum(here, 1.0), here))
    rank, seen = [], jnp.zeros((sources, tokens), F32)
    for e in range(experts):
        rank.append(seen)
        seen = seen + hit[:, e].astype(F32)
    unit = first[:, None] + jnp.where(alone[:, None], ALONE, jnp.stack(rank, axis=1)) + 1.0
    code = jnp.sum(jnp.where(taken, unit[:, :, None, :], 0.0), axis=3)
    lone = code > ALONE
    return tok, place, weight, jnp.where(lone, code - ALONE, code) - 1.0, lone


def longest_list(ids, per_group, experts, away):
    devices = away.shape[1]
    count = jnp.sum(ids[:, None] // experts == jnp.arange(devices)[None, :, None, None], axis=2)
    half = per_group // experts
    in_group = jnp.repeat(jnp.sum(count.reshape(ids.shape[0], devices // half, half, -1), axis=2), half, axis=1)
    rows = jnp.where(count == in_group, jnp.minimum(count, 1), count)
    return jnp.max(jnp.where(away, jnp.sum(rows, axis=2), 0))


def count_earlier(marks):
    tokens = marks.shape[1]
    earlier = (jnp.arange(tokens)[:, None] < jnp.arange(tokens)[None, :]).astype(BF)
    return jnp.dot(marks.astype(BF), earlier, preferred_element_type=F32)


def solution(mesh):
    groups = mesh.shape['grp']
    inner = mesh.shape['ing']
    devices = groups * inner
    tok_spec = P(('dp', 'grp', 'ing'), None)
    weight_spec = P(('grp', 'ing'), None, None)
    grad_spec = P(('dp', 'grp', 'ing'), None, None)

    def hop_y(a):
        return lax.ppermute(a, 'ing', [(0, 1), (1, 0)])

    def hop_g(a, bits):
        return lax.ppermute(a, 'grp', [(g, g ^ bits) for g in range(groups)])

    def device_fn(x_loc, ids_loc, gates_loc, dy_loc, w1, w3, w2):
        tokens, _ = x_loc.shape
        top_k = ids_loc.shape[1]
        experts = w1.shape[0]
        num_exp = experts * devices
        grp_cap = tokens * 2 // groups
        cap = 3 * tokens * top_k // (2 * num_exp)
        pad = -(-cap // 16) * 16
        grp, ing = lax.axis_index('grp'), lax.axis_index('ing')

        per_group = experts * inner
        own = jnp.concatenate([ids_loc.T.astype(F32), gates_loc.T], axis=0)[None]
        pair = jnp.concatenate([own, hop_y(own)], axis=0)
        pair_c = hop_g(pair, 1)
        quad_x = hop_g(jnp.concatenate([pair, pair_c], axis=0), 2)
        routing = jnp.stack([pair[1], pair_c[1], quad_x[1], quad_x[3], pair[0], pair_c[0], quad_x[0], quad_x[2]])

        x_far = hop_y(x_loc)
        dy_far = hop_y(dy_loc)
        x_near_c = hop_g(after(pair_c, x_loc), 1)
        x_near_x = hop_g(x_loc, 2)
        dy_near_c = hop_g(after(x_near_c, dy_loc), 1)
        x_far_c, x_far_x = hop_g(x_far, 1), hop_g(x_far, 2)
        x_near_xc, x_far_xc = hop_g(x_near_x, 1), hop_g(x_far_x, 1)
        dy_far_c, dy_far_x = hop_g(dy_far, 1), hop_g(dy_far, 2)
        dy_far_xc = hop_g(dy_far_x, 1)
        dy_near_x = hop_g(dy_loc, 2)
        dy_near_xc = hop_g(dy_near_x, 1)
        x_pairs = [(x_far, x_far_c), (x_far_x, x_far_xc), (x_loc, x_near_c), (x_near_x, x_near_xc)]
        dy_pairs = [(dy_far, dy_far_c), (dy_far_x, dy_far_xc), (dy_loc, dy_near_c), (dy_near_x, dy_near_xc)]

        ids_rel, gates_rel = routing[:, :top_k].astype(jnp.int32), routing[:, top_k:]
        units = tokens * SENT_SHARE[0] // SENT_SHARE[1]
        tok_rel, place_rel, weight_rel, unit_rel, lone_rel = slot_tables(ids_rel, gates_rel, (grp * inner + ing) * experts, experts, grp, per_group, cap)
        far = devices // 2
        source_ing = jnp.where(jnp.arange(devices) < far, 1 - ing, ing)
        away = source_ing[:, None] != (jnp.arange(devices) % inner)[None, :]
        over = longest_list(ids_rel, per_group, experts, away) > units
        over_flag = over.astype(jnp.int32).reshape(1)
        flat = [t[:far].reshape(far, 1, -1) for t in (unit_rel, place_rel, jnp.where(lone_rel, 1.0, weight_rel))]
        sent_here = flat[0] == jnp.arange(units, dtype=F32)[None, :, None]
        notes = jnp.stack([jnp.max(jnp.where(sent_here, flat[1], -1.0), axis=2), jnp.max(jnp.where(sent_here, flat[2], 0.0), axis=2)])
        notes = hop_y(notes)
        sent_place = notes[0].astype(jnp.int32).reshape(far, 1, units)
        sent_weight = notes[1].reshape(far, 1, units)
        own_groups = ids_loc.T[None] // per_group == (grp ^ jnp.arange(groups))[:, None, None]
        own_member = jnp.any(own_groups, axis=1)
        q_cols = jnp.where(own_member, count_earlier(own_member), -1.0).astype(jnp.int32).T
        slots = experts * cap
        tok_cols = tok_rel.astype(jnp.int32).reshape(devices, slots, 1)
        g_cols = weight_rel.reshape(devices, slots, 1)
        spare = ((0, 0), (0, 0), (0, pad - cap))
        q_rows = jnp.pad(place_rel, spare, constant_values=-1.0).astype(jnp.int32).reshape(devices, 1, experts * pad)
        g_rows = jnp.pad(weight_rel, spare).reshape(devices, 1, experts * pad)
        unit_rows = jnp.pad(unit_rel[:far], spare, constant_values=-1.0).astype(jnp.int32).reshape(far, 1, experts * pad)
        form_rows = jnp.pad(jnp.where(lone_rel, weight_rel, 1.0)[:far], spare).reshape(far, 1, experts * pad)

        xs, acts, ds, dh1s, dh3s, y_sums, dx_sums, y_sent, dx_sent = ([None] * 4 for _ in range(9))
        saved = {}
        last = None
        for step, c in KERNEL_ORDER:
            places = q_rows if last is None else after(last, q_rows)
            if step == 'n':
                xs[c], acts[c], ds[c], dh1s[c], dh3s[c], *sums = near_pair(c, *x_pairs[c], *dy_pairs[c], tok_cols, g_cols, places, g_rows, w1, w3, w2, cap, pad, grp_cap)
                y_sums[c], dx_sums[c] = sums[:PAIR], sums[PAIR:]
            elif step == 'm':
                xs[c], acts[c], ds[c], dh1s[c], dh3s[c], *sums = far_both_pair(c, *x_pairs[c], *dy_pairs[c], tok_cols, g_cols, places, g_rows, unit_rows, form_rows, over_flag, w1, w3, w2, cap, pad, grp_cap, units)
                y_sums[c], dx_sums[c], y_sent[c], dx_sent[c] = (sums[k:k + PAIR] for k in range(0, 4 * PAIR, PAIR))
            elif step == 'f':
                xs[c], acts[c], *saved[c], y0, y1, r0, r1 = far_forward_pair(c, *x_pairs[c], tok_cols, places, g_rows, unit_rows, form_rows, over_flag, w1, w3, w2, cap, pad, grp_cap, units)
                y_sums[c], y_sent[c] = (y0, y1), (r0, r1)
            else:
                ds[c], dh1s[c], dh3s[c], z0, z1, r0, r1 = far_backward_pair(c, *dy_pairs[c], tok_cols, g_cols, places, unit_rows, over_flag, w1, w3, w2, *saved[c], cap, pad, grp_cap, units)
                dx_sums[c], dx_sent[c] = (z0, z1), (r0, r1)
            last = (y_sums if step == 'f' else dx_sums)[c][0]

        grads = weight_grads(xs, acts, ds, dh1s, dh3s)

        def combine(results, sent, weighted, split):
            near = [*results[2], *results[3]]
            full = [*results[0], *results[1]]
            arrived = [hop_y(r) for r in (*sent[0], *sent[1])]
            sums = []
            for sources in split:

                def by_rows(ops):
                    return list(merge_sources(sources, ops[0], ops[1], sent_place, sent_weight, weighted))

                def by_sums(ops):
                    return [(n + hop_y(f)).astype(BF) for n, f in zip(ops[0], ops[2])]

                sums += lax.cond(over, by_sums, by_rows, tuple([rows[k] for k in sources] for rows in (near, arrived, full)))
            return [sums[0]] + [hop_g(sums[k], k) for k in (1, 2, 3)]

        y_parts = combine(y_sums, y_sent, True, ((0, 1), (2,), (3,)))
        y_out = collect(y_parts, q_cols)
        dx_parts = combine(dx_sums, dx_sent, False, ((0, 1), (2, 3)))
        dx_out = collect(dx_parts, q_cols)
        return y_out, dx_out, grads[0], grads[1], grads[2]

    return jax.shard_map(device_fn, mesh=mesh, in_specs=(tok_spec, tok_spec, tok_spec, tok_spec, weight_spec, weight_spec, weight_spec), out_specs=(tok_spec, tok_spec, grad_spec, grad_spec, grad_spec), check_vma=False)
```
